32 devices in a mesh: dp: 1 (over z), col: 4 (over y), row: 8 (over x, core).
Axes of the slice: x: 4, y: 4, z: 1, core: 2. Of those that a mesh axis runs over, the one named last changes fastest.
The devices are a block of a 4x4x8 slice.
Arguments:
- hidden: bfloat16 [128, 2048], P('dp', 'row')
- cache_len: int32 [128], P('dp')
- k_cache: bfloat16 [2, 128, 32, 512, 64], P(None, 'dp', ('col', 'row'))
- v_cache: bfloat16 [2, 128, 32, 512, 64], P(None, 'dp', ('col', 'row'))
- ln1_g: bfloat16 [2, 2048], P(None, 'row')
- ln1_b: bfloat16 [2, 2048], P(None, 'row')
- w_q: bfloat16 [2, 2048, 2048], P(None, 'row', 'col')
- b_q: bfloat16 [2, 2048], P(None, 'col')
- w_k: bfloat16 [2, 2048, 2048], P(None, 'row', 'col')
- b_k: bfloat16 [2, 2048], P(None, 'col')
- w_v: bfloat16 [2, 2048, 2048], P(None, 'row', 'col')
- b_v: bfloat16 [2, 2048], P(None, 'col')
- w_o: bfloat16 [2, 2048, 2048], P(None, 'col', 'row')
- b_o: bfloat16 [2, 2048], P(None, 'row')
- ln2_g: bfloat16 [2, 2048], P(None, 'row')
- ln2_b: bfloat16 [2, 2048], P(None, 'row')
- w_fc1: bfloat16 [2, 2048, 8192], P(None, 'row', 'col')
- b_fc1: bfloat16 [2, 8192], P(None, 'col')
- w_fc2: bfloat16 [2, 8192, 2048], P(None, 'col', 'row')
- b_fc2: bfloat16 [2, 2048], P(None, 'row')
Outputs:
- output 1: bfloat16 [128, 2048], P('dp', 'row')
- output 2: bfloat16 [2, 128, 32, 64], P(None, 'dp', ('col', 'row'))
- output 3: bfloat16 [2, 128, 32, 64], P(None, 'dp', ('col', 'row'))
All inputs are finite; a program needn't handle non-finite values.
Results may differ from the reference program's by a relative error of at most 0.019851.
Values are sent between devices in bfloat16 or wider.
A program may use at most 768 MiB of HBM per device.

```python
import jax
import jax.numpy as jnp
from jax import lax

BATCH = 128
D_MODEL = 2048
HEADS = 32
S_MAX = 512
LAYERS = 2
HEAD_DIM = D_MODEL // HEADS
FF_DIM = 4 * D_MODEL
EPS_LN = 1e-5


def setup_inputs(seed: int = 0, part: int = 0) -> dict:
    shared_key = jax.random.key(seed)
    part_key = jax.random.fold_in(shared_key, part)
    part_keys = jax.random.split(part_key, 6)
    weight_keys = jax.random.split(shared_key, 16)

    def normal(rng_key, shape):
        return jax.random.normal(rng_key, shape, jnp.float32)

    def weight(rng_key, shape, fan_in, gain):
        return (gain * fan_in ** -0.5 * normal(rng_key, shape)).astype(jnp.bfloat16)

    def vector(rng_key, shape, center, spread):
        return (center + spread * normal(rng_key, shape)).astype(jnp.bfloat16)

    hidden = normal(part_keys[0], (BATCH, D_MODEL)) + 0.7 * normal(part_keys[1], (BATCH, 1))
    lengths = jax.random.randint(part_keys[2], (BATCH,), 0, S_MAX)
    lengths = lengths.at[0].set(S_MAX - 1).at[1].set(0)
    cache_shape = (LAYERS, BATCH, HEADS, S_MAX, HEAD_DIM)
    k_cache = 1.5 * normal(part_keys[3], cache_shape)
    v_cache = normal(part_keys[4], cache_shape) + 0.8 * normal(part_keys[5], (LAYERS, BATCH, HEADS, 1, HEAD_DIM))
    vec_shape = (LAYERS, D_MODEL)
    square_shape = (LAYERS, D_MODEL, D_MODEL)
    return {
        "hidden": hidden.astype(jnp.bfloat16),
        "cache_len": lengths.astype(jnp.int32),
        "k_cache": k_cache.astype(jnp.bfloat16),
        "v_cache": v_cache.astype(jnp.bfloat16),
        "ln1_g": vector(weight_keys[0], vec_shape, 1.0, 0.3),
        "ln1_b": vector(weight_keys[1], vec_shape, 0.0, 0.3),
        "w_q": weight(weight_keys[2], square_shape, D_MODEL, 1.5),
        "b_q": vector(weight_keys[3], vec_shape, 0.0, 0.5),
        "w_k": weight(weight_keys[4], square_shape, D_MODEL, 1.0),
        "b_k": vector(weight_keys[5], vec_shape, 0.0, 0.5),
        "w_v": weight(weight_keys[6], square_shape, D_MODEL, 1.0),
        "b_v": vector(weight_keys[7], vec_shape, 0.0, 0.5),
        "w_o": weight(weight_keys[8], square_shape, D_MODEL, 1.0),
        "b_o": vector(weight_keys[9], vec_shape, 0.0, 0.3),
        "ln2_g": vector(weight_keys[10], vec_shape, 1.0, 0.3),
        "ln2_b": vector(weight_keys[11], vec_shape, 0.0, 0.3),
        "w_fc1": weight(weight_keys[12], (LAYERS, D_MODEL, FF_DIM), D_MODEL, 1.0),
        "b_fc1": vector(weight_keys[13], (LAYERS, FF_DIM), 0.0, 0.5),
        "w_fc2": weight(weight_keys[14], (LAYERS, FF_DIM, D_MODEL), FF_DIM, 1.0),
        "b_fc2": vector(weight_keys[15], vec_shape, 0.0, 0.3),
    }


def layer_norm(state, gain, shift):
    state_f32 = state.astype(jnp.float32)
    mean_val = jnp.sum(state_f32, axis=-1, keepdims=True) / D_MODEL
    mean_sq = jnp.sum(state_f32 * state_f32, axis=-1, keepdims=True) / D_MODEL
    variance = mean_sq - mean_val * mean_val
    normed = (state_f32 - mean_val) * lax.rsqrt(variance + EPS_LN) * gain.astype(jnp.float32) + shift.astype(jnp.float32)
    return normed.astype(jnp.bfloat16)


def project(normed, weight, bias):
    return jnp.dot(normed, weight, preferred_element_type=jnp.float32) + bias.astype(jnp.float32)


def attend_row(row_args):
    q_row, k_row, v_row, k_fresh, v_fresh, length = row_args
    positions = jnp.arange(S_MAX)
    at_new = (positions == length)[None, :, None]
    keys_all = jnp.where(at_new, k_fresh[:, None, :], k_row)
    values_all = jnp.where(at_new, v_fresh[:, None, :], v_row)
    scores = jnp.einsum("hd,hsd->hs", q_row.astype(jnp.float32), keys_all.astype(jnp.float32))
    scores = jnp.where((positions <= length)[None, :], scores, -jnp.inf)
    probs = jax.nn.softmax(scores, axis=-1).astype(jnp.bfloat16)
    mixed = jnp.einsum("hs,hsd->hd", probs.astype(jnp.float32), values_all.astype(jnp.float32))
    return mixed.astype(jnp.bfloat16)


def reference(hidden, cache_len, k_cache, v_cache, ln1_g, ln1_b, w_q, b_q, w_k, b_k, w_v, b_v, w_o, b_o, ln2_g, ln2_b, w_fc1, b_fc1, w_fc2, b_fc2):
    scale = HEAD_DIM ** -0.5

    def layer_step(state, layer_args):
        (k_layer, v_layer, gain_one, shift_one, wq_layer, bq_layer, wk_layer, bk_layer, wv_layer, bv_layer,
         wo_layer, bo_layer, gain_two, shift_two, fc1_layer, bfc1_layer, fc2_layer, bfc2_layer) = layer_args
        normed = layer_norm(state, gain_one, shift_one)
        q_all = (project(normed, wq_layer, bq_layer) * scale).astype(jnp.bfloat16).reshape(BATCH, HEADS, HEAD_DIM)
        k_all = project(normed, wk_layer, bk_layer).astype(jnp.bfloat16).reshape(BATCH, HEADS, HEAD_DIM)
        v_all = project(normed, wv_layer, bv_layer).astype(jnp.bfloat16).reshape(BATCH, HEADS, HEAD_DIM)
        attended = lax.map(attend_row, (q_all, k_layer, v_layer, k_all, v_all, cache_len))
        state_mid = (state.astype(jnp.float32) + project(attended.reshape(BATCH, D_MODEL), wo_layer, bo_layer)).astype(jnp.bfloat16)
        normed_two = layer_norm(state_mid, gain_two, shift_two)
        inner = jnp.maximum(project(normed_two, fc1_layer, bfc1_layer).astype(jnp.bfloat16), 0)
        state_out = (state_mid.astype(jnp.float32) + project(inner, fc2_layer, bfc2_layer)).astype(jnp.bfloat16)
        return state_out, (k_all, v_all)

    layer_inputs = (k_cache, v_cache, ln1_g, ln1_b, w_q, b_q, w_k, b_k, w_v, b_v, w_o, b_o, ln2_g, ln2_b, w_fc1, b_fc1, w_fc2, b_fc2)
    state_final, fresh_rows = lax.scan(layer_step, hidden, layer_inputs)
    return state_final, fresh_rows[0], fresh_rows[1]
```

```python
import functools

import jax
import jax.numpy as jnp
from jax import lax
from jax.experimental import pallas as pl
from jax.experimental.pallas import tpu as pltpu
from jax.sharding import PartitionSpec as P

EPS_LN = 1e-5
F32 = jnp.float32
BF16 = jnp.bfloat16
MESH = pl.DeviceIdType.MESH


def kernel(n_row, n_col, width,
           x_hbm, len_hbm, k_hbm, v_hbm, ln1g_hbm, ln1b_hbm, wq_hbm, bq_hbm, wk_hbm, bk_hbm, wv_hbm, bv_hbm,
           wo_hbm, bo_hbm, ln2g_hbm, ln2b_hbm, w1_hbm, b1_hbm, w2_hbm, b2_hbm,
           h_out, k_out, v_out,
           x_buf, len_buf, k_buf, v_buf, ln1g, ln1b, wq, bq, wk, bk, wv, bv, wo, bo, ln2g, ln2b, w1, b1, w2, b2,
           stat_src, stat_in, qkv_src, qkv_in, att_in, proj_in, up_src, up_in, act_in, down_in,
           state, twin, onehot, scores, probs_t, kt_buf, vt_buf, h_buf,
           in_sem, kv_sem, out_sem, send_sem, stat_sem, qkv_sem, att_sem, proj_sem, up_sem, act_sem, down_sem):
    layers = wq.shape[0]
    rows, cols = x_buf.shape
    head = k_buf.shape[2]
    lanes = 2 * head
    half = rows // 2
    n_chip = n_row // 2
    me = lax.axis_index("row")
    mine = lax.axis_index("col")
    chip = me // 2
    core = lax.rem(me, 2)

    smalls = [(x_hbm, x_buf), (len_hbm, len_buf), (ln1g_hbm, ln1g), (ln1b_hbm, ln1b), (bq_hbm, bq), (bk_hbm, bk),
              (bv_hbm, bv), (bo_hbm, bo), (ln2g_hbm, ln2g), (ln2b_hbm, ln2b), (b1_hbm, b1), (b2_hbm, b2)]
    small_copies = [pltpu.make_async_copy(src, dst, in_sem.at[i]) for i, (src, dst) in enumerate(smalls)]
    base = len(smalls)
    weights = [(wq_hbm, wq), (wk_hbm, wk), (wv_hbm, wv), (wo_hbm, wo), (w1_hbm, w1), (w2_hbm, w2)]
    weight_copies = [[pltpu.make_async_copy(src.at[l], dst.at[l], in_sem.at[base + l * len(weights) + i])
                      for i, (src, dst) in enumerate(weights)] for l in range(layers)]
    steps = rows // 16

    def cache_copy(l, which, t):
        src, dst = ((k_hbm, k_buf), (v_hbm, v_buf))[which]
        return pltpu.make_async_copy(src.at[l, pl.ds(16 * t, 16)], dst.at[l, pl.ds(16 * t, 16)], kv_sem.at[l, which, t])

    for copy in small_copies:
        copy.start()
    for l in range(layers):
        for copy in weight_copies[l][:3]:
            copy.start()
        for which in range(2):
            for t in range(steps):
                cache_copy(l, which, t).start()
        for copy in weight_copies[l][3:]:
            copy.start()

    barrier = pltpu.get_barrier_semaphore()
    for k in range(1, n_row):
        pl.semaphore_signal(barrier, inc=1, device_id={"row": lax.rem(me + k, n_row)}, device_id_type=MESH)
    for k in range(1, n_col):
        pl.semaphore_signal(barrier, inc=1, device_id={"col": lax.rem(mine + k, n_col)}, device_id_type=MESH)

    chip_order = [2, 1, 3] if n_chip == 4 else list(range(1, n_chip))

    def remote(src, dst, ssem, rsem, target):
        copy = pltpu.make_async_remote_copy(src_ref=src, dst_ref=dst, send_sem=ssem, recv_sem=rsem,
                                            device_id=target, device_id_type=MESH)
        copy.start()
        return copy

    def await_recv(dst, sem):
        pltpu.make_async_remote_copy(src_ref=dst, dst_ref=dst, send_sem=sem, recv_sem=sem,
                                     device_id={"row": me}, device_id_type=MESH).wait_recv()

    def row_peers():
        for dc in chip_order:
            for e in range(2):
                yield lax.rem(chip + dc, n_chip) * 2 + lax.rem(core + e, 2)
        yield chip * 2 + (1 - core)

    lane_id = lax.broadcasted_iota(jnp.int32, (16, 16 * head), 1)
    row_id = lax.broadcasted_iota(jnp.int32, (16, 16 * head), 0)
    onehot[...] = jnp.where(lane_id // head == row_id, 1.0, 0.0).astype(BF16)

    for copy in small_copies:
        copy.wait()

    def own_head(vec_ref, l):
        total = jnp.zeros((1, head), F32)
        for j in range(n_row):
            total = total + jnp.where(me == j, vec_ref[l:l + 1, j * head:(j + 1) * head].astype(F32), 0.0)
        return total

    len_col = jnp.transpose(jnp.broadcast_to(len_buf[...], (rows, rows)))[:, 0:1]
    state[...] = x_buf[...]
    pending = []

    def exchange_stats(n):
        xs = state[...].astype(F32)
        s1 = jnp.sum(xs, axis=1, keepdims=True)
        s2 = jnp.sum(xs * xs, axis=1, keepdims=True)
        lane = lax.broadcasted_iota(jnp.int32, (rows, 128), 1)
        both = jnp.where(lane == 0, s1, jnp.where(lane == 1, s2, 0.0))
        stat_src[n] = jnp.transpose(both)[0:8, :]
        if n == 0:
            pl.semaphore_wait(barrier, n_row + n_col - 2)
        for target in row_peers():
            pending.append(remote(stat_src.at[n], stat_in.at[n, me], send_sem.at[0], stat_sem.at[n, me], {"row": target}))
        stat_in[n, me] = stat_src[n]
        for k in range(1, n_row):
            j = lax.rem(me + k, n_row)
            await_recv(stat_in.at[n, j], stat_sem.at[n, j])
        total = stat_in[n, 0]
        for j in range(1, n_row):
            total = total + stat_in[n, j]
        mean = total[0:1, :] / width
        var = total[1:2, :] / width - mean * mean
        inv = lax.rsqrt(var + EPS_LN)
        mean_b = jnp.transpose(jnp.broadcast_to(mean, (128, rows)))
        inv_b = jnp.transpose(jnp.broadcast_to(inv, (128, rows)))
        return mean_b[:, 0:1], inv_b[:, 0:1]

    def layer_norm(n, gain, shift):
        mean, inv = exchange_stats(n)
        xs = state[...].astype(F32)
        return ((xs - mean) * inv * gain.astype(F32) + shift.astype(F32)).astype(BF16)

    low = lax.broadcasted_iota(jnp.int32, (rows, lanes), 1) < head
    low_half = low[0:half]

    for l in range(layers):
        normed = layer_norm(2 * l, ln1g[l:l + 1, :], ln1b[l:l + 1, :])
        for copy in weight_copies[l][:3]:
            copy.wait()
        for i, dc in enumerate(chip_order + [0]):
            dest = lax.rem(chip + dc, n_chip)
            at = pl.ds(pl.multiple_of(dest * lanes, lanes), lanes)
            qp = jnp.dot(normed, wq[l, :, at], preferred_element_type=F32)
            kp = jnp.dot(normed, wk[l, :, at], preferred_element_type=F32)
            vp = jnp.dot(normed, wv[l, :, at], preferred_element_type=F32)
            q_r = pltpu.roll(qp, head, axis=1)
            k_r = pltpu.roll(kp, head, axis=1)
            v_r = pltpu.roll(vp, head, axis=1)
            qkv_src[l, i, 0, 0:rows] = jnp.where(low, qp, k_r).astype(BF16)
            qkv_src[l, i, 1, 0:rows] = jnp.where(low, q_r, kp).astype(BF16)
            qkv_src[l, i, 0, rows:] = jnp.where(low_half, vp[0:half], v_r[half:]).astype(BF16)
            qkv_src[l, i, 1, rows:] = jnp.where(low_half, v_r[0:half], vp[half:]).astype(BF16)
            if dc != 0:
                for e in range(2):
                    pending.append(remote(qkv_src.at[l, i, e], qkv_in.at[l, me], send_sem.at[1], qkv_sem.at[l, me],
                                          {"row": dest * 2 + e}))
            else:
                pending.append(remote(qkv_src.at[l, i, 1 - core], qkv_in.at[l, me], send_sem.at[1], qkv_sem.at[l, me],
                                      {"row": dest * 2 + (1 - core)}))
        own = qkv_src[l, n_chip - 1, core]
        qkv_in[l, me] = own
        for k in range(1, n_row):
            j = lax.rem(me + k, n_row)
            await_recv(qkv_in.at[l, j], qkv_sem.at[l, j])
        total = qkv_in[l, 0].astype(F32)
        for j in range(1, n_row):
            total = total + qkv_in[l, j].astype(F32)
        scale = head ** -0.5
        qk = total[0:rows]
        vv = total[rows:]
        q_b = ((qk[:, 0:head] + own_head(bq, l)) * scale).astype(BF16)
        k_new = (pltpu.roll(qk, head, axis=1)[:, 0:head] + own_head(bk, l)).astype(BF16)
        v_new = (jnp.concatenate([vv[:, 0:head], pltpu.roll(vv, head, axis=1)[:, 0:head]], axis=0)
                 + own_head(bv, l)).astype(BF16)
        q_f = q_b.astype(F32)
        k_f = k_new.astype(F32)
        twin[...] = jnp.concatenate([q_f, q_f], axis=1).astype(BF16)
        kt_buf[l] = jnp.transpose(k_f).astype(BF16)
        v_t = jnp.transpose(v_new.astype(F32))
        vt_buf[l] = v_t.astype(BF16)
        pending.append(pltpu.make_async_copy(kt_buf.at[l], k_out.at[l], out_sem.at[0, l]))
        pending[-1].start()
        pending.append(pltpu.make_async_copy(vt_buf.at[l], v_out.at[l], out_sem.at[1, l]))
        pending[-1].start()
        score_new = jnp.sum(q_f * k_f, axis=1, keepdims=True)

        def score_step(t, carry, l=l):
            cache_copy(l, 0, t).wait()
            q_blk = twin[pl.ds(pl.multiple_of(16 * t, 16), 16), :]
            q_diag = jnp.concatenate([q_blk] * (16 * head // lanes), axis=1) * onehot[...]
            keys = k_buf[l, pl.ds(16 * t, 16)].reshape(16 * head, k_buf.shape[3])
            scores[pl.ds(pl.multiple_of(16 * t, 16), 16), :] = jnp.dot(q_diag, keys, preferred_element_type=F32)
            return carry

        lax.fori_loop(0, steps, score_step, 0)
        sc = scores[...]
        position = lax.broadcasted_iota(jnp.int32, sc.shape, 1)
        sc = jnp.where(position < len_col, sc, -jnp.inf)
        peak = jnp.maximum(jnp.max(sc, axis=1, keepdims=True), score_new)
        ex = jnp.exp(sc - peak)
        ex_new = jnp.exp(score_new - peak)
        mass = jnp.sum(ex, axis=1, keepdims=True) + ex_new
        scores[...] = ex / mass
        prob_new = (ex_new / mass).astype(BF16).astype(F32)
        for b in range(k_buf.shape[3] // 128):
            probs_t[b * 128:(b + 1) * 128, :] = jnp.transpose(scores[:, b * 128:(b + 1) * 128]).astype(BF16)
        prob_row = jnp.transpose(jnp.broadcast_to(prob_new, (rows, 128)))[0:1, :]
        lane64 = lax.broadcasted_iota(jnp.int32, (head, rows), 1)

        def mix_step(t, acc, l=l):
            cache_copy(l, 1, t).wait()
            values = v_buf[l, pl.ds(16 * t, 16)].reshape(16 * head, v_buf.shape[3])
            full = jnp.dot(values, probs_t[...], preferred_element_type=F32)
            for i in range(16):
                acc = jnp.where(lane64 == 16 * t + i, full[i * head:(i + 1) * head], acc)
            return acc

        mixed = lax.fori_loop(0, steps, mix_step, jnp.zeros((head, rows), F32))
        mixed = mixed + prob_row * v_t
        att_in[l, me] = mixed.astype(BF16)
        for target in row_peers():
            pending.append(remote(att_in.at[l, me], att_in.at[l, me], send_sem.at[2], att_sem.at[l, me], {"row": target}))
        weight_copies[l][3].wait()
        for k in range(1, n_row):
            j = lax.rem(me + k, n_row)
            await_recv(att_in.at[l, j], att_sem.at[l, j])
        gathered = att_in[l].reshape(n_row * head, rows)
        part = lax.dot_general(gathered, wo[l], (((0,), (0,)), ((), ())), preferred_element_type=F32)
        proj_in[l, mine] = part.astype(BF16)

        def all_reduce_col(buf, sem, bias, base_state):
            for k in (2, 1, 3) if n_col == 4 else range(1, n_col):
                pending.append(remote(buf.at[l, mine], buf.at[l, mine], send_sem.at[3], sem.at[l, mine],
                                      {"col": lax.rem(mine + k, n_col)}))
            for k in range(1, n_col):
                j = lax.rem(mine + k, n_col)
                await_recv(buf.at[l, j], sem.at[l, j])
            summed = buf[l, 0].astype(F32)
            for j in range(1, n_col):
                summed = summed + buf[l, j].astype(F32)
            return (base_state.astype(F32) + (summed + bias.astype(F32))).astype(BF16)

        state[...] = all_reduce_col(proj_in, proj_sem, bo[l:l + 1, :], state[...])
        normed = layer_norm(2 * l + 1, ln2g[l:l + 1, :], ln2b[l:l + 1, :])
        weight_copies[l][4].wait()
        for i, target in enumerate(row_peers()):
            at = pl.ds(pl.multiple_of(target * cols, cols), cols)
            up_src[l, i] = jnp.dot(normed, w1[l, :, at], preferred_element_type=F32).astype(BF16)
            pending.append(remote(up_src.at[l, i], up_in.at[l, me], send_sem.at[4], up_sem.at[l, me], {"row": target}))
        own_at = pl.ds(pl.multiple_of(me * cols, cols), cols)
        up_in[l, me] = jnp.dot(normed, w1[l, :, own_at], preferred_element_type=F32).astype(BF16)
        for k in range(1, n_row):
            j = lax.rem(me + k, n_row)
            await_recv(up_in.at[l, j], up_sem.at[l, j])
        summed = up_in[l, 0].astype(F32)
        for j in range(1, n_row):
            summed = summed + up_in[l, j].astype(F32)
        inner = jnp.maximum((summed + b1[l:l + 1, own_at].astype(F32)).astype(BF16), 0)
        act_in[l, me] = inner
        for target in row_peers():
            pending.append(remote(act_in.at[l, me], act_in.at[l, me], send_sem.at[5], act_sem.at[l, me], {"row": target}))
        weight_copies[l][5].wait()
        for k in range(1, n_row):
            j = lax.rem(me + k, n_row)
            await_recv(act_in.at[l, j], act_sem.at[l, j])
        part = jnp.dot(act_in[l, 0], w2[l, 0:cols, :], preferred_element_type=F32)
        for j in range(1, n_row):
            part = part + jnp.dot(act_in[l, j], w2[l, j * cols:(j + 1) * cols, :], preferred_element_type=F32)
        down_in[l, mine] = part.astype(BF16)
        state[...] = all_reduce_col(down_in, down_sem, b2[l:l + 1, :], state[...])

    h_buf[...] = state[...]
    last = pltpu.make_async_copy(h_buf, h_out, out_sem.at[0, 0])
    for copy in pending:
        if not copy.is_remote:
            copy.wait()
        else:
            copy.wait_send()
    last.start()
    last.wait()


def solution(mesh):
    n_row = mesh.shape["row"]
    n_col = mesh.shape["col"]
    act_spec = P("dp", "row")
    cache_spec = P(None, "dp", ("col", "row"), None, None)
    fresh_spec = P(None, "dp", ("col", "row"), None)
    in_weight = P(None, "row", "col")
    out_weight = P(None, "col", "row")
    col_vec = P(None, "col")
    row_vec = P(None, "row")
    in_specs = (act_spec, P("dp"), cache_spec, cache_spec, row_vec, row_vec,
                in_weight, col_vec, in_weight, col_vec, in_weight, col_vec,
                out_weight, row_vec, row_vec, row_vec, in_weight, col_vec, out_weight, row_vec)

    def local_step(hidden, cache_len, k_cache, v_cache, *params):
        rows, cols = hidden.shape
        layers, _, _, s_max, head = k_cache.shape
        keys = jnp.swapaxes(k_cache, 3, 4).reshape(layers, rows, head, s_max)
        values = jnp.swapaxes(v_cache, 3, 4).reshape(layers, rows, head, s_max)
        operands = (hidden, cache_len.reshape(1, rows), keys, values) + params
        vmem = [pltpu.VMEM(a.shape, a.dtype) for a in operands]
        dma = pltpu.SemaphoreType.DMA
        ff = params[12].shape[2]
        scratch = vmem + [
            pltpu.VMEM((2 * layers, 8, rows), F32),
            pltpu.VMEM((2 * layers, n_row, 8, rows), F32),
            pltpu.VMEM((layers, n_row // 2, 2, rows + rows // 2, 2 * head), BF16),
            pltpu.VMEM((layers, n_row, rows + rows // 2, 2 * head), BF16),
            pltpu.VMEM((layers, n_row, head, rows), BF16),
            pltpu.VMEM((layers, n_col, rows, cols), BF16),
            pltpu.VMEM((layers, n_row - 1, rows, ff // n_row), BF16),
            pltpu.VMEM((layers, n_row, rows, ff // n_row), BF16),
            pltpu.VMEM((layers, n_row, rows, ff // n_row), BF16),
            pltpu.VMEM((layers, n_col, rows, cols), BF16),
            pltpu.VMEM((rows, cols), BF16),
            pltpu.VMEM((rows, 2 * head), BF16),
            pltpu.VMEM((16, 16 * head), BF16),
            pltpu.VMEM((rows, s_max), F32),
            pltpu.VMEM((s_max, rows), BF16),
            pltpu.VMEM((layers, head, rows), BF16),
            pltpu.VMEM((layers, head, rows), BF16),
            pltpu.VMEM((rows, cols), BF16),
            dma((12 + 6 * layers,)),
            dma((layers, 2, rows // 16)),
            dma((2, layers)),
            dma((8,)),
            dma((2 * layers, n_row)),
            dma((layers, n_row)),
            dma((layers, n_row)),
            dma((layers, n_col)),
            dma((layers, n_row)),
            dma((layers, n_row)),
            dma((layers, n_col)),
        ]
        h, kt, vt = pl.pallas_call(
            functools.partial(kernel, n_row, n_col, cols * n_row),
            out_shape=(jax.ShapeDtypeStruct((rows, cols), BF16),
                       jax.ShapeDtypeStruct((layers, head, rows), BF16),
                       jax.ShapeDtypeStruct((layers, head, rows), BF16)),
            in_specs=[pl.BlockSpec(memory_space=pltpu.HBM)] * len(operands),
            out_specs=[pl.BlockSpec(memory_space=pltpu.HBM)] * 3,
            scratch_shapes=scratch,
            compiler_params=pltpu.CompilerParams(collective_id=0, has_side_effects=True,
                                                 vmem_limit_bytes=63 * 2 ** 20),
        )(*operands)
        k_new = jnp.swapaxes(kt, 1, 2).reshape(layers, rows, 1, head)
        v_new = jnp.swapaxes(vt, 1, 2).reshape(layers, rows, 1, head)
        return h, k_new, v_new

    return jax.shard_map(local_step, mesh=mesh, in_specs=in_specs,
                         out_specs=(act_spec, fresh_spec, fresh_spec), check_vma=False)
```

```python
import functools

import jax
import jax.numpy as jnp
from jax import lax
from jax.experimental import pallas as pl
from jax.experimental.pallas import tpu as pltpu
from jax.sharding import PartitionSpec as P

EPS_LN = 1e-5
F32 = jnp.float32
BF16 = jnp.bfloat16
MESH = pl.DeviceIdType.MESH


class Marks:
    def __init__(self):
        self.open = None

    def __call__(self, name):
        if self.open is not None:
            self.open.__exit__(None, None, None)
        self.open = None
        if name:
            self.open = jax.named_scope(name)
            self.open.__enter__()


def kernel(n_row, n_col, width,
           x_hbm, len_hbm, k_hbm, v_hbm, ln1g_hbm, ln1b_hbm, wq_hbm, bq_hbm, wk_hbm, bk_hbm, wv_hbm, bv_hbm,
           wo_hbm, bo_hbm, ln2g_hbm, ln2b_hbm, w1_hbm, b1_hbm, w2_hbm, b2_hbm,
           h_out, k_out, v_out,
           len_buf, k_buf, v_buf, ln1g, ln1b, wq, bq, wk, bk, wv, bv, wo, bo, ln2g, ln2b, w1, b1, w2, b2,
           state, pair, stat_src, stat_in, cq_src, cq_in, cu_src, cu_in,
           qkv_src, qkv_in, att_in, proj_in, up_src, up_in, act_in, down_in,
           twin, onehot, scores, probs_t,
           in_sem, kv_sem, send_sem, pw_sem, pair_sem, stat_sem, cq_sem, cu_sem,
           qkv_sem, att_sem, proj_sem, up_sem, act_sem, down_sem):
    mark = Marks()
    mark("entry")
    layers = wo.shape[0]
    rows, cols = state.shape[1:]
    head = k_buf.shape[2]
    s_max = k_buf.shape[3]
    lanes = 2 * head
    half = rows // 2
    n_chip = n_row // 2
    near = width // n_chip
    ff = w1.shape[3]
    me = lax.axis_index("row")
    mine = lax.axis_index("col")
    chip = me // 2
    core = lax.rem(me, 2)
    partner = chip * 2 + (1 - core)
    hops = [2, 1, 3] if n_chip == 4 else list(range(1, n_chip))
    far = len(hops)
    dests = [lax.rem(chip + dc, n_chip) for dc in hops] + [chip]
    pending = []

    def local(src, dst, sem):
        copy = pltpu.make_async_copy(src, dst, sem)
        copy.start()
        return copy

    def remote(src, dst, ssem, rsem, target):
        copy = pltpu.make_async_remote_copy(src_ref=src, dst_ref=dst, send_sem=ssem, recv_sem=rsem,
                                            device_id=target, device_id_type=MESH)
        copy.start()
        pending.append(copy)

    def await_recv(dst, sem):
        pltpu.make_async_remote_copy(src_ref=dst, dst_ref=dst, send_sem=sem, recv_sem=sem,
                                     device_id={"row": me}, device_id_type=MESH).wait_recv()

    def cache_copy(l, which, t):
        src, dst = ((k_hbm, k_buf), (v_hbm, v_buf))[which]
        return pltpu.make_async_copy(src.at[l, pl.ds(16 * t, 16)], dst.at[l, pl.ds(16 * t, 16)], kv_sem.at[l, which, t])

    steps = rows // 16
    norms = [(ln1g_hbm, ln1g), (ln1b_hbm, ln1b), (ln2g_hbm, ln2g), (ln2b_hbm, ln2b)]
    smalls = ([(x_hbm, state.at[0]), (len_hbm, len_buf), (bq_hbm, bq), (bk_hbm, bk), (bv_hbm, bv), (bo_hbm, bo),
               (b1_hbm, b1), (b2_hbm, b2)] + [(src, dst.at[0]) for src, dst in norms])
    small_copies = [local(src, dst, in_sem.at[0, i]) for i, (src, dst) in enumerate(smalls)]

    barrier = pltpu.get_barrier_semaphore()
    for k in range(1, n_row):
        pl.semaphore_signal(barrier, inc=1, device_id={"row": lax.rem(me + k, n_row)}, device_id_type=MESH)
    for k in range(1, n_col):
        pl.semaphore_signal(barrier, inc=1, device_id={"col": lax.rem(mine + k, n_col)}, device_id_type=MESH)

    def up_columns(i, which):
        return pl.ds(pl.multiple_of((dests[i] * 2 + which) * ff, ff), ff)

    def load_qkv(l):
        return [local(src.at[l], dst.at[l, 0:cols], in_sem.at[1 + l, i])
                for i, (src, dst) in enumerate([(wq_hbm, wq), (wk_hbm, wk), (wv_hbm, wv)])]

    def share_qkv(l):
        for i, (src, dst) in enumerate([(wq_hbm, wq), (wk_hbm, wk), (wv_hbm, wv)]):
            remote(src.at[l], dst.at[l, cols:], send_sem.at[6], pw_sem.at[l, i], {"row": partner})

    def load_rest(l):
        got = [local(wo_hbm.at[l], wo.at[l], in_sem.at[1 + l, 3]), local(w2_hbm.at[l], w2.at[l], in_sem.at[1 + l, 4])]
        return got + [local(w1_hbm.at[l, :, up_columns(i, core)], w1.at[l, i, 0:cols], in_sem.at[1 + l, 5 + i])
                      for i in range(n_chip)]

    def share_up(l):
        for i in range(n_chip):
            remote(w1_hbm.at[l, :, up_columns(i, 1 - core)], w1.at[l, i, cols:], send_sem.at[7], pw_sem.at[l, 3 + i],
                   {"row": partner})

    def load_cache(l):
        for which in range(2):
            for t in range(steps):
                cache_copy(l, which, t).start()

    loads = {("qkv", 0): load_qkv(0)}
    lane_id = lax.broadcasted_iota(jnp.int32, (16, 16 * head), 1)
    row_id = lax.broadcasted_iota(jnp.int32, (16, 16 * head), 0)
    onehot[...] = jnp.where(lane_id // head == row_id, 1.0, 0.0).astype(BF16)
    for copy in small_copies:
        copy.wait()
    mark("barrier")
    pl.semaphore_wait(barrier, n_row + n_col - 2)
    mark("entry2")

    def swap_state(n):
        remote(state.at[n], pair.at[n], send_sem.at[0], pair_sem.at[n], {"row": partner})

    swap_state(0)
    for i, (src, dst) in enumerate(norms):
        remote(dst.at[0], dst.at[1], send_sem.at[6], pw_sem.at[0, 3 + n_chip + i], {"row": partner})
    share_qkv(0)
    load_cache(0)
    loads["rest", 0] = load_rest(0)

    def own_head(vec_ref, l):
        total = jnp.zeros((1, head), F32)
        for j in range(n_row):
            total = total + jnp.where(me == j, vec_ref[l:l + 1, j * head:(j + 1) * head].astype(F32), 0.0)
        return total

    def side_operand(gain, shift, l):
        both = [jnp.concatenate([ref[0, l:l + 1], ref[1, l:l + 1]], axis=1).astype(F32) for ref in (gain, shift)]
        sub = lax.broadcasted_iota(jnp.int32, (16, near), 0)
        return jnp.where(sub == 0, both[0], jnp.where(sub == 1, both[1], 0.0)).astype(BF16)

    low = lax.broadcasted_iota(jnp.int32, (rows, lanes), 1) < head
    low_half = low[0:half]
    low8 = low[0:8]

    def split(q, k):
        q_own = jnp.where(core == 0, q, pltpu.roll(q, head, axis=1))
        k_own = jnp.where(core == 0, pltpu.roll(k, head, axis=1), k)
        return jnp.where(low[0:q.shape[0]], q_own, k_own)

    def qkv_tile(lhs, l, i):
        at = pl.ds(pl.multiple_of(dests[i] * lanes, lanes), lanes)
        return [jnp.dot(lhs, w[l, :, at], preferred_element_type=F32) for w in (wq, wk, wv)]

    def qkv_side(l):
        lhs = side_operand(ln1g, ln1b, l)
        for i in range(n_chip):
            q, k, v = qkv_tile(lhs, l, i)
            both = split(q, k)[0:8]
            vs = split(v, v)[0:8]
            vs = pltpu.roll(vs, 2, axis=0)
            sub = lax.broadcasted_iota(jnp.int32, (8, lanes), 0)
            cq_src[l, i] = jnp.where(sub < 2, both, vs)
            if i < far:
                remote(cq_src.at[l, i], cq_in.at[l, i], send_sem.at[1], cq_sem.at[l, i], {"row": dests[i] * 2 + core})

    def up_side(l):
        lhs = side_operand(ln2g, ln2b, l)
        for i in range(n_chip):
            cu_src[l, i] = jnp.dot(lhs, w1[l, i], preferred_element_type=F32)[0:8]
            if i < far:
                remote(cu_src.at[l, i], cu_in.at[l, i], send_sem.at[1], cu_sem.at[l, i], {"row": dests[i] * 2 + core})

    def normalize(n, gain, shift, l):
        await_recv(pair.at[n], pair_sem.at[n])
        mark("norm")
        xs = [state[n].astype(F32), pair[n].astype(F32)]
        s1 = jnp.sum(xs[0], axis=1, keepdims=True) + jnp.sum(xs[1], axis=1, keepdims=True)
        s2 = jnp.sum(xs[0] * xs[0], axis=1, keepdims=True) + jnp.sum(xs[1] * xs[1], axis=1, keepdims=True)
        mean = s1 / near
        inv = lax.rsqrt(jnp.maximum(s2 / near - mean * mean, 0.0) + EPS_LN)
        z = jnp.concatenate([((x - mean) * inv * gain[i, l:l + 1].astype(F32)).astype(BF16)
                             for i, x in enumerate(xs)], axis=1)
        return z, s1, s2

    def send_stats(n, s1, s2):
        lane = lax.broadcasted_iota(jnp.int32, (rows, 128), 1)
        both = jnp.where(lane == 0, s1, jnp.where(lane == 1, s2, 0.0))
        stat_src[n] = jnp.transpose(both)[0:8]
        for i in range(far):
            remote(stat_src.at[n], stat_in.at[n, i], send_sem.at[1], stat_sem.at[n, i], {"row": dests[i] * 2 + core})

    def stat_columns(n):
        for i in range(far):
            await_recv(stat_in.at[n, i], stat_sem.at[n, i])
        parts = [stat_in[n, i] for i in range(far)] + [stat_src[n]]
        total = parts[0]
        for part in parts[1:]:
            total = total + part
        mean = total[0:1] / width
        inv = lax.rsqrt(total[1:2] / width - mean * mean + EPS_LN)
        scales, shifts = [], []
        for part in parts:
            near_mean = part[0:1] / near
            near_var = jnp.maximum(part[1:2] / near - near_mean * near_mean, 0.0) + EPS_LN
            scales.append(inv * (near_var * lax.rsqrt(near_var)))
            shifts.append(inv * (near_mean - mean))
        table = jnp.concatenate(scales + shifts + [jnp.zeros((128 - 2 * n_chip, rows), F32)], axis=0)
        columns = jnp.transpose(table)
        return ([columns[:, i:i + 1] for i in range(n_chip)],
                [columns[:, n_chip + i:n_chip + i + 1] for i in range(n_chip)])

    len_col = jnp.transpose(jnp.broadcast_to(len_buf[...], (rows, rows)))[:, 0:1]

    def all_peers():
        for i in range(far):
            for e in range(2):
                yield dests[i] * 2 + lax.rem(core + e, 2)
        yield partner

    mark("side0")
    for copy in loads["qkv", 0]:
        copy.wait()
    for i in range(4):
        await_recv(norms[i][1].at[1], pw_sem.at[0, 3 + n_chip + i])
    for i, w in enumerate((wq, wk, wv)):
        await_recv(w.at[0, cols:], pw_sem.at[0, i])
    qkv_side(0)

    for l in range(layers):
        n = 2 * l
        if l > 0:
            for copy in loads["qkv", l]:
                copy.wait()
        mark("pair_wait")
        z, s1, s2 = normalize(n, ln1g, ln1b, l)
        mark("qkv_mm")
        for i in range(n_chip):
            q, k, v = qkv_tile(z, l, i)
            v_r = pltpu.roll(v, head, axis=1)
            low_v = jnp.where(core == 0, v, v_r)
            high_v = jnp.where(core == 0, v_r, v)
            block = qkv_src.at[l, i]
            block[0:rows] = split(q, k).astype(BF16)
            block[rows:] = jnp.where(low_half, low_v[0:half], high_v[half:]).astype(BF16)
            if i < far:
                remote(block, qkv_in.at[l, i], send_sem.at[2], qkv_sem.at[l, i], {"row": dests[i] * 2 + core})
            if i == 0:
                send_stats(n, s1, s2)
        if l == 0:
            share_up(0)
        mark("qkv_wait")
        for i in range(far):
            await_recv(cq_in.at[l, i], cq_sem.at[l, i])
        scales, shifts = stat_columns(n)
        total = jnp.zeros((rows + half, lanes), F32)
        const = jnp.zeros((8, lanes), F32)
        for i in [far] + list(range(far)):
            if i < far:
                await_recv(qkv_in.at[l, i], qkv_sem.at[l, i])
            part = (qkv_in[l, i] if i < far else qkv_src[l, i]).astype(F32)
            side = cq_in[l, i] if i < far else cq_src[l, i]
            scale_v = jnp.where(low_half, scales[i][0:half], scales[i][half:])
            shift_v = jnp.where(low_half, shifts[i][0:half], shifts[i][half:])
            total = total + jnp.concatenate([part[0:rows] * scales[i] + shifts[i] * side[0:1],
                                             part[rows:] * scale_v + shift_v * side[2:3]], axis=0)
            const = const + side
        mark("qkv_sum")
        qk = total[0:rows] + const[1:2]
        vv = total[rows:] + const[3:4]
        q_b = ((qk[:, 0:head] + own_head(bq, l)) * (head ** -0.5)).astype(BF16)
        k_new = (pltpu.roll(qk, head, axis=1)[:, 0:head] + own_head(bk, l)).astype(BF16)
        v_new = (jnp.concatenate([vv[:, 0:head], pltpu.roll(vv, head, axis=1)[:, 0:head]], axis=0)
                 + own_head(bv, l)).astype(BF16)
        q_f = q_b.astype(F32)
        k_f = k_new.astype(F32)
        twin[...] = jnp.concatenate([q_f, q_f], axis=1).astype(BF16)
        k_out[l] = jnp.transpose(k_f).astype(BF16)
        v_t = jnp.transpose(v_new.astype(F32))
        v_out[l] = v_t.astype(BF16)
        score_new = jnp.sum(q_f * k_f, axis=1, keepdims=True)

        mark("scores")

        def score_step(t, carry, l=l):
            for u in range(2):
                cache_copy(l, 0, 2 * t + u).wait()
            for u in range(2):
                at = pl.ds(pl.multiple_of(32 * t + 16 * u, 16), 16)
                q_diag = jnp.concatenate([twin[at, :]] * (16 * head // lanes), axis=1) * onehot[...]
                keys = k_buf[l, pl.ds(32 * t + 16 * u, 16)].reshape(16 * head, s_max)
                scores[at, :] = jnp.dot(q_diag, keys, preferred_element_type=F32)
            return carry

        lax.fori_loop(0, steps // 2, score_step, 0)
        mark("softmax")
        sc = scores[...]
        position = lax.broadcasted_iota(jnp.int32, sc.shape, 1)
        sc = jnp.where(position < len_col, sc, -jnp.inf)
        peak = jnp.maximum(jnp.max(sc, axis=1, keepdims=True), score_new)
        ex = jnp.exp(sc - peak)
        ex_new = jnp.exp(score_new - peak)
        mass = jnp.sum(ex, axis=1, keepdims=True) + ex_new
        scores[...] = ex / mass
        prob_new = (ex_new / mass).astype(BF16).astype(F32)
        for b in range(s_max // 128):
            probs_t[b * 128:(b + 1) * 128, :] = jnp.transpose(scores[:, b * 128:(b + 1) * 128]).astype(BF16)
        prob_row = jnp.transpose(jnp.broadcast_to(prob_new, (rows, 128)))[0:1, :]
        lane64 = lax.broadcasted_iota(jnp.int32, (head, rows), 1)
        mark("mix")

        def mix_step(t, acc, l=l):
            for u in range(2):
                cache_copy(l, 1, 2 * t + u).wait()
            values = v_buf[l, pl.ds(32 * t, 32)].reshape(32 * head, s_max)
            full = jnp.dot(values, probs_t[...], preferred_element_type=F32)
            for i in range(32):
                acc = jnp.where(lane64 == 32 * t + i, full[i * head:(i + 1) * head], acc)
            return acc

        mixed = lax.fori_loop(0, steps // 2, mix_step, jnp.zeros((head, rows), F32))
        mark("att_send")
        att_in[l, me] = (mixed + prob_row * v_t).astype(BF16)
        for target in all_peers():
            remote(att_in.at[l, me], att_in.at[l, me], send_sem.at[3], att_sem.at[l, me], {"row": target})
        mark("att_wait")
        if l + 1 < layers:
            loads["qkv", l + 1] = load_qkv(l + 1)
            load_cache(l + 1)
            loads["rest", l + 1] = load_rest(l + 1)
            share_qkv(l + 1)
            share_up(l + 1)
        for copy in loads["rest", l]:
            copy.wait()
        for i in range(n_chip):
            await_recv(w1.at[l, i, cols:], pw_sem.at[l, 3 + i])
        up_side(l)
        for k in range(1, n_row):
            j = lax.rem(me + k, n_row)
            await_recv(att_in.at[l, j], att_sem.at[l, j])
        mark("wo_mm")
        gathered = att_in[l].reshape(n_row * head, rows)
        part = lax.dot_general(gathered, wo[l], (((0,), (0,)), ((), ())), preferred_element_type=F32)
        proj_in[l, mine] = part.astype(BF16)

        def all_reduce_col(buf, sem, bias, base):
            mark("col_send")
            for k in (2, 1, 3) if n_col == 4 else range(1, n_col):
                remote(buf.at[l, mine], buf.at[l, mine], send_sem.at[4], sem.at[l, mine],
                       {"col": lax.rem(mine + k, n_col)})
            mark("col_wait")
            for k in range(1, n_col):
                j = lax.rem(mine + k, n_col)
                await_recv(buf.at[l, j], sem.at[l, j])
            mark("col_sum")
            summed = buf[l, 0].astype(F32)
            for j in range(1, n_col):
                summed = summed + buf[l, j].astype(F32)
            return (base.astype(F32) + (summed + bias.astype(F32))).astype(BF16)

        state[n + 1] = all_reduce_col(proj_in, proj_sem, bo[l:l + 1, :], state[n])
        swap_state(n + 1)
        mark("pair_wait")
        z, s1, s2 = normalize(n + 1, ln2g, ln2b, l)
        mark("up_mm")
        for i in range(n_chip):
            up_src[l, i] = jnp.dot(z, w1[l, i], preferred_element_type=F32).astype(BF16)
            if i < far:
                remote(up_src.at[l, i], up_in.at[l, i], send_sem.at[2], up_sem.at[l, i], {"row": dests[i] * 2 + core})
            if i == 0:
                send_stats(n + 1, s1, s2)
        mark("up_wait")
        if l + 1 < layers:
            for i, w in enumerate((wq, wk, wv)):
                await_recv(w.at[l + 1, cols:], pw_sem.at[l + 1, i])
            for copy in loads["qkv", l + 1]:
                copy.wait()
            loads["qkv", l + 1] = []
            qkv_side(l + 1)
        for i in range(far):
            await_recv(cu_in.at[l, i], cu_sem.at[l, i])
        scales, shifts = stat_columns(n + 1)
        total = jnp.zeros((rows, ff), F32)
        const = jnp.zeros((8, ff), F32)
        for i in [far] + list(range(far)):
            if i < far:
                await_recv(up_in.at[l, i], up_sem.at[l, i])
            part = (up_in[l, i] if i < far else up_src[l, i]).astype(F32)
            side = cu_in[l, i] if i < far else cu_src[l, i]
            total = total + (part * scales[i] + shifts[i] * side[0:1])
            const = const + side
        mark("up_sum")
        own_at = pl.ds(pl.multiple_of(me * ff, ff), ff)
        bias = b1[l:l + 1, own_at].astype(F32)
        act_in[l, me] = jnp.maximum((total + const[1:2] + bias).astype(BF16), 0)
        for i in range(far):
            remote(act_in.at[l, me], act_in.at[l, me], send_sem.at[5], act_sem.at[l, me], {"row": dests[i] * 2 + core})
        remote(act_in.at[l, me], act_in.at[l, me], send_sem.at[5], act_sem.at[l, me], {"row": partner})
        mark("act_wait")

        def down(j):
            return jnp.dot(act_in[l, j], w2[l, pl.ds(pl.multiple_of(j * ff, ff), ff), :], preferred_element_type=F32)

        part = down(me)
        await_recv(act_in.at[l, partner], act_sem.at[l, partner])
        part = part + down(partner)
        arrivals = [lax.rem(chip + n_chip - dc, n_chip) * 2 for dc in sorted(hops, key=lambda d: min(d, n_chip - d))]
        for j in arrivals:
            j = j + core
            await_recv(act_in.at[l, j], act_sem.at[l, j])
            remote(act_in.at[l, j], act_in.at[l, j], send_sem.at[5], act_sem.at[l, j], {"row": partner})
            part = part + down(j)
        for j in arrivals:
            j = j + 1 - core
            await_recv(act_in.at[l, j], act_sem.at[l, j])
            part = part + down(j)
        mark("down_mm")
        down_in[l, mine] = part.astype(BF16)
        new_state = all_reduce_col(down_in, down_sem, b2[l:l + 1, :], state[n + 1])
        if l + 1 < layers:
            state[n + 2] = new_state
            swap_state(n + 2)
        else:
            h_out[...] = new_state
    mark("tail")
    for copy in pending:
        copy.wait_send()
    mark(None)


def store(*refs):
    copies = [pltpu.make_async_copy(refs[i], refs[3 + i], refs[6].at[i]) for i in range(3)]
    for copy in copies:
        copy.start()
    for copy in copies:
        copy.wait()


def solution(mesh):
    n_row = mesh.shape["row"]
    n_col = mesh.shape["col"]
    act_spec = P("dp", "row")
    cache_spec = P(None, "dp", ("col", "row"), None, None)
    fresh_spec = P(None, "dp", ("col", "row"), None)
    in_weight = P(None, "row", "col")
    out_weight = P(None, "col", "row")
    col_vec = P(None, "col")
    row_vec = P(None, "row")
    in_specs = (act_spec, P("dp"), cache_spec, cache_spec, row_vec, row_vec,
                in_weight, col_vec, in_weight, col_vec, in_weight, col_vec,
                out_weight, row_vec, row_vec, row_vec, in_weight, col_vec, out_weight, row_vec)

    def local_step(hidden, cache_len, k_cache, v_cache, *params):
        rows, cols = hidden.shape
        layers, _, _, s_max, head = k_cache.shape
        keys = jnp.swapaxes(k_cache, 3, 4).reshape(layers, rows, head, s_max)
        values = jnp.swapaxes(v_cache, 3, 4).reshape(layers, rows, head, s_max)
        operands = (hidden, cache_len.reshape(1, rows), keys, values) + params
        dma = pltpu.SemaphoreType.DMA
        ff = params[12].shape[2]
        cols2 = 2 * cols
        n_chip = n_row // 2
        ff_own = ff // n_row
        shapes = [a.shape for a in operands]
        shapes = shapes[1:4] + [(2,) + s if i in (0, 1, 10, 11) else s for i, s in enumerate(shapes[4:])]
        for i in (5, 7, 9):
            shapes[i] = (layers, cols2, shapes[i][2])
        shapes[15] = (layers, n_chip, cols2, ff_own)
        vmem = [pltpu.VMEM(s, a.dtype) for s, a in zip(shapes, operands[1:])]
        scratch = vmem + [
            pltpu.VMEM((2 * layers, rows, cols), BF16),
            pltpu.VMEM((2 * layers, rows, cols), BF16),
            pltpu.VMEM((2 * layers, 8, rows), F32),
            pltpu.VMEM((2 * layers, n_chip - 1, 8, rows), F32),
            pltpu.VMEM((layers, n_chip, 8, 2 * head), F32),
            pltpu.VMEM((layers, n_chip - 1, 8, 2 * head), F32),
            pltpu.VMEM((layers, n_chip, 8, ff_own), F32),
            pltpu.VMEM((layers, n_chip - 1, 8, ff_own), F32),
            pltpu.VMEM((layers, n_chip, rows + rows // 2, 2 * head), BF16),
            pltpu.VMEM((layers, n_chip - 1, rows + rows // 2, 2 * head), BF16),
            pltpu.VMEM((layers, n_row, head, rows), BF16),
            pltpu.VMEM((layers, n_col, rows, cols), BF16),
            pltpu.VMEM((layers, n_chip, rows, ff_own), BF16),
            pltpu.VMEM((layers, n_chip - 1, rows, ff_own), BF16),
            pltpu.VMEM((layers, n_row, rows, ff_own), BF16),
            pltpu.VMEM((layers, n_col, rows, cols), BF16),
            pltpu.VMEM((rows, 2 * head), BF16),
            pltpu.VMEM((16, 16 * head), BF16),
            pltpu.VMEM((rows, s_max), F32),
            pltpu.VMEM((s_max, rows), BF16),
            dma((1 + layers, 12)),
            dma((layers, 2, rows // 16)),
            dma((8,)),
            dma((layers, 7 + n_chip)),
            dma((2 * layers,)),
            dma((2 * layers, n_chip - 1)),
            dma((layers, n_chip - 1)),
            dma((layers, n_chip - 1)),
            dma((layers, n_chip - 1)),
            dma((layers, n_row)),
            dma((layers, n_col)),
            dma((layers, n_chip - 1)),
            dma((layers, n_row)),
            dma((layers, n_col)),
        ]
        h, kt, vt = pl.pallas_call(
            functools.partial(kernel, n_row, n_col, cols * n_row),
            out_shape=(pltpu.VMEM((rows, cols), BF16),
                       pltpu.VMEM((layers, head, rows), BF16),
                       pltpu.VMEM((layers, head, rows), BF16)),
            in_specs=[pl.BlockSpec(memory_space=pltpu.HBM)] * len(operands),
            out_specs=[pl.BlockSpec(memory_space=pltpu.VMEM)] * 3,
            scratch_shapes=scratch,
            compiler_params=pltpu.CompilerParams(collective_id=0, has_side_effects=True,
                                                 vmem_limit_bytes=63 * 2 ** 20),
        )(*operands)
        h, kt, vt = pl.pallas_call(
            store,
            out_shape=(jax.ShapeDtypeStruct((rows, cols), BF16),
                       jax.ShapeDtypeStruct((layers, head, rows), BF16),
                       jax.ShapeDtypeStruct((layers, head, rows), BF16)),
            in_specs=[pl.BlockSpec(memory_space=pltpu.VMEM)] * 3,
            out_specs=[pl.BlockSpec(memory_space=pltpu.HBM)] * 3,
            scratch_shapes=[dma((3,))],
        )(*[pltpu.with_memory_space_constraint(a, pltpu.VMEM) for a in (h, kt, vt)])
        k_new = jnp.swapaxes(kt, 1, 2).reshape(layers, rows, 1, head)
        v_new = jnp.swapaxes(vt, 1, 2).reshape(layers, rows, 1, head)
        return h, k_new, v_new

    return jax.shard_map(local_step, mesh=mesh, in_specs=in_specs,
                         out_specs=(act_spec, fresh_spec, fresh_spec), check_vma=False)
```

```python
import functools

import jax
import jax.numpy as jnp
from jax import lax
from jax.experimental import pallas as pl
from jax.experimental.pallas import tpu as pltpu
from jax.sharding import PartitionSpec as P

EPS_LN = 1e-5
F32 = jnp.float32
BF16 = jnp.bfloat16
MESH = pl.DeviceIdType.MESH


class Marks:
    def __init__(self):
        self.open = None

    def __call__(self, name):
        if self.open is not None:
            self.open.__exit__(None, None, None)
        self.open = None
        if name:
            self.open = jax.named_scope(name)
            self.open.__enter__()


HALVES = 2


def kernel(n_row, n_col, width,
           x_hbm, len_hbm, k_hbm, v_hbm, ln1g_hbm, ln1b_hbm, wq_hbm, bq_hbm, wk_hbm, bk_hbm, wv_hbm, bv_hbm,
           wo_hbm, bo_hbm, ln2g_hbm, ln2b_hbm, w1_hbm, b1_hbm, w2_hbm, b2_hbm,
           h_out, k_out, v_out,
           len_buf, k_buf, v_buf, ln1g, ln1b, wq, bq, wk, bk, wv, bv, wo, bo, ln2g, ln2b, w1, b1, w2, b2,
           state, pair, stat_src, stat_in, cq_src, cq_in, cu_src, cu_in, w_in, w_share,
           qkv_src, qkv_in, att_in, proj_in, up_src, up_in, act_in, down_in,
           twin, onehot, scores, probs_t,
           in_sem, kv_sem, send_sem, pw_sem, pair_sem, stat_sem, cq_sem, cu_sem,
           qkv_sem, att_sem, proj_sem, up_sem, act_sem, down_sem):
    mark = Marks()
    mark("entry")
    layers = wo.shape[0]
    rows, cols = state.shape[2:]
    batch = rows * HALVES
    head = k_buf.shape[2]
    s_max = k_buf.shape[3]
    lanes = 2 * head
    half = rows // 2
    n_chip = n_row // 2
    near = width // n_chip
    ff = w1.shape[3]
    me = lax.axis_index("row")
    mine = lax.axis_index("col")
    chip = me // 2
    core = lax.rem(me, 2)
    partner = chip * 2 + (1 - core)
    hops = [2, 1, 3]
    far = len(hops)
    dests = [lax.rem(chip + dc, n_chip) for dc in hops] + [chip]
    peers = [dest * 2 + core for dest in dests[:far]]
    arrivals = [lax.rem(chip + n_chip - dc, n_chip) * 2 for dc in (1, 3, 2)]
    pending = []

    def local(src, dst, sem):
        copy = pltpu.make_async_copy(src, dst, sem)
        copy.start()
        return copy

    def remote(src, dst, ssem, rsem, target):
        copy = pltpu.make_async_remote_copy(src_ref=src, dst_ref=dst, send_sem=ssem, recv_sem=rsem,
                                            device_id=target, device_id_type=MESH)
        copy.start()
        pending.append(copy)

    def await_recv(dst, sem):
        pltpu.make_async_remote_copy(src_ref=dst, dst_ref=dst, send_sem=sem, recv_sem=sem,
                                     device_id={"row": me}, device_id_type=MESH).wait_recv()

    def cache_copy(l, which, t):
        src, dst = ((k_hbm, k_buf), (v_hbm, v_buf))[which]
        return pltpu.make_async_copy(src.at[l, pl.ds(16 * t, 16)], dst.at[l, pl.ds(16 * t, 16)], kv_sem.at[l, which, t])

    norms = [(ln1g_hbm, ln1g), (ln1b_hbm, ln1b), (ln2g_hbm, ln2g), (ln2b_hbm, ln2b)]
    smalls = ([(len_hbm, len_buf), (bq_hbm, bq), (bk_hbm, bk), (bv_hbm, bv), (bo_hbm, bo), (b1_hbm, b1), (b2_hbm, b2)]
              + [(src, dst.at[0]) for src, dst in norms]
              + [(x_hbm.at[h * rows:(h + 1) * rows], state.at[0, h]) for h in range(HALVES)])
    small_copies = [local(src, dst, in_sem.at[0, i]) for i, (src, dst) in enumerate(smalls)]

    def load_qkv(l):
        return [local(src.at[l], dst.at[l], in_sem.at[1 + l, i])
                for i, (src, dst) in enumerate([(wq_hbm, wq), (wk_hbm, wk), (wv_hbm, wv)])]

    loads = {("qkv", 0): load_qkv(0)}
    barrier = pltpu.get_barrier_semaphore()
    for k in range(1, n_row):
        pl.semaphore_signal(barrier, inc=1, device_id={"row": lax.rem(me + k, n_row)}, device_id_type=MESH)
    for k in range(1, n_col):
        pl.semaphore_signal(barrier, inc=1, device_id={"col": lax.rem(mine + k, n_col)}, device_id_type=MESH)

    def up_columns(i, which):
        return pl.ds(pl.multiple_of((dests[i] * 2 + which) * ff, ff), ff)

    def load_rest(l):
        got = [local(wo_hbm.at[l, :, i], wo.at[l, i], in_sem.at[1 + l, 3 + i]) for i in range(2)]
        got.append(local(w2_hbm.at[l], w2.at[l], in_sem.at[1 + l, 5]))
        return got + [local(w1_hbm.at[l, :, up_columns(i, core)], w1.at[l, i, 0:cols], in_sem.at[1 + l, 6 + i])
                      for i in range(n_chip)]

    def share_up(l):
        for i in range(n_chip):
            remote(w1_hbm.at[l, :, up_columns(i, 1 - core)], w1.at[l, i, cols:], send_sem.at[7], pw_sem.at[l, 1 + i],
                   {"row": partner})

    def load_cache(l):
        for which in range(2):
            for t in range(batch // 16):
                cache_copy(l, which, t).start()

    low = lax.broadcasted_iota(jnp.int32, (cols, lanes), 1) < head
    low_half = low[0:half]

    def repack(l):
        def tile(w, i):
            return w[l, :, pl.ds(pl.multiple_of(dests[i] * lanes, lanes), lanes)].astype(F32)

        pairs = [(wq, 0, wk, 0), (wv, 0, wv, 1), (wq, 1, wk, 1), (wq, 2, wk, 2), (wv, 2, wv, 3), (wq, 3, wk, 3)]
        for t, (wa, ia, wb, ib) in enumerate(pairs):
            a, b = tile(wa, ia), tile(wb, ib)
            first = jnp.where(low, a, pltpu.roll(b, head, axis=1)).astype(BF16)
            second = jnp.where(low, pltpu.roll(a, head, axis=1), b).astype(BF16)
            at = slice(t * lanes, (t + 1) * lanes)
            w_in[l, 0:cols, at] = jnp.where(core == 0, first, second)
            w_share[l, :, at] = jnp.where(core == 0, second, first)

    def share_qkv(l):
        remote(w_share.at[l], w_in.at[l, cols:], send_sem.at[6], pw_sem.at[l, 0], {"row": partner})

    def swap_state(n, h):
        remote(state.at[n, h], pair.at[n, h], send_sem.at[0], pair_sem.at[n, h], {"row": partner})

    lane_id = lax.broadcasted_iota(jnp.int32, (16, 16 * head), 1)
    row_id = lax.broadcasted_iota(jnp.int32, (16, 16 * head), 0)
    onehot[...] = jnp.where(lane_id // head == row_id, 1.0, 0.0).astype(BF16)
    for copy in small_copies:
        copy.wait()
    mark("load0")
    for copy in loads["qkv", 0]:
        copy.wait()
    load_cache(0)
    loads["rest", 0] = load_rest(0)
    mark("repack0")
    repack(0)
    mark("barrier")
    pl.semaphore_wait(barrier, n_row + n_col - 2)
    mark("entry2")
    for h in range(HALVES):
        swap_state(0, h)
    for i, (src, dst) in enumerate(norms):
        remote(dst.at[0], dst.at[1], send_sem.at[6], pw_sem.at[0, 1 + n_chip + i], {"row": partner})
    share_qkv(0)

    def own_head(vec_ref, l):
        total = jnp.zeros((1, head), F32)
        for j in range(n_row):
            total = total + jnp.where(me == j, vec_ref[l:l + 1, j * head:(j + 1) * head].astype(F32), 0.0)
        return total

    def side_operand(gain, shift, l):
        both = [jnp.concatenate([ref[0, l:l + 1], ref[1, l:l + 1]], axis=1).astype(F32) for ref in (gain, shift)]
        sub = lax.broadcasted_iota(jnp.int32, (16, near), 0)
        return jnp.where(sub == 0, both[0], jnp.where(sub == 1, both[1], 0.0)).astype(BF16)

    def qkv_products(lhs, l):
        wide = 2 * lanes
        for t in range(3):
            full = jnp.dot(lhs, w_in[l, :, t * wide:(t + 1) * wide], preferred_element_type=F32)
            yield full[:, 0:lanes], full[:, lanes:]

    def qkv_blocks(lhs, l):
        tiles = qkv_products(lhs, l)
        qk0, v01 = next(tiles)
        yield qk0, v01, 0
        qk1, qk2 = next(tiles)
        yield qk1, v01, 1
        v23, qk3 = next(tiles)
        yield qk2, v23, 0
        yield qk3, v23, 1

    def qkv_side(l):
        lhs = side_operand(ln1g, ln1b, l)
        for i, (qk, v, side) in enumerate(qkv_blocks(lhs, l)):
            v, low8 = v[0:8], low[0:8]
            v_r = pltpu.roll(v, head, axis=1)
            vs = jnp.where(low8, v, v_r) if side == 0 else jnp.where(low8, v_r, v)
            sub = lax.broadcasted_iota(jnp.int32, (8, lanes), 0)
            cq_src[l, i] = jnp.where(sub < 2, qk[0:8], pltpu.roll(vs, 2, axis=0))
            if i < far:
                remote(cq_src.at[l, i], cq_in.at[l, i], send_sem.at[1], cq_sem.at[l, i], {"row": peers[i]})

    def up_side(l):
        lhs = side_operand(ln2g, ln2b, l)
        for i in range(n_chip):
            cu_src[l, i] = jnp.dot(lhs, w1[l, i], preferred_element_type=F32)[0:8]
            if i < far:
                remote(cu_src.at[l, i], cu_in.at[l, i], send_sem.at[1], cu_sem.at[l, i], {"row": peers[i]})

    def normalize(n, h, gain, l):
        await_recv(pair.at[n, h], pair_sem.at[n, h])
        mark("norm")
        xs = [state[n, h].astype(F32), pair[n, h].astype(F32)]
        s1 = jnp.sum(xs[0] + xs[1], axis=1, keepdims=True)
        s2 = jnp.sum(xs[0] * xs[0] + xs[1] * xs[1], axis=1, keepdims=True)
        mean = s1 / near
        inv = lax.rsqrt(jnp.maximum(s2 / near - mean * mean, 0.0) + EPS_LN)
        z = jnp.concatenate([((x - mean) * inv * gain[i, l:l + 1].astype(F32)).astype(BF16)
                             for i, x in enumerate(xs)], axis=1)
        return z, s1, s2

    def send_stats(n, h, s1, s2):
        lane = lax.broadcasted_iota(jnp.int32, (rows, 128), 1)
        both = jnp.where(lane == 0, s1, jnp.where(lane == 1, s2, 0.0))
        both = jnp.concatenate([both, jnp.zeros((128 - rows, 128), F32)], axis=0)
        stat_src[n, h] = jnp.transpose(both)[0:8]
        for i in range(far):
            remote(stat_src.at[n, h], stat_in.at[n, h, i], send_sem.at[1], stat_sem.at[n, h, i], {"row": peers[i]})

    def stat_columns(n, h):
        for i in range(far):
            await_recv(stat_in.at[n, h, i], stat_sem.at[n, h, i])
        parts = [stat_in[n, h, i] for i in range(far)] + [stat_src[n, h]]
        total = parts[0]
        for part in parts[1:]:
            total = total + part
        mean = total[0:1] / width
        inv = lax.rsqrt(total[1:2] / width - mean * mean + EPS_LN)
        scales, shifts = [], []
        for part in parts:
            near_mean = part[0:1] / near
            near_var = jnp.maximum(part[1:2] / near - near_mean * near_mean, 0.0) + EPS_LN
            scales.append(inv * (near_var * lax.rsqrt(near_var)))
            shifts.append(inv * (near_mean - mean))
        table = jnp.concatenate(scales + shifts + [jnp.zeros((128 - 2 * n_chip, 128), F32)], axis=0)
        columns = jnp.transpose(table)[0:rows]
        return ([columns[:, i:i + 1] for i in range(n_chip)],
                [columns[:, n_chip + i:n_chip + i + 1] for i in range(n_chip)])

    len_all = jnp.transpose(jnp.broadcast_to(len_buf[...], (batch, batch)))
    fresh = {}

    def qkv_go(l, h):
        n = 2 * l
        mark("pair_wait")
        z, s1, s2 = normalize(n, h, ln1g, l)
        mark("qkv_mm")
        for i, (qk, v, side) in enumerate(qkv_blocks(z, l)):
            v_r = pltpu.roll(v, head, axis=1)
            a, b = (v, v_r) if side == 0 else (v_r, v)
            block = qkv_src.at[l, h, i]
            block[0:rows] = qk.astype(BF16)
            block[rows:] = jnp.where(low_half, a[0:half], b[half:]).astype(BF16)
            if i < far:
                remote(block, qkv_in.at[l, h, i], send_sem.at[2], qkv_sem.at[l, h, i], {"row": peers[i]})
            if i == 0:
                send_stats(n, h, s1, s2)

    def qkv_recv(l, h):
        mark("qkv_wait")
        for i in range(far if h == 0 else 0):
            await_recv(cq_in.at[l, i], cq_sem.at[l, i])
        scales, shifts = stat_columns(2 * l, h)
        qk = jnp.zeros((rows, lanes), F32)
        vv = jnp.zeros((half, lanes), F32)
        const = jnp.zeros((8, lanes), F32)
        for i in (far, 1, 2, 0):
            if i < far:
                await_recv(qkv_in.at[l, h, i], qkv_sem.at[l, h, i])
            block = qkv_in.at[l, h, i] if i < far else qkv_src.at[l, h, i]
            side = cq_in[l, i] if i < far else cq_src[l, i]
            scale_v = jnp.where(low_half, scales[i][0:half], scales[i][half:])
            shift_v = jnp.where(low_half, shifts[i][0:half], shifts[i][half:])
            qk = qk + (block[0:rows].astype(F32) * scales[i] + shifts[i] * side[0:1])
            vv = vv + (block[rows:].astype(F32) * scale_v + shift_v * side[2:3])
            const = const + side
        mark("qkv_sum")
        qk = qk + const[1:2]
        vv = vv + const[3:4]
        q_b = ((qk[:, 0:head] + own_head(bq, l)) * (head ** -0.5)).astype(BF16)
        k_new = (pltpu.roll(qk, head, axis=1)[:, 0:head] + own_head(bk, l)).astype(BF16)
        v_new = (jnp.concatenate([vv[:, 0:head], pltpu.roll(vv, head, axis=1)[:, 0:head]], axis=0)
                 + own_head(bv, l)).astype(BF16)
        q_f = q_b.astype(F32)
        k_f = k_new.astype(F32)
        mine_rows = slice(h * rows, (h + 1) * rows)
        twin[mine_rows, :] = jnp.concatenate([q_f, q_f], axis=1).astype(BF16)
        k_out[l, :, mine_rows] = jnp.transpose(k_f).astype(BF16)
        v_t = jnp.transpose(v_new.astype(F32))
        v_out[l, :, mine_rows] = v_t.astype(BF16)
        fresh[l, h] = (jnp.sum(q_f * k_f, axis=1, keepdims=True), v_t)

    def attend(l, h):
        score_new, v_t = fresh[l, h]
        base = h * rows
        mark("scores")

        def score_step(t, carry):
            for u in range(2):
                cache_copy(l, 0, base // 16 + 2 * t + u).wait()
            for u in range(2):
                at = pl.ds(pl.multiple_of(base + 32 * t + 16 * u, 16), 16)
                q_diag = jnp.concatenate([twin[at, :]] * (16 * head // lanes), axis=1) * onehot[...]
                keys = k_buf[l, pl.ds(base + 32 * t + 16 * u, 16)].reshape(16 * head, s_max)
                scores[at, :] = jnp.dot(q_diag, keys, preferred_element_type=F32)
            return carry

        lax.fori_loop(0, rows // 32, score_step, 0)
        mark("softmax")
        mine_rows = slice(base, base + rows)
        sc = scores[mine_rows, :]
        position = lax.broadcasted_iota(jnp.int32, sc.shape, 1)
        sc = jnp.where(position < len_all[mine_rows, 0:1], sc, -jnp.inf)
        peak = jnp.maximum(jnp.max(sc, axis=1, keepdims=True), score_new)
        ex = jnp.exp(sc - peak)
        ex_new = jnp.exp(score_new - peak)
        mass = jnp.sum(ex, axis=1, keepdims=True) + ex_new
        scores[mine_rows, :] = ex / mass
        prob_new = (ex_new / mass).astype(BF16).astype(F32)
        for b in range(s_max // 128):
            probs_t[h, b * 128:(b + 1) * 128, :] = jnp.transpose(scores[mine_rows, b * 128:(b + 1) * 128]).astype(BF16)
        prob_row = jnp.transpose(jnp.broadcast_to(prob_new, (rows, 128)))[0:1, :]
        lane = lax.broadcasted_iota(jnp.int32, (head, rows), 1)
        mark("mix")

        def mix_step(t, acc):
            for u in range(2):
                cache_copy(l, 1, base // 16 + 2 * t + u).wait()
            values = v_buf[l, pl.ds(base + 32 * t, 32)].reshape(32 * head, s_max)
            full = jnp.dot(values, probs_t[h], preferred_element_type=F32)
            for i in range(32):
                acc = jnp.where(lane == 32 * t + i, full[i * head:(i + 1) * head], acc)
            return acc

        mixed = lax.fori_loop(0, rows // 32, mix_step, jnp.zeros((head, rows), F32))
        mark("att_send")
        mixed = mixed + prob_row * v_t
        att_in[l, h, me] = jnp.concatenate([mixed[0:head // 2], mixed[head // 2:]], axis=1).astype(BF16)
        for target in [d * 2 + lax.rem(core + e, 2) for d in dests[:far] for e in range(2)] + [partner]:
            remote(att_in.at[l, h, me], att_in.at[l, h, me], send_sem.at[3], att_sem.at[l, h, me], {"row": target})

    def col_send(buf, sem, l, h):
        mark("col_send")
        for k in (2, 1, 3):
            remote(buf.at[l, h, mine], buf.at[l, h, mine], send_sem.at[4], sem.at[l, h, mine],
                   {"col": lax.rem(mine + k, n_col)})

    def col_recv(buf, sem, l, h, bias, base):
        mark("col_wait")
        for k in range(1, n_col):
            j = lax.rem(mine + k, n_col)
            await_recv(buf.at[l, h, j], sem.at[l, h, j])
        mark("col_sum")
        summed = buf[l, h, 0].astype(F32)
        for j in range(1, n_col):
            summed = summed + buf[l, h, j].astype(F32)
        return (base.astype(F32) + (summed + bias.astype(F32))).astype(BF16)

    def project(l, h):
        mark("att_wait")
        for k in range(1, n_row):
            j = lax.rem(me + k, n_row)
            await_recv(att_in.at[l, h, j], att_sem.at[l, h, j])
        mark("wo_mm")
        gathered = att_in[l, h].reshape(n_row * head // 2, 2 * rows)
        both = [lax.dot_general(gathered, wo[l, i].reshape(n_row * head // 2, cols), (((0,), (0,)), ((), ())),
                                preferred_element_type=F32) for i in range(2)]
        proj_in[l, h, mine] = (both[0][0:rows] + both[1][rows:]).astype(BF16)
        col_send(proj_in, proj_sem, l, h)

    def up_go(l, h):
        n = 2 * l + 1
        mark("pair_wait")
        z, s1, s2 = normalize(n, h, ln2g, l)
        mark("up_mm")
        for i in range(n_chip):
            up_src[l, h, i] = jnp.dot(z, w1[l, i], preferred_element_type=F32).astype(BF16)
            if i < far:
                remote(up_src.at[l, h, i], up_in.at[l, h, i], send_sem.at[2], up_sem.at[l, h, i], {"row": peers[i]})
            if i == 0:
                send_stats(n, h, s1, s2)

    def up_recv(l, h):
        mark("up_wait")
        for i in range(far if h == 0 else 0):
            await_recv(cu_in.at[l, i], cu_sem.at[l, i])
        scales, shifts = stat_columns(2 * l + 1, h)
        total = jnp.zeros((rows, ff), F32)
        const = jnp.zeros((8, ff), F32)
        for i in (far, 1, 2, 0):
            if i < far:
                await_recv(up_in.at[l, h, i], up_sem.at[l, h, i])
            part = (up_in[l, h, i] if i < far else up_src[l, h, i]).astype(F32)
            side = cu_in[l, i] if i < far else cu_src[l, i]
            total = total + (part * scales[i] + shifts[i] * side[0:1])
            const = const + side
        mark("up_sum")
        own_at = pl.ds(pl.multiple_of(me * ff, ff), ff)
        bias = b1[l:l + 1, own_at].astype(F32)
        act_in[l, h, me] = jnp.maximum((total + const[1:2] + bias).astype(BF16), 0)
        for target in peers + [partner]:
            remote(act_in.at[l, h, me], act_in.at[l, h, me], send_sem.at[5], act_sem.at[l, h, me], {"row": target})

    def down(l, h):
        mark("act_wait")

        def term(j):
            return jnp.dot(act_in[l, h, j], w2[l, pl.ds(pl.multiple_of(j * ff, ff), ff), :], preferred_element_type=F32)

        part = term(me)
        await_recv(act_in.at[l, h, partner], act_sem.at[l, h, partner])
        part = part + term(partner)
        for j in arrivals:
            j = j + core
            await_recv(act_in.at[l, h, j], act_sem.at[l, h, j])
            remote(act_in.at[l, h, j], act_in.at[l, h, j], send_sem.at[5], act_sem.at[l, h, j], {"row": partner})
            part = part + term(j)
        mark("fwd_wait")
        for j in arrivals:
            j = j + 1 - core
            await_recv(act_in.at[l, h, j], act_sem.at[l, h, j])
            part = part + term(j)
        mark("down_mm")
        down_in[l, h, mine] = part.astype(BF16)
        col_send(down_in, down_sem, l, h)

    mark("side0")
    for i in range(4):
        await_recv(norms[i][1].at[1], pw_sem.at[0, 1 + n_chip + i])
    await_recv(w_in.at[0, cols:], pw_sem.at[0, 0])
    halves = range(HALVES)
    for l in range(layers):
        n = 2 * l
        for h in halves:
            qkv_go(l, h)
            if l == 0 and h == 0:
                qkv_side(0)
        if l == 0:
            share_up(0)
        for h in halves:
            qkv_recv(l, h)
            attend(l, h)
        mark("loads")
        if l + 1 < layers:
            loads["qkv", l + 1] = load_qkv(l + 1)
            load_cache(l + 1)
            loads["rest", l + 1] = load_rest(l + 1)
            share_up(l + 1)
        for copy in loads["rest", l]:
            copy.wait()
        for i in range(n_chip):
            await_recv(w1.at[l, i, cols:], pw_sem.at[l, 1 + i])
        up_side(l)
        for h in halves:
            project(l, h)
        if l + 1 < layers:
            mark("repack")
            for copy in loads["qkv", l + 1]:
                copy.wait()
            repack(l + 1)
            share_qkv(l + 1)
        for h in halves:
            state[n + 1, h] = col_recv(proj_in, proj_sem, l, h, bo[l:l + 1, :], state[n, h])
            swap_state(n + 1, h)
        for h in halves:
            up_go(l, h)
        if l + 1 < layers:
            mark("side")
            await_recv(w_in.at[l + 1, cols:], pw_sem.at[l + 1, 0])
            qkv_side(l + 1)
        for h in halves:
            up_recv(l, h)
        for h in halves:
            down(l, h)
        for h in halves:
            new_state = col_recv(down_in, down_sem, l, h, b2[l:l + 1, :], state[n + 1, h])
            if l + 1 < layers:
                state[n + 2, h] = new_state
                swap_state(n + 2, h)
            else:
                h_out[h * rows:(h + 1) * rows] = new_state
    mark("tail")
    for copy in pending:
        copy.wait_send()
    mark(None)


def store(*refs):
    copies = [pltpu.make_async_copy(refs[i], refs[3 + i], refs[6].at[i]) for i in range(3)]
    for copy in copies:
        copy.start()
    for copy in copies:
        copy.wait()


def solution(mesh):
    n_row = mesh.shape["row"]
    n_col = mesh.shape["col"]
    act_spec = P("dp", "row")
    cache_spec = P(None, "dp", ("col", "row"), None, None)
    fresh_spec = P(None, "dp", ("col", "row"), None)
    in_weight = P(None, "row", "col")
    out_weight = P(None, "col", "row")
    col_vec = P(None, "col")
    row_vec = P(None, "row")
    in_specs = (act_spec, P("dp"), cache_spec, cache_spec, row_vec, row_vec,
                in_weight, col_vec, in_weight, col_vec, in_weight, col_vec,
                out_weight, row_vec, row_vec, row_vec, in_weight, col_vec, out_weight, row_vec)

    def local_step(hidden, cache_len, k_cache, v_cache, *params):
        rows, cols = hidden.shape
        layers, _, _, s_max, head = k_cache.shape
        keys = jnp.swapaxes(k_cache, 3, 4).reshape(layers, rows, head, s_max)
        values = jnp.swapaxes(v_cache, 3, 4).reshape(layers, rows, head, s_max)
        operands = [hidden, cache_len.reshape(1, rows), keys, values, *params]
        operands[12] = params[8].reshape(layers, n_row, 2, head // 2, cols)
        dma = pltpu.SemaphoreType.DMA
        ff = params[12].shape[2]
        n_chip = n_row // 2
        ff_own = ff // n_row
        part = rows // HALVES
        shapes = [a.shape for a in operands]
        shapes = shapes[1:4] + [(2,) + s if i in (0, 1, 10, 11) else s for i, s in enumerate(shapes[4:])]
        shapes[11] = (layers, 2, n_row, head // 2, cols)
        shapes[15] = (layers, n_chip, 2 * cols, ff_own)
        vmem = [pltpu.VMEM(s, a.dtype) for s, a in zip(shapes, operands[1:])]
        scratch = vmem + [
            pltpu.VMEM((2 * layers, HALVES, part, cols), BF16),
            pltpu.VMEM((2 * layers, HALVES, part, cols), BF16),
            pltpu.VMEM((2 * layers, HALVES, 8, 128), F32),
            pltpu.VMEM((2 * layers, HALVES, n_chip - 1, 8, 128), F32),
            pltpu.VMEM((layers, n_chip, 8, 2 * head), F32),
            pltpu.VMEM((layers, n_chip - 1, 8, 2 * head), F32),
            pltpu.VMEM((layers, n_chip, 8, ff_own), F32),
            pltpu.VMEM((layers, n_chip - 1, 8, ff_own), F32),
            pltpu.VMEM((layers, 2 * cols, 3 * head * n_chip), BF16),
            pltpu.VMEM((layers, cols, 3 * head * n_chip), BF16),
            pltpu.VMEM((layers, HALVES, n_chip, part + part // 2, 2 * head), BF16),
            pltpu.VMEM((layers, HALVES, n_chip - 1, part + part // 2, 2 * head), BF16),
            pltpu.VMEM((layers, HALVES, n_row, head // 2, 2 * part), BF16),
            pltpu.VMEM((layers, HALVES, n_col, part, cols), BF16),
            pltpu.VMEM((layers, HALVES, n_chip, part, ff_own), BF16),
            pltpu.VMEM((layers, HALVES, n_chip - 1, part, ff_own), BF16),
            pltpu.VMEM((layers, HALVES, n_row, part, ff_own), BF16),
            pltpu.VMEM((layers, HALVES, n_col, part, cols), BF16),
            pltpu.VMEM((rows, 2 * head), BF16),
            pltpu.VMEM((16, 16 * head), BF16),
            pltpu.VMEM((rows, s_max), F32),
            pltpu.VMEM((HALVES, s_max, part), BF16),
            dma((1 + layers, 16)),
            dma((layers, 2, rows // 16)),
            dma((8,)),
            dma((layers, 5 + n_chip)),
            dma((2 * layers, HALVES)),
            dma((2 * layers, HALVES, n_chip - 1)),
            dma((layers, n_chip - 1)),
            dma((layers, n_chip - 1)),
            dma((layers, HALVES, n_chip - 1)),
            dma((layers, HALVES, n_row)),
            dma((layers, HALVES, n_col)),
            dma((layers, HALVES, n_chip - 1)),
            dma((layers, HALVES, n_row)),
            dma((layers, HALVES, n_col)),
        ]
        h, kt, vt = pl.pallas_call(
            functools.partial(kernel, n_row, n_col, cols * n_row),
            out_shape=(pltpu.VMEM((rows, cols), BF16),
                       pltpu.VMEM((layers, head, rows), BF16),
                       pltpu.VMEM((layers, head, rows), BF16)),
            in_specs=[pl.BlockSpec(memory_space=pltpu.HBM)] * len(operands),
            out_specs=[pl.BlockSpec(memory_space=pltpu.VMEM)] * 3,
            scratch_shapes=scratch,
            compiler_params=pltpu.CompilerParams(collective_id=0, has_side_effects=True,
                                                 vmem_limit_bytes=63 * 2 ** 20),
        )(*operands)
        h, kt, vt = pl.pallas_call(
            store,
            out_shape=(jax.ShapeDtypeStruct((rows, cols), BF16),
                       jax.ShapeDtypeStruct((layers, head, rows), BF16),
                       jax.ShapeDtypeStruct((layers, head, rows), BF16)),
            in_specs=[pl.BlockSpec(memory_space=pltpu.VMEM)] * 3,
            out_specs=[pl.BlockSpec(memory_space=pltpu.HBM)] * 3,
            scratch_shapes=[dma((3,))],
        )(*[pltpu.with_memory_space_constraint(a, pltpu.VMEM) for a in (h, kt, vt)])
        k_new = jnp.swapaxes(kt, 1, 2).reshape(layers, rows, 1, head)
        v_new = jnp.swapaxes(vt, 1, 2).reshape(layers, rows, 1, head)
        return h, k_new, v_new

    return jax.shard_map(local_step, mesh=mesh, in_specs=in_specs,
                         out_specs=(act_spec, fresh_spec, fresh_spec), check_vma=False)
```

```python
import functools

import jax
import jax.numpy as jnp
from jax import lax
from jax.experimental import pallas as pl
from jax.experimental.pallas import tpu as pltpu
from jax.sharding import PartitionSpec as P

EPS_LN = 1e-5
F32 = jnp.float32
BF16 = jnp.bfloat16
MESH = pl.DeviceIdType.MESH


class Marks:
    def __init__(self):
        self.open = None

    def __call__(self, name):
        if self.open is not None:
            self.open.__exit__(None, None, None)
        self.open = None
        if name:
            self.open = jax.named_scope(name)
            self.open.__enter__()


HALVES = 2
STAGES = {"go": (0.6, 3.6), "attend": (3.1, 3.4), "project": (0.3, 3.6), "up": (0.6, 3.8), "act": (0.3, 3.7), "down": (0.4, 3.6)}


def stage_order(layers, parts):
    names = list(STAGES)
    ready = {part: 0.0 for part in range(parts)}
    done = {part: 0 for part in range(parts)}
    now, order = 0.0, []
    while ready:
        part = min(ready, key=lambda p: (max(ready[p], now), -done[p], p))
        if done[part] == layers * len(names):
            order.append(("end", layers, part))
            del ready[part]
            continue
        layer, name = divmod(done[part], len(names))
        cost, delay = STAGES[names[name]]
        now = max(now, ready[part]) + cost
        order.append((names[name], layer, part))
        done[part] += 1
        ready[part] = now + delay
    return order


def kernel(n_row, n_col, width,
           x_hbm, len_hbm, k_hbm, v_hbm, ln1g_hbm, ln1b_hbm, wq_hbm, bq_hbm, wk_hbm, bk_hbm, wv_hbm, bv_hbm,
           wo_hbm, bo_hbm, ln2g_hbm, ln2b_hbm, w1_hbm, b1_hbm, w2_hbm, b2_hbm,
           h_out, k_out, v_out,
           x_buf, len_buf, k_buf, v_buf, ln1g, ln1b, wq, bq, wk, bk, wv, bv, wo, bo, ln2g, ln2b, w1, b1, w2, b2,
           state, stat_src, stat_in, cq_src, cq_in, cu_src, cu_in, bias_own,
           qkv_src, qkv_in, att_src, att_in, proj_in, up_src, up_in, act_src, act_in, down_in, h_src, h_in, mid_in,
           twin, onehot, scores, probs_t,
           in_sem, kv_sem, send_sem, pw_sem, pair_sem, stat_sem, cq_sem, cu_sem,
           qkv_sem, att_sem, proj_sem, up_sem, act_sem, down_sem, h_sem, qw_sem):
    mark = Marks()
    mark("entry")
    layers = wo.shape[0]
    batch, cols = x_buf.shape
    rows = batch // HALVES
    sub = rows // 2
    head = k_buf.shape[2]
    s_max = k_buf.shape[3]
    lanes = 2 * head
    n_chip = n_row // 2
    near = 2 * cols
    ff = w1.shape[2] // n_row
    packs = 128 // sub
    thin = head // packs
    me = lax.axis_index("row")
    mine = lax.axis_index("col")
    chip = me // 2
    core = lax.rem(me, 2)
    partner = chip * 2 + (1 - core)
    flip = mine // 2
    side = lax.rem(core + flip, 2)
    hops = [2, 1, 3]
    far = len(hops)
    chips = [lax.rem(chip + dc, n_chip) for dc in hops] + [chip]
    mates = [c * 2 + core for c in chips[:far]]
    own_at = pl.ds(pl.multiple_of(core * cols, cols), cols)
    pending = []

    def local(src, dst, sem):
        copy = pltpu.make_async_copy(src, dst, sem)
        copy.start()
        return copy

    def remote(src, dst, ssem, rsem, target):
        copy = pltpu.make_async_remote_copy(src_ref=src, dst_ref=dst, send_sem=ssem, recv_sem=rsem,
                                            device_id=target, device_id_type=MESH)
        copy.start()
        pending.append(copy)

    def await_recv(dst, sem):
        pltpu.make_async_remote_copy(src_ref=dst, dst_ref=dst, send_sem=sem, recv_sem=sem,
                                     device_id={"row": me}, device_id_type=MESH).wait_recv()

    def everyone():
        for i in range(far):
            for e in (0, 1):
                yield i, e, chips[i] * 2 + lax.rem(e + flip, 2)
        yield far, 1 - side, partner

    def senders():
        for i in range(far):
            for e in (0, 1):
                yield i, e
        yield far, 1 - side

    def col_peer(k, half):
        y = lax.rem(mine + k, n_col)
        return {"row": chip * 2 + lax.rem(half + y // 2, 2), "col": y}

    def cache_copy(l, which, t):
        src, dst = ((k_hbm, k_buf), (v_hbm, v_buf))[which]
        return pltpu.make_async_copy(src.at[l, pl.ds(16 * t, 16)], dst.at[l, pl.ds(16 * t, 16)], kv_sem.at[l, which, t])

    shared = [(ln1g_hbm, ln1g), (ln1b_hbm, ln1b), (ln2g_hbm, ln2g), (ln2b_hbm, ln2b), (bo_hbm, bo), (b2_hbm, b2)]
    smalls = ([(x_hbm, x_buf), (len_hbm, len_buf), (bq_hbm, bq), (bk_hbm, bk), (bv_hbm, bv), (b1_hbm, b1)]
              + [(src, dst.at[core]) for src, dst in shared])
    small_copies = [local(src, dst, in_sem.at[0, i]) for i, (src, dst) in enumerate(smalls)]
    qkv_weights = [(wq_hbm, wq), (wk_hbm, wk), (wv_hbm, wv)]

    def load_qkv(l):
        return [local(src.at[l], dst.at[l, own_at], in_sem.at[1 + l, i]) for i, (src, dst) in enumerate(qkv_weights)]

    loads = {("qkv", 0): load_qkv(0)}
    barrier = pltpu.get_barrier_semaphore()
    for k in range(1, n_row):
        pl.semaphore_signal(barrier, inc=1, device_id={"row": lax.rem(me + k, n_row)}, device_id_type=MESH)
    for k in range(1, n_col):
        for e in (0, 1):
            pl.semaphore_signal(barrier, inc=1, device_id=col_peer(k, e), device_id_type=MESH)

    def rest_of(l):
        return ([(wo_hbm.at[l, :, i], wo.at[l, i, :, :, own_at]) for i in range(packs)]
                + [(w1_hbm.at[l], w1.at[l, own_at]), (w2_hbm.at[l], w2.at[l, :, own_at])])

    def load_rest(l):
        return [local(src, dst, in_sem.at[1 + l, 3 + i]) for i, (src, dst) in enumerate(rest_of(l))]

    def tile_at(i):
        return pl.ds(pl.multiple_of(chips[i] * lanes, lanes), lanes)

    def share_qkv(l):
        for i in range(n_chip):
            for t, (_, dst) in enumerate(qkv_weights):
                tile = dst.at[l, own_at, tile_at(i)]
                remote(tile, tile, send_sem.at[6], qw_sem.at[l, i, t], {"row": partner})

    def await_qkv(l, i):
        for t, (_, dst) in enumerate(qkv_weights):
            await_recv(dst.at[l, own_at, tile_at(i)], qw_sem.at[l, i, t])

    def share_rest(l, which):
        for i, (src, dst) in enumerate(rest_of(l)):
            if i in which:
                remote(src, dst, send_sem.at[7], pw_sem.at[l, 3 + i], {"row": partner})

    def await_rest(l, which):
        for i, (src, dst) in enumerate(rest_of(l)):
            if i in which:
                loads["rest", l][i].wait()
                await_recv(dst, pw_sem.at[l, 3 + i])

    ONLY_WO, ONLY_W1, ONLY_W2 = range(packs), (packs,), (packs + 1,)

    def load_cache(l):
        for which in range(2):
            for t in range(batch // 16):
                cache_copy(l, which, t).start()

    low = lax.broadcasted_iota(jnp.int32, (rows, lanes), 1) < head
    lane_id = lax.broadcasted_iota(jnp.int32, (16, 16 * head), 1)
    row_id = lax.broadcasted_iota(jnp.int32, (16, 16 * head), 0)
    onehot[...] = jnp.where(lane_id // head == row_id, 1.0, 0.0).astype(BF16)
    for copy in small_copies:
        copy.wait()

    def own_head(vec_ref, l):
        total = jnp.zeros((1, head), F32)
        for j in range(n_row):
            total = total + jnp.where(me == j, vec_ref[l:l + 1, j * head:(j + 1) * head].astype(F32), 0.0)
        return total

    zero = jnp.zeros((1, lanes), F32)
    for l in range(layers):
        vb = own_head(bv, l)
        bias_own[l] = jnp.concatenate([zero, jnp.concatenate([own_head(bq, l), own_head(bk, l)], axis=1), zero,
                                       jnp.concatenate([vb, vb], axis=1)] + [zero] * 4, axis=0)
    len_all = jnp.transpose(jnp.broadcast_to(len_buf[...], (batch, batch)))
    for h in range(HALVES):
        state[0, h, :, own_at] = x_buf[pl.ds(pl.multiple_of(h * rows + side * sub, sub), sub)]
    mark("load0")
    for copy in loads["qkv", 0]:
        copy.wait()
    load_cache(0)
    loads["rest", 0] = load_rest(0)
    for l in range(1, layers):
        loads["qkv", l] = load_qkv(l)
    mark("barrier")
    pl.semaphore_wait(barrier, n_row + 2 * n_col - 3)
    mark("entry2")
    for h in range(HALVES):
        there = pl.ds(pl.multiple_of(h * rows + (1 - side) * sub, sub), sub)
        remote(x_buf.at[there], state.at[0, h, :, own_at], send_sem.at[0], pair_sem.at[0, h], {"row": partner})
    for i, (src, dst) in enumerate(shared):
        remote(dst.at[core], dst.at[core], send_sem.at[6], pair_sem.at[1, i], {"row": partner})
    share_qkv(0)

    def full_row(ref, l):
        return jnp.concatenate([ref[0, l:l + 1], ref[1, l:l + 1]], axis=1).astype(F32)

    def side_operand(gain, shift, l):
        at = lax.broadcasted_iota(jnp.int32, (16, near), 0)
        return jnp.where(at == 0, full_row(gain, l), jnp.where(at == 1, full_row(shift, l), 0.0)).astype(BF16)

    def chip_tile(w, l, i):
        return w[l, :, tile_at(i)]

    def qkv_side(l):
        lhs = side_operand(ln1g, ln1b, l)
        for i in range(n_chip):
            q, k, v = [jnp.dot(lhs, chip_tile(w, l, i), preferred_element_type=F32)[0:8] for w in (wq, wk, wv)]
            q_r, k_r, v_r = [pltpu.roll(a, head, axis=1) for a in (q, k, v)]
            low8 = low[0:8]
            qk = jnp.where(core == 0, jnp.where(low8, q, k_r), jnp.where(low8, q_r, k))
            vs = jnp.where(core == 0, jnp.where(low8, v, v_r), jnp.where(low8, v_r, v))
            at = lax.broadcasted_iota(jnp.int32, (8, lanes), 0)
            cq_src[l, i] = jnp.where(at < 2, qk, pltpu.roll(vs, 2, axis=0))
        for i in range(far):
            remote(cq_src.at[l, i], cq_in.at[l, i], send_sem.at[1], cq_sem.at[l, i], {"row": mates[i]})

    def up_side(l):
        lhs = side_operand(ln2g, ln2b, l)
        for i in range(n_chip):
            at = pl.ds(pl.multiple_of((chips[i] * 2 + core) * ff, ff), ff)
            cu_src[l, i] = jnp.dot(lhs, w1[l, :, at], preferred_element_type=F32)[0:8]
        for i in range(far):
            remote(cu_src.at[l, i], cu_in.at[l, i], send_sem.at[1], cu_sem.at[l, i], {"row": mates[i]})

    def normalize(n, h, gain, l):
        mark("norm")
        x = state[n, h].astype(F32)
        s1 = jnp.sum(x, axis=1, keepdims=True)
        s2 = jnp.sum(x * x, axis=1, keepdims=True)
        mean = s1 / near
        inv = lax.rsqrt(jnp.maximum(s2 / near - mean * mean, 0.0) + EPS_LN)
        z = ((x - mean) * inv * full_row(gain, l)).astype(BF16)
        lane = lax.broadcasted_iota(jnp.int32, (sub, 128), 1)
        both = jnp.where(lane == 0, s1, jnp.where(lane == 1, s2, 0.0))
        both = jnp.concatenate([both, jnp.zeros((128 - sub, 128), F32)], axis=0)
        mine_stat = jnp.transpose(both)[0:2]
        stat_src[n, h] = mine_stat
        stat_in[n, h, far, side] = mine_stat
        return z

    def send_stats(n, h):
        for i, e, target in everyone():
            remote(stat_src.at[n, h], stat_in.at[n, h, i, side], send_sem.at[1], stat_sem.at[n, h, i, side], {"row": target})

    def stat_columns(n, h):
        for i, e in senders():
            await_recv(stat_in.at[n, h, i, e], stat_sem.at[n, h, i, e])
        table = []
        for e in (0, 1):
            parts = [stat_in[n, h, i, e] for i in range(n_chip)]
            total = parts[0]
            for part in parts[1:]:
                total = total + part
            mean = total[0:1] / width
            inv = lax.rsqrt(total[1:2] / width - mean * mean + EPS_LN)
            shifts = []
            for part in parts:
                near_mean = part[0:1] / near
                near_var = jnp.maximum(part[1:2] / near - near_mean * near_mean, 0.0) + EPS_LN
                table.append(inv * (near_var * lax.rsqrt(near_var)))
                shifts.append(inv * (near_mean - mean))
            table.extend(shifts)
        columns = jnp.concatenate(table + [jnp.zeros((128 - 4 * n_chip, 128), F32)], axis=0)
        columns = jnp.transpose(columns)[0:sub]

        def pick(start):
            return [[columns[:, e * 2 * n_chip + start + i:e * 2 * n_chip + start + i + 1] for i in range(n_chip)] for e in (0, 1)]

        return pick(0), pick(n_chip)

    def fold(column):
        return jnp.where(low[0:sub // 2], column[0:sub // 2], column[sub // 2:])

    def send_blocks(src, dst, sem, l, h, first, last):
        for i in range(first, last):
            for c in (0, 1) if i < far else (1 - core,):
                remote(src.at[l, h, i, c], dst.at[l, h, i, side], send_sem.at[2], sem.at[l, h, i, side],
                       {"row": chips[i] * 2 + c})
        if last == n_chip:
            dst[l, h, far, side] = src[l, h, far, core]

    fresh = {}

    def qkv_go(l, h):
        n = 2 * l
        z = normalize(n, h, ln1g, l)
        mark("qkv_mm")
        for i in range(n_chip):
            if l == 0 and h == 0:
                await_qkv(0, i)
            q, k, v = [jnp.dot(z, chip_tile(w, l, i), preferred_element_type=F32) for w in (wq, wk, wv)]
            q_r, k_r, v_r = [pltpu.roll(a, head, axis=1) for a in (q, k, v)]
            low_s, low_h = low[0:sub], low[0:sub // 2]
            qkv_src[l, h, i, 0, 0:sub] = jnp.where(low_s, q, k_r).astype(BF16)
            qkv_src[l, h, i, 1, 0:sub] = jnp.where(low_s, q_r, k).astype(BF16)
            qkv_src[l, h, i, 0, sub:] = jnp.where(low_h, v[:sub // 2], v_r[sub // 2:]).astype(BF16)
            qkv_src[l, h, i, 1, sub:] = jnp.where(low_h, v_r[:sub // 2], v[sub // 2:]).astype(BF16)
            if i == 0:
                send_blocks(qkv_src, qkv_in, qkv_sem, l, h, 0, 1)
                send_stats(n, h)
        send_blocks(qkv_src, qkv_in, qkv_sem, l, h, 1, n_chip)

    def qkv_recv(l, h):
        mark("qkv_wait")
        if h == 0:
            const = bias_own[l] + cq_src[l, far]
            cq_in[l, far] = cq_src[l, far]
            for i in range(far):
                await_recv(cq_in.at[l, i], cq_sem.at[l, i])
                const = const + cq_in[l, i]
            bias_own[l] = const
        scales, shifts = stat_columns(2 * l, h)
        qk, vv = [], []
        for e in (0, 1):
            a = jnp.broadcast_to(bias_own[l, 1:2], (sub, lanes))
            b = jnp.broadcast_to(bias_own[l, 3:4], (sub // 2, lanes))
            for i in range(n_chip):
                a = a + shifts[e][i] * cq_in[l, i, 0:1]
                b = b + fold(shifts[e][i]) * cq_in[l, i, 2:3]
            qk.append(a)
            vv.append(b)
        for i, e in senders():
            await_recv(qkv_in.at[l, h, i, e], qkv_sem.at[l, h, i, e])
        mark("qkv_sum")
        for e in (0, 1):
            for i in range(n_chip):
                qk[e] = qk[e] + qkv_in[l, h, i, e, 0:sub].astype(F32) * scales[e][i]
                vv[e] = vv[e] + qkv_in[l, h, i, e, sub:].astype(F32) * fold(scales[e][i])
        qk = jnp.concatenate(qk, axis=0)
        q_b = (qk[:, 0:head] * (head ** -0.5)).astype(BF16)
        k_new = pltpu.roll(qk, head, axis=1)[:, 0:head].astype(BF16)
        v_new = jnp.concatenate([piece for b in vv for piece in (b[:, 0:head], pltpu.roll(b, head, axis=1)[:, 0:head])],
                                axis=0).astype(BF16)
        q_f = q_b.astype(F32)
        k_f = k_new.astype(F32)
        twin[h * rows:(h + 1) * rows, :] = jnp.concatenate([q_f, q_f], axis=1).astype(BF16)
        fresh[l, h] = (jnp.sum(q_f * k_f, axis=1, keepdims=True), k_f, v_new.astype(F32))

    def attend(l, h):
        score_new, k_f, v_f = fresh[l, h]
        base = h * rows
        mine_rows = slice(base, base + rows)
        mark("scores")
        for t in range(rows // 16):
            cache_copy(l, 0, base // 16 + t).wait()
        for t in range(rows // 16):
            at = slice(base + 16 * t, base + 16 * (t + 1))
            q_diag = jnp.concatenate([twin[at, :]] * (16 * head // lanes), axis=1) * onehot[...]
            keys = k_buf[l, at].reshape(16 * head, s_max)
            scores[at, :] = jnp.dot(q_diag, keys, preferred_element_type=F32)
        mark("softmax")
        sc = scores[mine_rows, :]
        position = lax.broadcasted_iota(jnp.int32, sc.shape, 1)
        sc = jnp.where(position < len_all[mine_rows, 0:1], sc, -jnp.inf)
        peak = jnp.maximum(jnp.max(sc, axis=1, keepdims=True), score_new)
        ex = jnp.exp(sc - peak)
        ex_new = jnp.exp(score_new - peak)
        mass = jnp.sum(ex, axis=1, keepdims=True) + ex_new
        scores[mine_rows, :] = ex / mass
        prob_new = (ex_new / mass).astype(BF16).astype(F32)
        for b in range(s_max // 128):
            probs_t[h, b * 128:(b + 1) * 128, :] = jnp.transpose(scores[mine_rows, b * 128:(b + 1) * 128]).astype(BF16)
        prob_row = jnp.transpose(jnp.broadcast_to(prob_new, (rows, 128)))[0:1, :]
        lane = lax.broadcasted_iota(jnp.int32, (head, rows), 1)
        mark("mix")

        def mix_step(t, acc):
            for u in range(2):
                cache_copy(l, 1, base // 16 + 2 * t + u).wait()
            values = v_buf[l, pl.ds(base + 32 * t, 32)].reshape(32 * head, s_max)
            full = jnp.dot(values, probs_t[h], preferred_element_type=F32)
            for i in range(32):
                acc = jnp.where(lane == 32 * t + i, full[i * head:(i + 1) * head], acc)
            return acc

        mixed = lax.fori_loop(0, rows // 32, mix_step, jnp.zeros((head, rows), F32))
        mark("att_send")
        v_t = jnp.transpose(v_f)
        mixed = mixed + prob_row * v_t
        for e in (0, 1):
            att_src[l, h, e] = jnp.concatenate(
                [mixed[i * thin:(i + 1) * thin, e * sub:(e + 1) * sub] for i in range(packs)], axis=1).astype(BF16)
        for i, e, target in everyone():
            remote(att_src.at[l, h, e], att_in.at[l, h, me], send_sem.at[3], att_sem.at[l, h, me], {"row": target})
        att_in[l, h, me] = att_src[l, h, side]
        fresh[l, h] = (k_f, v_t)

    def keep_fresh(l, h):
        k_f, v_t = fresh[l, h]
        k_out[l, :, h * rows:(h + 1) * rows] = jnp.transpose(k_f).astype(BF16)
        v_out[l, :, h * rows:(h + 1) * rows] = v_t.astype(BF16)

    def col_send(buf, sem, l, h):
        mark("col_send")
        for k in (2, 1, 3):
            remote(buf.at[l, h, mine], buf.at[l, h, mine], send_sem.at[4], sem.at[l, h, mine], col_peer(k, side))

    def col_recv(buf, sem, l, h, bias, base):
        mark("col_wait")
        for k in range(1, n_col):
            j = lax.rem(mine + k, n_col)
            await_recv(buf.at[l, h, j], sem.at[l, h, j])
        mark("col_sum")
        summed = buf[l, h, 0].astype(F32)
        for j in range(1, n_col):
            summed = summed + buf[l, h, j].astype(F32)
        return (base.astype(F32) + (summed + full_row(bias, l))).astype(BF16)

    def project(l, h):
        mark("att_wait")
        for k in range(1, n_row):
            j = lax.rem(me + k, n_row)
            await_recv(att_in.at[l, h, j], att_sem.at[l, h, j])
        mark("wo_mm")
        gathered = att_in[l, h].reshape(n_row * thin, 128)
        total = jnp.zeros((sub, near), F32)
        for i in range(packs):
            total = total + lax.dot_general(gathered, wo[l, i].reshape(n_row * thin, near), (((0,), (0,)), ((), ())),
                                            preferred_element_type=F32)[i * sub:(i + 1) * sub]
        proj_in[l, h, mine] = total.astype(BF16)
        col_send(proj_in, proj_sem, l, h)

    def up_go(l, h):
        n = 2 * l + 1
        z = normalize(n, h, ln2g, l)
        mark("up_mm")
        for i in range(n_chip):
            at = pl.ds(pl.multiple_of(chips[i] * 2 * ff, 2 * ff), 2 * ff)
            full = jnp.dot(z, w1[l, :, at], preferred_element_type=F32).astype(BF16)
            for c in (0, 1):
                up_src[l, h, i, c] = full[:, c * ff:(c + 1) * ff]
            if i == 0:
                send_blocks(up_src, up_in, up_sem, l, h, 0, 1)
                send_stats(n, h)
        send_blocks(up_src, up_in, up_sem, l, h, 1, n_chip)

    def up_recv(l, h):
        mark("up_wait")
        if h == 0:
            const = b1[l:l + 1, pl.ds(pl.multiple_of(me * ff, ff), ff)].astype(F32) + cu_src[l, far, 1:2]
            cu_in[l, far] = cu_src[l, far]
            for i in range(far):
                await_recv(cu_in.at[l, i], cu_sem.at[l, i])
                const = const + cu_in[l, i, 1:2]
            cu_in[l, far, 1:2] = const
        scales, shifts = stat_columns(2 * l + 1, h)
        totals = []
        for e in (0, 1):
            total = jnp.broadcast_to(cu_in[l, far, 1:2], (sub, ff))
            for i in range(n_chip):
                total = total + shifts[e][i] * cu_in[l, i, 0:1]
            totals.append(total)
        for i, e in senders():
            await_recv(up_in.at[l, h, i, e], up_sem.at[l, h, i, e])
        mark("up_sum")
        for e in (0, 1):
            for i in range(n_chip):
                totals[e] = totals[e] + up_in[l, h, i, e].astype(F32) * scales[e][i]
            act_src[l, h, e] = jnp.maximum(totals[e].astype(BF16), 0)
        for i, e, target in everyone():
            remote(act_src.at[l, h, e], act_in.at[l, h, me], send_sem.at[5], act_sem.at[l, h, me], {"row": target})
        act_in[l, h, me] = act_src[l, h, side]

    def down(l, h):
        mark("act_wait")
        for k in range(1, n_row):
            j = lax.rem(me + k, n_row)
            await_recv(act_in.at[l, h, j], act_sem.at[l, h, j])
        mark("down_mm")
        both = jnp.concatenate([act_in[l, h, j] for j in range(n_row)], axis=1)
        part = jnp.dot(both, w2[l], preferred_element_type=F32).astype(BF16)
        if l + 1 < layers:
            down_in[l, h, mine] = part
            col_send(down_in, down_sem, l, h)
            return
        mark("col_send")
        for c in (0, 1):
            h_src[h, c] = part[:, c * cols:(c + 1) * cols]
        for k in (2, 1, 3):
            for c in (0, 1):
                remote(h_src.at[h, c], h_in.at[h, mine, side], send_sem.at[4], h_sem.at[h, mine, side],
                       {"row": chip * 2 + c, "col": lax.rem(mine + k, n_col)})
        remote(h_src.at[h, 1 - core], h_in.at[h, mine, side], send_sem.at[4], h_sem.at[h, mine, side], {"row": partner})
        h_in[h, mine, side] = h_src[h, core]

    def finish(h):
        mark("col_wait")
        await_recv(mid_in.at[h], pair_sem.at[2, h])
        for k in range(1, n_col):
            for e in (0, 1):
                j = lax.rem(mine + k, n_col)
                await_recv(h_in.at[h, j, e], h_sem.at[h, j, e])
        await_recv(h_in.at[h, mine, 1 - side], h_sem.at[h, mine, 1 - side])
        mark("last")
        bias = b2[core, layers - 1:layers].astype(F32)
        for e in (0, 1):
            summed = h_in[h, 0, e].astype(F32)
            for j in range(1, n_col):
                summed = summed + h_in[h, j, e].astype(F32)
            base = jnp.where(side == e, state[2 * layers - 1, h, :, own_at].astype(F32), mid_in[h].astype(F32))
            at = h * rows + e * sub
            h_out[at:at + sub] = (base + (summed + bias)).astype(BF16)

    mark("side0")
    for h in range(HALVES):
        await_recv(state.at[0, h, :, own_at], pair_sem.at[0, h])
    for i, (src, dst) in enumerate(shared):
        await_recv(dst.at[core], pair_sem.at[1, i])
    last = HALVES - 1
    for stage, l, h in stage_order(layers, HALVES):
        n = 2 * l
        if l > 0 and stage == "go":
            new_state = col_recv(down_in, down_sem, l - 1, h, b2, state[n - 1, h])
        if stage == "go":
            if l > 0:
                state[n, h] = new_state
            qkv_go(l, h)
            mark("side")
            if l == 0 and h == 0:
                qkv_side(0)
            if l == 0 and h == last:
                share_rest(0, range(packs + 2))
            if l > 0 and h == 0:
                await_rest(l, ONLY_W1)
                up_side(l)
        elif stage == "attend":
            qkv_recv(l, h)
            attend(l, h)
            if l + 1 < layers and h == 0:
                mark("side")
                for copy in loads["qkv", l + 1]:
                    copy.wait()
                share_qkv(l + 1)
                load_cache(l + 1)
                loads["rest", l + 1] = load_rest(l + 1)
                share_rest(l + 1, range(packs + 1))
            if l + 1 < layers and h == last:
                share_rest(l + 1, ONLY_W2)
        elif stage == "project":
            if h == 0:
                await_rest(l, ONLY_WO)
            project(l, h)
            mark("side")
            if h == 0 and l == 0:
                await_rest(l, ONLY_W1)
                up_side(l)
            keep_fresh(l, h)
        elif stage == "up":
            state[n + 1, h] = col_recv(proj_in, proj_sem, l, h, bo, state[n, h])
            up_go(l, h)
            if l + 1 == layers:
                there = pl.ds(pl.multiple_of((1 - core) * cols, cols), cols)
                remote(state.at[n + 1, h, :, there], mid_in.at[h], send_sem.at[0], pair_sem.at[2, h], {"row": partner})
            if h == 0 and l + 1 < layers:
                mark("side")
                for i in range(n_chip):
                    await_qkv(l + 1, i)
                qkv_side(l + 1)
        elif stage == "act":
            up_recv(l, h)
        elif stage == "down":
            if h == 0:
                await_rest(l, ONLY_W2)
            down(l, h)
        else:
            finish(h)
    mark("tail")
    for copy in pending:
        copy.wait_send()
    mark(None)


def store(*refs):
    copies = [pltpu.make_async_copy(refs[i], refs[3 + i], refs[6].at[i]) for i in range(3)]
    for copy in copies:
        copy.start()
    for copy in copies:
        copy.wait()


def solution(mesh):
    n_row = mesh.shape["row"]
    n_col = mesh.shape["col"]
    act_spec = P("dp", "row")
    cache_spec = P(None, "dp", ("col", "row"), None, None)
    fresh_spec = P(None, "dp", ("col", "row"), None)
    in_weight = P(None, "row", "col")
    out_weight = P(None, "col", "row")
    col_vec = P(None, "col")
    row_vec = P(None, "row")
    in_specs = (act_spec, P("dp"), cache_spec, cache_spec, row_vec, row_vec,
                in_weight, col_vec, in_weight, col_vec, in_weight, col_vec,
                out_weight, row_vec, row_vec, row_vec, in_weight, col_vec, out_weight, row_vec)

    def local_step(hidden, cache_len, k_cache, v_cache, *params):
        rows, cols = hidden.shape
        layers, _, _, s_max, head = k_cache.shape
        keys = jnp.swapaxes(k_cache, 3, 4).reshape(layers, rows, head, s_max)
        values = jnp.swapaxes(v_cache, 3, 4).reshape(layers, rows, head, s_max)
        operands = [hidden, cache_len.reshape(1, rows), keys, values, *params]
        packs = 256 * HALVES // rows
        operands[12] = params[8].reshape(layers, n_row, packs, head // packs, cols)
        dma = pltpu.SemaphoreType.DMA
        ff = params[12].shape[2]
        n_chip = n_row // 2
        ff_own = ff // n_row
        near = 2 * cols
        sub = rows // HALVES // 2
        shapes = [(2,) + a.shape if i in (4, 5, 13, 14, 15, 19) else a.shape for i, a in enumerate(operands)]
        for i in (6, 8, 10, 16):
            shapes[i] = (layers, near, shapes[i][2])
        shapes[12] = (layers, packs, n_row, head // packs, near)
        shapes[18] = (layers, ff, near)
        vmem = [pltpu.VMEM(s, a.dtype) for s, a in zip(shapes, operands)]
        block = sub + sub // 2
        scratch = vmem + [
            pltpu.VMEM((2 * layers, HALVES, sub, near), BF16),
            pltpu.VMEM((2 * layers, HALVES, 2, 128), F32),
            pltpu.VMEM((2 * layers, HALVES, n_chip, 2, 2, 128), F32),
            pltpu.VMEM((layers, n_chip, 8, 2 * head), F32),
            pltpu.VMEM((layers, n_chip, 8, 2 * head), F32),
            pltpu.VMEM((layers, n_chip, 8, ff_own), F32),
            pltpu.VMEM((layers, n_chip, 8, ff_own), F32),
            pltpu.VMEM((layers, 8, 2 * head), F32),
            pltpu.VMEM((layers, HALVES, n_chip, 2, block, 2 * head), BF16),
            pltpu.VMEM((layers, HALVES, n_chip, 2, block, 2 * head), BF16),
            pltpu.VMEM((layers, HALVES, 2, head // packs, 128), BF16),
            pltpu.VMEM((layers, HALVES, n_row, head // packs, 128), BF16),
            pltpu.VMEM((layers, HALVES, n_col, sub, near), BF16),
            pltpu.VMEM((layers, HALVES, n_chip, 2, sub, ff_own), BF16),
            pltpu.VMEM((layers, HALVES, n_chip, 2, sub, ff_own), BF16),
            pltpu.VMEM((layers, HALVES, 2, sub, ff_own), BF16),
            pltpu.VMEM((layers, HALVES, n_row, sub, ff_own), BF16),
            pltpu.VMEM((layers, HALVES, n_col, sub, near), BF16),
            pltpu.VMEM((HALVES, 2, sub, cols), BF16),
            pltpu.VMEM((HALVES, n_col, 2, sub, cols), BF16),
            pltpu.VMEM((HALVES, sub, cols), BF16),
            pltpu.VMEM((rows, 2 * head), BF16),
            pltpu.VMEM((16, 16 * head), BF16),
            pltpu.VMEM((rows, s_max), F32),
            pltpu.VMEM((HALVES, s_max, rows // HALVES), BF16),
            dma((1 + layers, 16)),
            dma((layers, 2, rows // 16)),
            dma((9,)),
            dma((layers, 5 + packs)),
            dma((3, 8)),
            dma((2 * layers, HALVES, n_chip, 2)),
            dma((layers, n_chip)),
            dma((layers, n_chip)),
            dma((layers, HALVES, n_chip, 2)),
            dma((layers, HALVES, n_row)),
            dma((layers, HALVES, n_col)),
            dma((layers, HALVES, n_chip, 2)),
            dma((layers, HALVES, n_row)),
            dma((layers, HALVES, n_col)),
            dma((HALVES, n_col, 2)),
            dma((layers, n_chip, 3)),
        ]
        h, kt, vt = pl.pallas_call(
            functools.partial(kernel, n_row, n_col, cols * n_row),
            out_shape=(pltpu.VMEM((rows, cols), BF16),
                       pltpu.VMEM((layers, head, rows), BF16),
                       pltpu.VMEM((layers, head, rows), BF16)),
            in_specs=[pl.BlockSpec(memory_space=pltpu.HBM)] * len(operands),
            out_specs=[pl.BlockSpec(memory_space=pltpu.VMEM)] * 3,
            scratch_shapes=scratch,
            compiler_params=pltpu.CompilerParams(collective_id=0, has_side_effects=True,
                                                 vmem_limit_bytes=63 * 2 ** 20),
        )(*operands)
        h, kt, vt = pl.pallas_call(
            store,
            out_shape=(jax.ShapeDtypeStruct((rows, cols), BF16),
                       jax.ShapeDtypeStruct((layers, head, rows), BF16),
                       jax.ShapeDtypeStruct((layers, head, rows), BF16)),
            in_specs=[pl.BlockSpec(memory_space=pltpu.VMEM)] * 3,
            out_specs=[pl.BlockSpec(memory_space=pltpu.HBM)] * 3,
            scratch_shapes=[dma((3,))],
        )(*[pltpu.with_memory_space_constraint(a, pltpu.VMEM) for a in (h, kt, vt)])
        k_new = jnp.swapaxes(kt, 1, 2).reshape(layers, rows, 1, head)
        v_new = jnp.swapaxes(vt, 1, 2).reshape(layers, rows, 1, head)
        return h, k_new, v_new

    return jax.shard_map(local_step, mesh=mesh, in_specs=in_specs,
                         out_specs=(act_spec, fresh_spec, fresh_spec), check_vma=False)
```

```python
import functools

import jax
import jax.numpy as jnp
from jax import lax
from jax.experimental import pallas as pl
from jax.experimental.pallas import tpu as pltpu
from jax.sharding import PartitionSpec as P

EPS_LN = 1e-5
F32 = jnp.float32
BF16 = jnp.bfloat16
LOGICAL = pl.DeviceIdType.LOGICAL


class Marks:
    def __init__(self):
        self.open = None

    def __call__(self, name):
        if self.open is not None:
            self.open.__exit__(None, None, None)
        self.open = None
        if name:
            self.open = jax.named_scope(name)
            self.open.__enter__()


HALVES = 2
ON_VPU = 20
STAGES = {"go": (0.6, 3.6), "attend": (3.1, 3.4), "project": (0.3, 3.6), "up": (0.6, 3.8), "act": (0.3, 3.7), "down": (0.4, 3.6)}


def stage_order(layers, parts):
    names = list(STAGES)
    ready = {part: 0.0 for part in range(parts)}
    done = {part: 0 for part in range(parts)}
    now, order = 0.0, []
    while ready:
        part = min(ready, key=lambda p: (max(ready[p], now), -done[p], p))
        if done[part] == layers * len(names):
            order.append(("end", layers, part))
            del ready[part]
            continue
        layer, name = divmod(done[part], len(names))
        cost, delay = STAGES[names[name]]
        now = max(now, ready[part]) + cost
        order.append((names[name], layer, part))
        done[part] += 1
        ready[part] = now + delay
    return order


def kernel(n_row, n_col, width,
           x_hbm, len_hbm, k_hbm, v_hbm, ln1g_hbm, ln1b_hbm, wq_hbm, bq_hbm, wk_hbm, bk_hbm, wv_hbm, bv_hbm,
           wo_hbm, bo_hbm, ln2g_hbm, ln2b_hbm, w1_hbm, b1_hbm, w2_hbm, b2_hbm,
           h_out, k_out, v_out,
           x_buf, len_buf, k_buf, v_buf, ln1g, ln1b, wqkv, bq, bk, bv, wo, bo, ln2g, ln2b, w1, b1, w2, b2,
           state, stat_src, stat_in, cq_src, cq_in, cu_src, cu_in, bias_own,
           qkv_src, qkv_in, att_src, att_in, proj_in, up_src, up_in, act_src, act_in, down_in, h_src, h_in, mid_in,
           twin, onehot, scores, probs_t,
           in_sem, kv_sem, send_sem, pw_sem, pair_sem, stat_sem, cq_sem, cu_sem,
           qkv_sem, att_sem, proj_sem, up_sem, act_sem, down_sem, h_sem, qw_sem):
    mark = Marks()
    mark("entry")
    layers = wo.shape[0]
    batch, cols = x_buf.shape
    rows = batch // HALVES
    sub = rows // 2
    head = k_buf.shape[2]
    s_max = k_buf.shape[3]
    lanes = 2 * head
    n_chip = n_row // 2
    near = 2 * cols
    ff = w1.shape[2] // n_row
    packs = 2
    me = lax.axis_index("row")
    mine = lax.axis_index("col")
    chip = me // 2
    core = lax.rem(me, 2)
    partner = chip * 2 + (1 - core)
    flip = mine // 2
    side = lax.rem(core + flip, 2)
    hops = [2, 1, 3]
    far = len(hops)
    chips = [lax.rem(chip + dc, n_chip) for dc in hops] + [chip]
    mates = [c * 2 + core for c in chips[:far]]
    own_at = pl.ds(pl.multiple_of(core * cols, cols), cols)
    pending = []
    line = (lax.axis_index("dp") * n_col + mine) * n_row
    column = [(lax.axis_index("dp") * n_col + lax.rem(mine + k, n_col)) * n_row for k in range(n_col)]

    def local(src, dst, sem):
        copy = pltpu.make_async_copy(src, dst, sem)
        copy.start()
        return copy

    def remote(src, dst, ssem, rsem, target):
        copy = pltpu.make_async_remote_copy(src_ref=src, dst_ref=dst, send_sem=ssem, recv_sem=rsem,
                                            device_id=target, device_id_type=LOGICAL)
        copy.start()
        pending.append(copy)

    def await_recv(dst, sem):
        pltpu.make_async_remote_copy(src_ref=dst, dst_ref=dst, send_sem=sem, recv_sem=sem,
                                     device_id=line + me, device_id_type=LOGICAL).wait_recv()

    def everyone():
        for i in range(far):
            for e in (0, 1):
                yield i, e, chips[i] * 2 + lax.rem(e + flip, 2)
        yield far, 1 - side, partner

    def senders():
        for i in range(far):
            for e in (0, 1):
                yield i, e
        yield far, 1 - side

    def col_peer(k, half):
        y = lax.rem(mine + k, n_col)
        return column[k] + chip * 2 + lax.rem(half + y // 2, 2)

    def cache_copy(l, which, t):
        src, dst = ((k_hbm, k_buf), (v_hbm, v_buf))[which]
        return pltpu.make_async_copy(src.at[l, pl.ds(16 * t, 16)], dst.at[l, pl.ds(16 * t, 16)], kv_sem.at[l, which, t])

    shared = [(ln1g_hbm, ln1g), (ln1b_hbm, ln1b), (ln2g_hbm, ln2g), (ln2b_hbm, ln2b), (bo_hbm, bo), (b2_hbm, b2)]
    smalls = ([(x_hbm, x_buf), (len_hbm, len_buf), (bq_hbm, bq), (bk_hbm, bk), (bv_hbm, bv), (b1_hbm, b1)]
              + [(src, dst.at[core]) for src, dst in shared])
    small_copies = [local(src, dst, in_sem.at[0, i]) for i, (src, dst) in enumerate(smalls)]

    def load_qkv(l):
        return [local(src.at[l, :, pl.ds(pl.multiple_of(chips[i] * lanes, lanes), lanes)],
                      wqkv.at[l, own_at, (3 * i + t) * lanes:(3 * i + t + 1) * lanes],
                      in_sem.at[1 + l, 3 * i + t]) for i in range(n_chip) for t, src in enumerate((wq_hbm, wk_hbm, wv_hbm))]

    loads = {("qkv", 0): load_qkv(0)}
    barrier = pltpu.get_barrier_semaphore()
    for k in range(1, n_row):
        pl.semaphore_signal(barrier, inc=1, device_id=line + lax.rem(me + k, n_row), device_id_type=LOGICAL)
    for k in range(1, n_col):
        for e in (0, 1):
            pl.semaphore_signal(barrier, inc=1, device_id=col_peer(k, e), device_id_type=LOGICAL)

    def rest_of(l):
        return ([(wo_hbm.at[l], wo.at[l, :, i, :, own_at]) for i in range(packs)]
                + [(w2_hbm.at[l], w2.at[l, :, own_at])]
                + [(w1_hbm.at[l, :, pl.ds(pl.multiple_of(chips[i] * 2 * ff, 2 * ff), 2 * ff)],
                    w1.at[l, own_at, i * 2 * ff:(i + 1) * 2 * ff]) for i in range(n_chip)])

    def load_rest(l):
        return [local(src, dst, in_sem.at[1 + l, 3 * n_chip + i]) for i, (src, dst) in enumerate(rest_of(l))]

    def tile_at(i):
        return slice(i * 3 * lanes, (i + 1) * 3 * lanes)

    def share_qkv(l):
        for i in range(n_chip):
            tile = wqkv.at[l, own_at, tile_at(i)]
            remote(tile, tile, send_sem.at[6], qw_sem.at[l, i], line + partner)

    def await_qkv(l, i):
        await_recv(wqkv.at[l, own_at, tile_at(i)], qw_sem.at[l, i])

    def share_rest(l, which):
        for i, (src, dst) in enumerate(rest_of(l)):
            if i in which:
                remote(src, dst, send_sem.at[7], pw_sem.at[l, 3 + i], line + partner)

    def await_rest(l, which):
        for i, (src, dst) in enumerate(rest_of(l)):
            if i in which:
                loads["rest", l][i].wait()
                await_recv(dst, pw_sem.at[l, 3 + i])

    ONLY_WO, ONLY_W2, ONLY_W1 = range(packs), (packs,), range(packs + 1, packs + 1 + n_chip)

    def load_cache(l):
        for which in range(2):
            for t in range(batch // 16):
                cache_copy(l, which, t).start()

    low = lax.broadcasted_iota(jnp.int32, (rows, lanes), 1) < head
    lane_id = lax.broadcasted_iota(jnp.int32, (16, 16 * head), 1)
    row_id = lax.broadcasted_iota(jnp.int32, (16, 16 * head), 0)
    onehot[...] = jnp.where(lane_id // head == row_id, 1.0, 0.0).astype(BF16)
    for copy in small_copies:
        copy.wait()

    len_all = jnp.transpose(jnp.broadcast_to(len_buf[...], (batch, batch)))
    for h in range(HALVES):
        state[0, h, :, own_at] = x_buf[pl.ds(pl.multiple_of(h * rows + side * sub, sub), sub)]
    mark("load0")
    for copy in loads["qkv", 0]:
        copy.wait()
    load_cache(0)
    loads["rest", 0] = load_rest(0)
    for l in range(1, layers):
        loads["qkv", l] = load_qkv(l)
    mark("barrier")
    pl.semaphore_wait(barrier, n_row + 2 * n_col - 3)
    mark("entry2")
    for h in range(HALVES):
        there = pl.ds(pl.multiple_of(h * rows + (1 - side) * sub, sub), sub)
        remote(x_buf.at[there], state.at[0, h, :, own_at], send_sem.at[0], pair_sem.at[0, h], line + partner)
    for i, (src, dst) in enumerate(shared):
        remote(dst.at[core], dst.at[core], send_sem.at[6], pair_sem.at[1, i], line + partner)
    share_qkv(0)

    def full_row(ref, l):
        return jnp.concatenate([ref[0, l:l + 1], ref[1, l:l + 1]], axis=1).astype(F32)

    def side_operand(gain, shift, l):
        at = lax.broadcasted_iota(jnp.int32, (16, near), 0)
        return jnp.where(at == 0, full_row(gain, l), jnp.where(at == 1, full_row(shift, l), 0.0)).astype(BF16)

    def qkv_tiles(lhs, l, first, last):
        full = jnp.dot(lhs, wqkv[l, :, first * 3 * lanes:last * 3 * lanes], preferred_element_type=F32)
        return [[full[:, (3 * i + t) * lanes:(3 * i + t + 1) * lanes] for t in range(3)] for i in range(last - first)]

    def qkv_side(l):
        lhs = side_operand(ln1g, ln1b, l)
        for i, tiles in enumerate(qkv_tiles(lhs, l, 0, n_chip)):
            q, k, v = [a[0:8] for a in tiles]
            q_r, k_r, v_r = [pltpu.roll(a, head, axis=1) for a in (q, k, v)]
            low8 = low[0:8]
            qk = jnp.where(core == 0, jnp.where(low8, q, k_r), jnp.where(low8, q_r, k))
            vs = jnp.where(core == 0, jnp.where(low8, v, v_r), jnp.where(low8, v_r, v))
            at = lax.broadcasted_iota(jnp.int32, (8, lanes), 0)
            cq_src[l, i] = jnp.where(at < 2, qk, pltpu.roll(vs, 2, axis=0))
        for i in range(far):
            remote(cq_src.at[l, i], cq_in.at[l, i], send_sem.at[1], cq_sem.at[l, i], line + mates[i])

    def up_side(l):
        lhs = side_operand(ln2g, ln2b, l)
        for i in range(n_chip):
            at = pl.ds(pl.multiple_of((2 * i + core) * ff, ff), ff)
            cu_src[l, i] = jnp.dot(lhs, w1[l, :, at], preferred_element_type=F32)[0:8]
        for i in range(far):
            remote(cu_src.at[l, i], cu_in.at[l, i], send_sem.at[1], cu_sem.at[l, i], line + mates[i])

    def normalize(n, h, gain, l):
        mark("norm")
        x = state[n, h].astype(F32)
        s1 = jnp.sum(x, axis=1, keepdims=True)
        s2 = jnp.sum(x * x, axis=1, keepdims=True)
        mean = s1 / near
        inv = lax.rsqrt(jnp.maximum(s2 / near - mean * mean, 0.0) + EPS_LN)
        z = ((x - mean) * inv * full_row(gain, l)).astype(BF16)
        lane = lax.broadcasted_iota(jnp.int32, (sub, 128), 1)
        both = jnp.where(lane == 0, s1, jnp.where(lane == 1, s2, 0.0))
        both = jnp.concatenate([both, jnp.zeros((128 - sub, 128), F32)], axis=0)
        mine_stat = jnp.transpose(both)[0:2]
        stat_src[n, h] = mine_stat
        stat_in[n, h, far, side] = mine_stat
        return z

    def send_stats(n, h):
        for i, e, target in everyone():
            remote(stat_src.at[n, h], stat_in.at[n, h, i, side], send_sem.at[1], stat_sem.at[n, h, i, side], line + target)

    def stat_columns(n, h):
        for i, e in senders():
            await_recv(stat_in.at[n, h, i, e], stat_sem.at[n, h, i, e])
        table = []
        for e in (0, 1):
            parts = [stat_in[n, h, i, e] for i in range(n_chip)]
            total = parts[0]
            for part in parts[1:]:
                total = total + part
            mean = total[0:1] / width
            inv = lax.rsqrt(total[1:2] / width - mean * mean + EPS_LN)
            shifts = []
            for part in parts:
                near_mean = part[0:1] / near
                near_var = jnp.maximum(part[1:2] / near - near_mean * near_mean, 0.0) + EPS_LN
                table.append(inv * (near_var * lax.rsqrt(near_var)))
                shifts.append(inv * (near_mean - mean))
            table.extend(shifts)
        columns = jnp.transpose(jnp.concatenate(table, axis=0))[0:sub]

        def pick(start):
            return [[columns[:, e * 2 * n_chip + start + i:e * 2 * n_chip + start + i + 1] for i in range(n_chip)] for e in (0, 1)]

        return pick(0), pick(n_chip)

    def fold(column):
        return jnp.where(low[0:sub // 2], column[0:sub // 2], column[sub // 2:])

    def send_blocks(src, dst, sem, l, h, first, last):
        for i in range(first, last):
            for c in (0, 1) if i < far else (1 - core,):
                remote(src.at[l, h, i, c], dst.at[l, h, i, side], send_sem.at[2], sem.at[l, h, i, side],
                       line + chips[i] * 2 + c)
        if last == n_chip:
            dst[l, h, far, side] = src[l, h, far, core]

    fresh = {}

    def qkv_go(l, h):
        n = 2 * l
        z = normalize(n, h, ln1g, l)
        send_stats(n, h)
        mark("qkv_mm")
        for i in range(n_chip):
            if l == 0 and h == 0:
                await_qkv(0, i)
                q, k, v = qkv_tiles(z, l, i, i + 1)[0]
            else:
                if i < 2:
                    tiles = qkv_tiles(z, l, i, 1 if i == 0 else n_chip)
                q, k, v = tiles[max(i - 1, 0)]
            q_r, k_r, v_r = [pltpu.roll(a, head, axis=1) for a in (q, k, v)]
            low_s, low_h = low[0:sub], low[0:sub // 2]
            qkv_src[l, h, i, 0, 0:sub] = jnp.where(low_s, q, k_r).astype(BF16)
            qkv_src[l, h, i, 1, 0:sub] = jnp.where(low_s, q_r, k).astype(BF16)
            qkv_src[l, h, i, 0, sub:] = jnp.where(low_h, v[:sub // 2], v_r[sub // 2:]).astype(BF16)
            qkv_src[l, h, i, 1, sub:] = jnp.where(low_h, v_r[:sub // 2], v[sub // 2:]).astype(BF16)
            if i == 0:
                send_blocks(qkv_src, qkv_in, qkv_sem, l, h, 0, 1)
        send_blocks(qkv_src, qkv_in, qkv_sem, l, h, 1, n_chip)

    def qkv_recv(l, h):
        mark("qkv_wait")
        if h == 0:
            const = bias_own[l] + cq_src[l, far]
            cq_in[l, far] = cq_src[l, far]
            for i in range(far):
                await_recv(cq_in.at[l, i], cq_sem.at[l, i])
                const = const + cq_in[l, i]
            bias_own[l] = const
        scales, shifts = stat_columns(2 * l, h)
        qk, vv = [], []
        for e in (0, 1):
            a = jnp.broadcast_to(bias_own[l, 1:2], (sub, lanes))
            b = jnp.broadcast_to(bias_own[l, 3:4], (sub // 2, lanes))
            for i in range(n_chip):
                a = a + shifts[e][i] * cq_in[l, i, 0:1]
                b = b + fold(shifts[e][i]) * cq_in[l, i, 2:3]
            qk.append(a)
            vv.append(b)
        for i, e in senders():
            await_recv(qkv_in.at[l, h, i, e], qkv_sem.at[l, h, i, e])
        mark("qkv_sum")
        for e in (0, 1):
            for i in range(n_chip):
                qk[e] = qk[e] + qkv_in[l, h, i, e, 0:sub].astype(F32) * scales[e][i]
                vv[e] = vv[e] + qkv_in[l, h, i, e, sub:].astype(F32) * fold(scales[e][i])
        qk = jnp.concatenate(qk, axis=0)
        q_b = (qk[:, 0:head] * (head ** -0.5)).astype(BF16)
        k_new = pltpu.roll(qk, head, axis=1)[:, 0:head].astype(BF16)
        v_new = jnp.concatenate([piece for b in vv for piece in (b[:, 0:head], pltpu.roll(b, head, axis=1)[:, 0:head])],
                                axis=0).astype(BF16)
        q_f = q_b.astype(F32)
        k_f = k_new.astype(F32)
        twin[h * rows:(h + 1) * rows, :] = jnp.concatenate([q_f, q_f], axis=1).astype(BF16)
        fresh[l, h] = (jnp.sum(q_f * k_f, axis=1, keepdims=True), k_f, v_new.astype(F32))

    def attend(l, h):
        score_new, k_f, v_f = fresh[l, h]
        base = h * rows
        mine_rows = slice(base, base + rows)
        mark("scores")
        for t in range(rows // 16):
            cache_copy(l, 0, base // 16 + t).wait()
        for t in range(rows // 16):
            at = slice(base + 16 * t, base + 16 * (t + 1))
            q_diag = jnp.concatenate([twin[at, :]] * (16 * head // lanes), axis=1) * onehot[...]
            keys = k_buf[l, at].reshape(16 * head, s_max)
            scores[at, :] = jnp.dot(q_diag, keys, preferred_element_type=F32)
        mark("softmax")
        sc = scores[mine_rows, :]
        position = lax.broadcasted_iota(jnp.int32, sc.shape, 1)
        sc = jnp.where(position < len_all[mine_rows, 0:1], sc, -jnp.inf)
        peak = jnp.maximum(jnp.max(sc, axis=1, keepdims=True), score_new)
        ex = jnp.exp(sc - peak)
        ex_new = jnp.exp(score_new - peak)
        mass = jnp.sum(ex, axis=1, keepdims=True) + ex_new
        inv = 1.0 / mass
        scores[mine_rows, :] = (ex * inv).astype(BF16).astype(F32)
        prob_new = (ex_new * inv).astype(BF16).astype(F32)
        for b in range(s_max // 128):
            probs_t[h, b * 128:(b + 1) * 128, :] = jnp.transpose(scores[mine_rows, b * 128:(b + 1) * 128]).astype(BF16)
        lane = lax.broadcasted_iota(jnp.int32, (head, rows), 1)
        mark("mix")

        def mix_step(t, acc):
            for u in range(2):
                cache_copy(l, 1, base // 16 + 2 * t + u).wait()
            on_mxu = 32 - ON_VPU
            values = v_buf[l, pl.ds(base + 32 * t, on_mxu)].reshape(on_mxu * head, s_max)
            full = jnp.dot(values, probs_t[h], preferred_element_type=F32)
            for i in range(on_mxu, 32):
                prob = scores[pl.ds(base + 32 * t + i, 1), :]
                terms = v_buf[l, base + 32 * t + i].astype(F32) * prob
                short = terms[:, 0:128]
                for b in range(1, s_max // 128):
                    short = short + terms[:, b * 128:(b + 1) * 128]
                acc = jnp.where(lane == 32 * t + i, jnp.sum(short, axis=1, keepdims=True), acc)
            for i in range(on_mxu):
                acc = jnp.where(lane == 32 * t + i, full[i * head:(i + 1) * head], acc)
            return acc

        mixed = lax.fori_loop(0, rows // 32, mix_step, jnp.zeros((head, rows), F32))
        mark("att_send")
        mixed = jnp.transpose(mixed) + prob_new * v_f
        for e in (0, 1):
            first = mixed[e * sub:e * sub + sub // 2]
            second = mixed[e * sub + sub // 2:(e + 1) * sub]
            att_src[l, h, e] = jnp.concatenate([first, second], axis=1).astype(BF16)
        for i, e, target in everyone():
            remote(att_src.at[l, h, e], att_in.at[l, h, me], send_sem.at[3], att_sem.at[l, h, me], line + target)
        att_in[l, h, me] = att_src[l, h, side]
        fresh[l, h] = (k_f, v_f)

    def keep_fresh(l, h):
        k_f, v_f = fresh[l, h]
        k_out[l, :, h * rows:(h + 1) * rows] = jnp.transpose(k_f).astype(BF16)
        v_out[l, :, h * rows:(h + 1) * rows] = jnp.transpose(v_f).astype(BF16)

    def col_send(buf, sem, l, h):
        mark("col_send")
        for k in (2, 1, 3):
            remote(buf.at[l, h, mine], buf.at[l, h, mine], send_sem.at[4], sem.at[l, h, mine], col_peer(k, side))

    def col_recv(buf, sem, l, h, bias, base):
        mark("col_wait")
        for k in range(1, n_col):
            j = lax.rem(mine + k, n_col)
            await_recv(buf.at[l, h, j], sem.at[l, h, j])
        mark("col_sum")
        summed = buf[l, h, 0].astype(F32)
        for j in range(1, n_col):
            summed = summed + buf[l, h, j].astype(F32)
        return (base.astype(F32) + (summed + full_row(bias, l))).astype(BF16)

    def project(l, h):
        mark("att_wait")
        for k in range(1, n_row):
            j = lax.rem(me + k, n_row)
            await_recv(att_in.at[l, h, j], att_sem.at[l, h, j])
        mark("wo_mm")
        low_h = low[0:sub // 2]
        pieces = []
        for j in range(n_row):
            piece = att_in[l, h, j]
            none = jnp.zeros_like(piece)
            pieces.append(jnp.concatenate([jnp.where(low_h, piece, none), jnp.where(low_h, none, piece)], axis=0))
        total = jnp.dot(jnp.concatenate(pieces, axis=1), wo[l].reshape(n_row * lanes, near), preferred_element_type=F32)
        proj_in[l, h, mine] = total.astype(BF16)
        col_send(proj_in, proj_sem, l, h)

    def up_go(l, h):
        n = 2 * l + 1
        z = normalize(n, h, ln2g, l)
        send_stats(n, h)
        mark("up_mm")
        for first, last in ((0, 1), (1, n_chip)):
            full = jnp.dot(z, w1[l, :, first * 2 * ff:last * 2 * ff], preferred_element_type=F32).astype(BF16)
            for i in range(first, last):
                for c in (0, 1):
                    at = (2 * (i - first) + c) * ff
                    up_src[l, h, i, c] = full[:, at:at + ff]
            send_blocks(up_src, up_in, up_sem, l, h, first, last)

    def up_recv(l, h):
        mark("up_wait")
        if h == 0:
            const = b1[l:l + 1, pl.ds(pl.multiple_of(me * ff, ff), ff)].astype(F32) + cu_src[l, far, 1:2]
            cu_in[l, far] = cu_src[l, far]
            for i in range(far):
                await_recv(cu_in.at[l, i], cu_sem.at[l, i])
                const = const + cu_in[l, i, 1:2]
            cu_in[l, far, 1:2] = const
        scales, shifts = stat_columns(2 * l + 1, h)
        totals = []
        for e in (0, 1):
            total = jnp.broadcast_to(cu_in[l, far, 1:2], (sub, ff))
            for i in range(n_chip):
                total = total + shifts[e][i] * cu_in[l, i, 0:1]
            totals.append(total)
        for i, e in senders():
            await_recv(up_in.at[l, h, i, e], up_sem.at[l, h, i, e])
        mark("up_sum")
        for e in (0, 1):
            for i in range(n_chip):
                totals[e] = totals[e] + up_in[l, h, i, e].astype(F32) * scales[e][i]
            act_src[l, h, e] = jnp.maximum(totals[e].astype(BF16), 0)
        for i, e, target in everyone():
            remote(act_src.at[l, h, e], act_in.at[l, h, me], send_sem.at[5], act_sem.at[l, h, me], line + target)
        act_in[l, h, me] = act_src[l, h, side]

    def down(l, h):
        mark("act_wait")
        part = None
        for place, dc in enumerate((0, 1, 3, 2)):
            c = lax.rem(chip + n_chip - dc, n_chip)
            if dc == 0:
                await_recv(act_in.at[l, h, partner], act_sem.at[l, h, partner])
            else:
                for e in (0, 1):
                    await_recv(act_in.at[l, h, 2 * c + e], act_sem.at[l, h, 2 * c + e])
            both = jnp.concatenate([act_in[l, h, 2 * c], act_in[l, h, 2 * c + 1]], axis=1)
            at = pl.ds(pl.multiple_of(c * 2 * ff, 2 * ff), 2 * ff)
            term = jnp.dot(both, w2[l, at, :], preferred_element_type=F32)
            part = term if part is None else part + term
        mark("down_mm")
        part = part.astype(BF16)
        if l + 1 < layers:
            down_in[l, h, mine] = part
            col_send(down_in, down_sem, l, h)
            return
        mark("col_send")
        for c in (0, 1):
            h_src[h, c] = part[:, c * cols:(c + 1) * cols]
        for k in (2, 1, 3):
            for c in (0, 1):
                remote(h_src.at[h, c], h_in.at[h, mine, side], send_sem.at[4], h_sem.at[h, mine, side],
                       column[k] + chip * 2 + c)
        remote(h_src.at[h, 1 - core], h_in.at[h, mine, side], send_sem.at[4], h_sem.at[h, mine, side], line + partner)
        h_in[h, mine, side] = h_src[h, core]

    def finish(h):
        mark("col_wait")
        await_recv(mid_in.at[h], pair_sem.at[2, h])
        for k in range(1, n_col):
            for e in (0, 1):
                j = lax.rem(mine + k, n_col)
                await_recv(h_in.at[h, j, e], h_sem.at[h, j, e])
        await_recv(h_in.at[h, mine, 1 - side], h_sem.at[h, mine, 1 - side])
        mark("last")
        bias = b2[core, layers - 1:layers].astype(F32)
        for e in (0, 1):
            summed = h_in[h, 0, e].astype(F32)
            for j in range(1, n_col):
                summed = summed + h_in[h, j, e].astype(F32)
            base = jnp.where(side == e, state[2 * layers - 1, h, :, own_at].astype(F32), mid_in[h].astype(F32))
            at = h * rows + e * sub
            h_out[at:at + sub] = (base + (summed + bias)).astype(BF16)

    mark("side0")
    for h in range(HALVES):
        await_recv(state.at[0, h, :, own_at], pair_sem.at[0, h])
    for i, (src, dst) in enumerate(shared):
        await_recv(dst.at[core], pair_sem.at[1, i])
    def own_head(vec_ref, l):
        total = jnp.zeros((1, head), F32)
        for j in range(n_row):
            total = total + jnp.where(me == j, vec_ref[l:l + 1, j * head:(j + 1) * head].astype(F32), 0.0)
        return total

    def own_biases():
        zero = jnp.zeros((1, lanes), F32)
        for l in range(layers):
            vb = own_head(bv, l)
            bias_own[l] = jnp.concatenate([zero, jnp.concatenate([own_head(bq, l), own_head(bk, l)], axis=1), zero,
                                           jnp.concatenate([vb, vb], axis=1)] + [zero] * 4, axis=0)

    last = HALVES - 1
    for stage, l, h in stage_order(layers, HALVES):
        n = 2 * l
        if l > 0 and stage == "go":
            new_state = col_recv(down_in, down_sem, l - 1, h, b2, state[n - 1, h])
        if stage == "go":
            if l > 0:
                state[n, h] = new_state
            qkv_go(l, h)
            mark("side")
            if l == 0 and h == 0:
                qkv_side(0)
            if l == 0 and h == last:
                own_biases()
                share_rest(0, ONLY_WO)
                share_rest(0, ONLY_W1)
                share_rest(0, ONLY_W2)
            if l > 0 and h == 0:
                await_rest(l, ONLY_W1)
                up_side(l)
        elif stage == "attend":
            qkv_recv(l, h)
            attend(l, h)
            if l + 1 < layers and h == 0:
                mark("side")
                for copy in loads["qkv", l + 1]:
                    copy.wait()
                share_qkv(l + 1)
                load_cache(l + 1)
                loads["rest", l + 1] = load_rest(l + 1)
                share_rest(l + 1, ONLY_WO)
                share_rest(l + 1, ONLY_W1)
            if l + 1 < layers and h == last:
                share_rest(l + 1, ONLY_W2)
        elif stage == "project":
            if h == 0:
                await_rest(l, ONLY_WO)
            project(l, h)
            mark("side")
            if h == 0 and l == 0:
                await_rest(l, ONLY_W1)
                up_side(l)
            keep_fresh(l, h)
        elif stage == "up":
            state[n + 1, h] = col_recv(proj_in, proj_sem, l, h, bo, state[n, h])
            up_go(l, h)
            if l + 1 == layers:
                there = pl.ds(pl.multiple_of((1 - core) * cols, cols), cols)
                remote(state.at[n + 1, h, :, there], mid_in.at[h], send_sem.at[0], pair_sem.at[2, h], line + partner)
            if h == 0 and l + 1 < layers:
                mark("side")
                for i in range(n_chip):
                    await_qkv(l + 1, i)
                qkv_side(l + 1)
        elif stage == "act":
            up_recv(l, h)
        elif stage == "down":
            if h == 0:
                await_rest(l, ONLY_W2)
            down(l, h)
        else:
            finish(h)
    mark("tail")
    for copy in pending:
        copy.wait_send()
    mark(None)


def store(*refs):
    copies = [pltpu.make_async_copy(refs[i], refs[3 + i], refs[6].at[i]) for i in range(3)]
    for copy in copies:
        copy.start()
    for copy in copies:
        copy.wait()


def solution(mesh):
    n_row = mesh.shape["row"]
    n_col = mesh.shape["col"]
    act_spec = P("dp", "row")
    cache_spec = P(None, "dp", ("col", "row"), None, None)
    fresh_spec = P(None, "dp", ("col", "row"), None)
    in_weight = P(None, "row", "col")
    out_weight = P(None, "col", "row")
    col_vec = P(None, "col")
    row_vec = P(None, "row")
    in_specs = (act_spec, P("dp"), cache_spec, cache_spec, row_vec, row_vec,
                in_weight, col_vec, in_weight, col_vec, in_weight, col_vec,
                out_weight, row_vec, row_vec, row_vec, in_weight, col_vec, out_weight, row_vec)

    def local_step(hidden, cache_len, k_cache, v_cache, *params):
        rows, cols = hidden.shape
        layers, _, _, s_max, head = k_cache.shape
        keys = jnp.swapaxes(k_cache, 3, 4).reshape(layers, rows, head, s_max)
        values = jnp.swapaxes(v_cache, 3, 4).reshape(layers, rows, head, s_max)
        operands = [hidden, cache_len.reshape(1, rows), keys, values, *params]
        packs = 2
        operands[12] = params[8].reshape(layers, n_row, head, cols)
        dma = pltpu.SemaphoreType.DMA
        ff = params[12].shape[2]
        n_chip = n_row // 2
        ff_own = ff // n_row
        near = 2 * cols
        sub = rows // HALVES // 2
        shapes = [(2,) + a.shape if i in (4, 5, 13, 14, 15, 19) else a.shape for i, a in enumerate(operands)]
        shapes[6] = (layers, near, 3 * shapes[6][2])
        shapes[16] = (layers, near, ff)
        shapes[12] = (layers, n_row, 2, head, near)
        shapes[18] = (layers, ff, near)
        vmem = [pltpu.VMEM(s, a.dtype) for i, (s, a) in enumerate(zip(shapes, operands)) if i not in (8, 10)]
        block = sub + sub // 2
        scratch = vmem + [
            pltpu.VMEM((2 * layers, HALVES, sub, near), BF16),
            pltpu.VMEM((2 * layers, HALVES, 2, 128), F32),
            pltpu.VMEM((2 * layers, HALVES, n_chip, 2, 2, 128), F32),
            pltpu.VMEM((layers, n_chip, 8, 2 * head), F32),
            pltpu.VMEM((layers, n_chip, 8, 2 * head), F32),
            pltpu.VMEM((layers, n_chip, 8, ff_own), F32),
            pltpu.VMEM((layers, n_chip, 8, ff_own), F32),
            pltpu.VMEM((layers, 8, 2 * head), F32),
            pltpu.VMEM((layers, HALVES, n_chip, 2, block, 2 * head), BF16),
            pltpu.VMEM((layers, HALVES, n_chip, 2, block, 2 * head), BF16),
            pltpu.VMEM((layers, HALVES, 2, sub // 2, 2 * head), BF16),
            pltpu.VMEM((layers, HALVES, n_row, sub // 2, 2 * head), BF16),
            pltpu.VMEM((layers, HALVES, n_col, sub, near), BF16),
            pltpu.VMEM((layers, HALVES, n_chip, 2, sub, ff_own), BF16),
            pltpu.VMEM((layers, HALVES, n_chip, 2, sub, ff_own), BF16),
            pltpu.VMEM((layers, HALVES, 2, sub, ff_own), BF16),
            pltpu.VMEM((layers, HALVES, n_row, sub, ff_own), BF16),
            pltpu.VMEM((layers, HALVES, n_col, sub, near), BF16),
            pltpu.VMEM((HALVES, 2, sub, cols), BF16),
            pltpu.VMEM((HALVES, n_col, 2, sub, cols), BF16),
            pltpu.VMEM((HALVES, sub, cols), BF16),
            pltpu.VMEM((rows, 2 * head), BF16),
            pltpu.VMEM((16, 16 * head), BF16),
            pltpu.VMEM((rows, s_max), F32),
            pltpu.VMEM((HALVES, s_max, rows // HALVES), BF16),
            dma((1 + layers, 24)),
            dma((layers, 2, rows // 16)),
            dma((9,)),
            dma((layers, 5 + packs + n_chip)),
            dma((3, 8)),
            dma((2 * layers, HALVES, n_chip, 2)),
            dma((layers, n_chip)),
            dma((layers, n_chip)),
            dma((layers, HALVES, n_chip, 2)),
            dma((layers, HALVES, n_row)),
            dma((layers, HALVES, n_col)),
            dma((layers, HALVES, n_chip, 2)),
            dma((layers, HALVES, n_row)),
            dma((layers, HALVES, n_col)),
            dma((HALVES, n_col, 2)),
            dma((layers, n_chip)),
        ]
        h, kt, vt = pl.pallas_call(
            functools.partial(kernel, n_row, n_col, cols * n_row),
            out_shape=(pltpu.VMEM((rows, cols), BF16),
                       pltpu.VMEM((layers, head, rows), BF16),
                       pltpu.VMEM((layers, head, rows), BF16)),
            in_specs=[pl.BlockSpec(memory_space=pltpu.HBM)] * len(operands),
            out_specs=[pl.BlockSpec(memory_space=pltpu.VMEM)] * 3,
            scratch_shapes=scratch,
            compiler_params=pltpu.CompilerParams(collective_id=0, has_side_effects=True,
                                                 vmem_limit_bytes=63 * 2 ** 20),
        )(*operands)
        h, kt, vt = pl.pallas_call(
            store,
            out_shape=(jax.ShapeDtypeStruct((rows, cols), BF16),
                       jax.ShapeDtypeStruct((layers, head, rows), BF16),
                       jax.ShapeDtypeStruct((layers, head, rows), BF16)),
            in_specs=[pl.BlockSpec(memory_space=pltpu.VMEM)] * 3,
            out_specs=[pl.BlockSpec(memory_space=pltpu.HBM)] * 3,
            scratch_shapes=[dma((3,))],
        )(*[pltpu.with_memory_space_constraint(a, pltpu.VMEM) for a in (h, kt, vt)])
        k_new = jnp.swapaxes(kt, 1, 2).reshape(layers, rows, 1, head)
        v_new = jnp.swapaxes(vt, 1, 2).reshape(layers, rows, 1, head)
        return h, k_new, v_new

    return jax.shard_map(local_step, mesh=mesh, in_specs=in_specs,
                         out_specs=(act_spec, fresh_spec, fresh_spec), check_vma=False)
```

```python
import functools

import jax
import jax.numpy as jnp
from jax import lax
from jax.experimental import pallas as pl
from jax.experimental.pallas import tpu as pltpu
from jax.sharding import PartitionSpec as P

EPS_LN = 1e-5
F32 = jnp.float32
BF16 = jnp.bfloat16
LOGICAL = pl.DeviceIdType.LOGICAL


class Marks:
    def __init__(self):
        self.open = None

    def __call__(self, name):
        if self.open is not None:
            self.open.__exit__(None, None, None)
        self.open = None
        if name:
            self.open = jax.named_scope(name)
            self.open.__enter__()


HALVES = 2
SCORES_ON_VPU = 4
ON_VPU = 20
STAGES = {"go": (0.6, 3.6), "attend": (3.1, 3.4), "project": (0.3, 3.6), "up": (0.6, 3.8), "act": (0.3, 3.7), "down": (0.4, 3.6)}


def stage_order(layers, parts):
    names = list(STAGES)
    ready = {part: 0.0 for part in range(parts)}
    done = {part: 0 for part in range(parts)}
    now, order = 0.0, []
    while ready:
        part = min(ready, key=lambda p: (max(ready[p], now), -done[p], p))
        if done[part] == layers * len(names):
            order.append(("end", layers, part))
            del ready[part]
            continue
        layer, name = divmod(done[part], len(names))
        cost, delay = STAGES[names[name]]
        now = max(now, ready[part]) + cost
        order.append((names[name], layer, part))
        done[part] += 1
        ready[part] = now + delay
    return order


def kernel(n_row, n_col, width,
           x_hbm, len_hbm, k_hbm, v_hbm, ln1g_hbm, ln1b_hbm, wq_hbm, bq_hbm, wk_hbm, bk_hbm, wv_hbm, bv_hbm,
           wo_hbm, bo_hbm, ln2g_hbm, ln2b_hbm, w1_hbm, b1_hbm, w2_hbm, b2_hbm,
           h_out, k_out, v_out,
           x_buf, len_buf, k_buf, v_buf, ln1g, ln1b, wqkv, bq, bk, bv, wo, bo, ln2g, ln2b, w1, b1, w2, b2,
           state, stat_src, stat_in, cq_src, cq_in, cu_src, cu_in, bias_own,
           qkv_src, qkv_in, att_src, att_in, proj_in, up_src, up_in, act_src, act_in, down_in, h_src, h_in, mid_in,
           twin, onehot, scores, probs_t,
           in_sem, kv_sem, send_sem, pw_sem, pair_sem, stat_sem, cq_sem, cu_sem,
           qkv_sem, att_sem, proj_sem, up_sem, act_sem, down_sem, h_sem, qw_sem):
    mark = Marks()
    mark("entry")
    layers = wo.shape[0]
    batch, cols = x_buf.shape
    rows = batch // HALVES
    sub = rows // 2
    head = k_buf.shape[2]
    s_max = k_buf.shape[3]
    lanes = 2 * head
    n_chip = n_row // 2
    near = 2 * cols
    ff = w1.shape[2] // n_row
    packs = 2
    me = lax.axis_index("row")
    mine = lax.axis_index("col")
    chip = me // 2
    core = lax.rem(me, 2)
    partner = chip * 2 + (1 - core)
    flip = mine // 2
    side = lax.rem(core + flip, 2)
    hops = [2, 1, 3]
    far = len(hops)
    chips = [lax.rem(chip + dc, n_chip) for dc in hops] + [chip]
    mates = [c * 2 + core for c in chips[:far]]
    own_at = pl.ds(pl.multiple_of(core * cols, cols), cols)
    pending = []
    line = (lax.axis_index("dp") * n_col + mine) * n_row
    column = [(lax.axis_index("dp") * n_col + lax.rem(mine + k, n_col)) * n_row for k in range(n_col)]

    def local(src, dst, sem):
        copy = pltpu.make_async_copy(src, dst, sem)
        copy.start()
        return copy

    def remote(src, dst, ssem, rsem, target):
        copy = pltpu.make_async_remote_copy(src_ref=src, dst_ref=dst, send_sem=ssem, recv_sem=rsem,
                                            device_id=target, device_id_type=LOGICAL)
        copy.start()
        pending.append(copy)

    def await_recv(dst, sem):
        pltpu.make_async_remote_copy(src_ref=dst, dst_ref=dst, send_sem=sem, recv_sem=sem,
                                     device_id=line + me, device_id_type=LOGICAL).wait_recv()

    def everyone():
        for i in range(far):
            for e in (0, 1):
                yield i, e, chips[i] * 2 + lax.rem(e + flip, 2)
        yield far, 1 - side, partner

    def senders():
        for i in range(far):
            for e in (0, 1):
                yield i, e
        yield far, 1 - side

    def col_peer(k, half):
        y = lax.rem(mine + k, n_col)
        return column[k] + chip * 2 + lax.rem(half + y // 2, 2)

    def cache_copy(l, which, t):
        src, dst = ((k_hbm, k_buf), (v_hbm, v_buf))[which]
        return pltpu.make_async_copy(src.at[l, pl.ds(16 * t, 16)], dst.at[l, pl.ds(16 * t, 16)], kv_sem.at[l, which, t])

    shared = [(ln1g_hbm, ln1g), (ln1b_hbm, ln1b), (ln2g_hbm, ln2g), (ln2b_hbm, ln2b), (bo_hbm, bo), (b2_hbm, b2)]
    smalls = ([(x_hbm, x_buf), (len_hbm, len_buf), (bq_hbm, bq), (bk_hbm, bk), (bv_hbm, bv), (b1_hbm, b1)]
              + [(src, dst.at[core]) for src, dst in shared])
    small_copies = [local(src, dst, in_sem.at[0, i]) for i, (src, dst) in enumerate(smalls)]

    def load_qkv(l):
        return [local(src.at[l, :, pl.ds(pl.multiple_of(chips[i] * lanes, lanes), lanes)],
                      wqkv.at[l, own_at, (3 * i + t) * lanes:(3 * i + t + 1) * lanes],
                      in_sem.at[1 + l, 3 * i + t]) for i in range(n_chip) for t, src in enumerate((wq_hbm, wk_hbm, wv_hbm))]

    loads = {("qkv", 0): load_qkv(0)}
    barrier = pltpu.get_barrier_semaphore()
    for k in range(1, n_row):
        pl.semaphore_signal(barrier, inc=1, device_id=line + lax.rem(me + k, n_row), device_id_type=LOGICAL)
    for k in range(1, n_col):
        for e in (0, 1):
            pl.semaphore_signal(barrier, inc=1, device_id=col_peer(k, e), device_id_type=LOGICAL)

    def rest_of(l):
        return ([(wo_hbm.at[l], wo.at[l, :, i, :, own_at]) for i in range(packs)]
                + [(w2_hbm.at[l], w2.at[l, :, own_at])]
                + [(w1_hbm.at[l, :, pl.ds(pl.multiple_of(chips[i] * 2 * ff, 2 * ff), 2 * ff)],
                    w1.at[l, own_at, i * 2 * ff:(i + 1) * 2 * ff]) for i in range(n_chip)])

    def load_rest(l):
        return [local(src, dst, in_sem.at[1 + l, 3 * n_chip + i]) for i, (src, dst) in enumerate(rest_of(l))]

    def tile_at(i):
        return slice(i * 3 * lanes, (i + 1) * 3 * lanes)

    def share_qkv(l):
        for i in range(n_chip):
            share_tile(l, i)

    def share_tile(l, i):
        tile = wqkv.at[l, own_at, tile_at(i)]
        remote(tile, tile, send_sem.at[6], qw_sem.at[l, i], line + partner)

    def await_qkv(l, i):
        await_recv(wqkv.at[l, own_at, tile_at(i)], qw_sem.at[l, i])

    def share_rest(l, which):
        for i, (src, dst) in enumerate(rest_of(l)):
            if i in which:
                remote(src, dst, send_sem.at[7], pw_sem.at[l, 3 + i], line + partner)

    def await_rest(l, which):
        for i, (src, dst) in enumerate(rest_of(l)):
            if i in which:
                loads["rest", l][i].wait()
                await_recv(dst, pw_sem.at[l, 3 + i])

    ONLY_WO, ONLY_W2, ONLY_W1 = range(packs), (packs,), range(packs + 1, packs + 1 + n_chip)

    def load_cache(l):
        for which in range(2):
            for t in range(batch // 16):
                cache_copy(l, which, t).start()

    low = lax.broadcasted_iota(jnp.int32, (rows, lanes), 1) < head
    lane_id = lax.broadcasted_iota(jnp.int32, (16, 16 * head), 1)
    row_id = lax.broadcasted_iota(jnp.int32, (16, 16 * head), 0)
    onehot[...] = jnp.where(lane_id // head == row_id, 1.0, 0.0).astype(BF16)
    for copy in small_copies:
        copy.wait()

    mark("barrier")
    pl.semaphore_wait(barrier, n_row + 2 * n_col - 3)
    mark("entry2")
    for h in range(HALVES):
        there = pl.ds(pl.multiple_of(h * rows + (1 - side) * sub, sub), sub)
        remote(x_buf.at[there], state.at[0, h, :, own_at], send_sem.at[0], pair_sem.at[0, h], line + partner)

    def share_vectors(which):
        for i in which:
            mine_half = shared[i][1].at[core]
            remote(mine_half, mine_half, send_sem.at[6], pair_sem.at[1, i], line + partner)

    share_vectors((0,))
    for i in range(n_chip):
        for t in range(3):
            loads["qkv", 0][3 * i + t].wait()
        share_tile(0, i)
    share_vectors(range(1, len(shared)))
    for h in range(HALVES):
        state[0, h, :, own_at] = x_buf[pl.ds(pl.multiple_of(h * rows + side * sub, sub), sub)]
    load_cache(0)
    loads["rest", 0] = load_rest(0)
    for l in range(1, layers):
        loads["qkv", l] = load_qkv(l)
    len_all = jnp.transpose(jnp.broadcast_to(len_buf[...], (batch, batch)))

    def full_row(ref, l):
        return jnp.concatenate([ref[0, l:l + 1], ref[1, l:l + 1]], axis=1).astype(F32)

    def side_operand(gain, shift, l):
        at = lax.broadcasted_iota(jnp.int32, (16, near), 0)
        return jnp.where(at == 0, full_row(gain, l), jnp.where(at == 1, full_row(shift, l), 0.0)).astype(BF16)

    def qkv_tiles(lhs, l, first, last):
        full = jnp.dot(lhs, wqkv[l, :, first * 3 * lanes:last * 3 * lanes], preferred_element_type=F32)
        return [[full[:, (3 * i + t) * lanes:(3 * i + t + 1) * lanes] for t in range(3)] for i in range(last - first)]

    def qkv_side(l):
        lhs = side_operand(ln1g, ln1b, l)
        for i, tiles in enumerate(qkv_tiles(lhs, l, 0, n_chip)):
            q, k, v = [a[0:8] for a in tiles]
            q_r, k_r, v_r = [pltpu.roll(a, head, axis=1) for a in (q, k, v)]
            low8 = low[0:8]
            qk = jnp.where(core == 0, jnp.where(low8, q, k_r), jnp.where(low8, q_r, k))
            vs = jnp.where(core == 0, jnp.where(low8, v, v_r), jnp.where(low8, v_r, v))
            at = lax.broadcasted_iota(jnp.int32, (8, lanes), 0)
            cq_src[l, i] = jnp.where(at < 2, qk, pltpu.roll(vs, 2, axis=0))
        for i in range(far):
            remote(cq_src.at[l, i], cq_in.at[l, i], send_sem.at[1], cq_sem.at[l, i], line + mates[i])

    def up_side(l):
        lhs = side_operand(ln2g, ln2b, l)
        for i in range(n_chip):
            at = pl.ds(pl.multiple_of((2 * i + core) * ff, ff), ff)
            cu_src[l, i] = jnp.dot(lhs, w1[l, :, at], preferred_element_type=F32)[0:8]
        for i in range(far):
            remote(cu_src.at[l, i], cu_in.at[l, i], send_sem.at[1], cu_sem.at[l, i], line + mates[i])

    def normalize(n, h, gain, l):
        mark("norm")
        x = state[n, h].astype(F32)
        s1 = jnp.sum(x, axis=1, keepdims=True)
        s2 = jnp.sum(x * x, axis=1, keepdims=True)
        mean = s1 / near
        inv = lax.rsqrt(jnp.maximum(s2 / near - mean * mean, 0.0) + EPS_LN)
        z = ((x - mean) * inv * full_row(gain, l)).astype(BF16)
        lane = lax.broadcasted_iota(jnp.int32, (sub, 128), 1)
        both = jnp.where(lane == 0, s1, jnp.where(lane == 1, s2, 0.0))
        both = jnp.concatenate([both, jnp.zeros((128 - sub, 128), F32)], axis=0)
        mine_stat = jnp.transpose(both)[0:2]
        stat_src[n, h] = mine_stat
        stat_in[n, h, far, side] = mine_stat
        return z

    def send_stats(n, h):
        for i, e, target in everyone():
            remote(stat_src.at[n, h], stat_in.at[n, h, i, side], send_sem.at[1], stat_sem.at[n, h, i, side], line + target)

    def stat_columns(n, h):
        for i, e in senders():
            await_recv(stat_in.at[n, h, i, e], stat_sem.at[n, h, i, e])
        table = []
        for e in (0, 1):
            parts = [stat_in[n, h, i, e] for i in range(n_chip)]
            total = parts[0]
            for part in parts[1:]:
                total = total + part
            mean = total[0:1] / width
            inv = lax.rsqrt(total[1:2] / width - mean * mean + EPS_LN)
            shifts = []
            for part in parts:
                near_mean = part[0:1] / near
                near_var = jnp.maximum(part[1:2] / near - near_mean * near_mean, 0.0) + EPS_LN
                table.append(inv * (near_var * lax.rsqrt(near_var)))
                shifts.append(inv * (near_mean - mean))
            table.extend(shifts)
        columns = jnp.transpose(jnp.concatenate(table, axis=0))[0:sub]

        def pick(start):
            return [[columns[:, e * 2 * n_chip + start + i:e * 2 * n_chip + start + i + 1] for i in range(n_chip)] for e in (0, 1)]

        return pick(0), pick(n_chip)

    def fold(column):
        return jnp.where(low[0:sub // 2], column[0:sub // 2], column[sub // 2:])

    def send_blocks(src, dst, sem, l, h, first, last):
        for i in range(first, last):
            for c in (0, 1) if i < far else (1 - core,):
                remote(src.at[l, h, i, c], dst.at[l, h, i, side], send_sem.at[2], sem.at[l, h, i, side],
                       line + chips[i] * 2 + c)
        if last == n_chip:
            dst[l, h, far, side] = src[l, h, far, core]

    fresh = {}

    def qkv_go(l, h):
        n = 2 * l
        z = normalize(n, h, ln1g, l)
        send_stats(n, h)
        mark("qkv_mm")
        for i in range(n_chip):
            if l == 0 and h == 0:
                await_qkv(0, i)
                q, k, v = qkv_tiles(z, l, i, i + 1)[0]
            else:
                if i < 2:
                    tiles = qkv_tiles(z, l, i, 1 if i == 0 else n_chip)
                q, k, v = tiles[max(i - 1, 0)]
            q_r, k_r, v_r = [pltpu.roll(a, head, axis=1) for a in (q, k, v)]
            low_s, low_h = low[0:sub], low[0:sub // 2]
            qkv_src[l, h, i, 0, 0:sub] = jnp.where(low_s, q, k_r).astype(BF16)
            qkv_src[l, h, i, 1, 0:sub] = jnp.where(low_s, q_r, k).astype(BF16)
            qkv_src[l, h, i, 0, sub:] = jnp.where(low_h, v[:sub // 2], v_r[sub // 2:]).astype(BF16)
            qkv_src[l, h, i, 1, sub:] = jnp.where(low_h, v_r[:sub // 2], v[sub // 2:]).astype(BF16)
            if i == 0:
                send_blocks(qkv_src, qkv_in, qkv_sem, l, h, 0, 1)
        send_blocks(qkv_src, qkv_in, qkv_sem, l, h, 1, n_chip)

    def qkv_recv(l, h):
        mark("qkv_wait")
        if h == 0:
            const = bias_own[l] + cq_src[l, far]
            cq_in[l, far] = cq_src[l, far]
            for i in range(far):
                await_recv(cq_in.at[l, i], cq_sem.at[l, i])
                const = const + cq_in[l, i]
            bias_own[l] = const
        scales, shifts = stat_columns(2 * l, h)
        qk, vv = [], []
        for e in (0, 1):
            a = jnp.broadcast_to(bias_own[l, 1:2], (sub, lanes))
            b = jnp.broadcast_to(bias_own[l, 3:4], (sub // 2, lanes))
            for i in range(n_chip):
                a = a + shifts[e][i] * cq_in[l, i, 0:1]
                b = b + fold(shifts[e][i]) * cq_in[l, i, 2:3]
            qk.append(a)
            vv.append(b)
        for i, e in senders():
            await_recv(qkv_in.at[l, h, i, e], qkv_sem.at[l, h, i, e])
        mark("qkv_sum")
        for e in (0, 1):
            for i in range(n_chip):
                qk[e] = qk[e] + qkv_in[l, h, i, e, 0:sub].astype(F32) * scales[e][i]
                vv[e] = vv[e] + qkv_in[l, h, i, e, sub:].astype(F32) * fold(scales[e][i])
        qk = jnp.concatenate(qk, axis=0)
        q_b = (qk[:, 0:head] * (head ** -0.5)).astype(BF16)
        k_new = pltpu.roll(qk, head, axis=1)[:, 0:head].astype(BF16)
        v_new = jnp.concatenate([piece for b in vv for piece in (b[:, 0:head], pltpu.roll(b, head, axis=1)[:, 0:head])],
                                axis=0).astype(BF16)
        q_f = q_b.astype(F32)
        k_f = k_new.astype(F32)
        twin[h * rows:(h + 1) * rows, :] = jnp.concatenate([q_f, q_f], axis=1).astype(BF16)
        fresh[l, h] = (jnp.sum(q_f * k_f, axis=1, keepdims=True), k_f, v_new.astype(F32))

    def attend(l, h):
        score_new, k_f, v_f = fresh[l, h]
        base = h * rows
        mine_rows = slice(base, base + rows)
        mark("scores")
        for t in range(rows // 16):
            cache_copy(l, 0, base // 16 + t).wait()
        on_mxu = 16 - SCORES_ON_VPU
        q_t = jnp.transpose(twin[mine_rows, :].astype(F32))[0:head]
        for t in range(rows // 16):
            at = slice(base + 16 * t, base + 16 * (t + 1))
            q_diag = jnp.concatenate([twin[at, :]] * (on_mxu * head // lanes), axis=1) * onehot[:, 0:on_mxu * head]
            keys = k_buf[l, base + 16 * t:base + 16 * t + on_mxu].reshape(on_mxu * head, s_max)
            scores[base + 16 * t:base + 16 * t + on_mxu, :] = jnp.dot(q_diag, keys, preferred_element_type=F32)[0:on_mxu]
            for i in range(on_mxu, 16):
                b = 16 * t + i
                terms = k_buf[l, base + b].astype(F32) * q_t[:, b:b + 1]
                scores[base + b:base + b + 1, :] = jnp.sum(terms, axis=0, keepdims=True)
        mark("softmax")
        sc = scores[mine_rows, :]
        position = lax.broadcasted_iota(jnp.int32, sc.shape, 1)
        sc = jnp.where(position < len_all[mine_rows, 0:1], sc, -jnp.inf)
        peak = jnp.maximum(jnp.max(sc, axis=1, keepdims=True), score_new)
        ex = jnp.exp(sc - peak)
        ex_new = jnp.exp(score_new - peak)
        mass = jnp.sum(ex, axis=1, keepdims=True) + ex_new
        inv = 1.0 / mass
        scores[mine_rows, :] = (ex * inv).astype(BF16).astype(F32)
        prob_new = (ex_new * inv).astype(BF16).astype(F32)
        for b in range(s_max // 128):
            probs_t[h, b * 128:(b + 1) * 128, :] = jnp.transpose(scores[mine_rows, b * 128:(b + 1) * 128]).astype(BF16)
        lane = lax.broadcasted_iota(jnp.int32, (head, rows), 1)
        mark("mix")

        def mix_step(t, acc):
            for u in range(2):
                cache_copy(l, 1, base // 16 + 2 * t + u).wait()
            on_mxu = 32 - ON_VPU
            values = v_buf[l, pl.ds(base + 32 * t, on_mxu)].reshape(on_mxu * head, s_max)
            full = jnp.dot(values, probs_t[h], preferred_element_type=F32)
            for i in range(on_mxu, 32):
                prob = scores[pl.ds(base + 32 * t + i, 1), :]
                terms = v_buf[l, base + 32 * t + i].astype(F32) * prob
                short = terms[:, 0:128]
                for b in range(1, s_max // 128):
                    short = short + terms[:, b * 128:(b + 1) * 128]
                acc = jnp.where(lane == 32 * t + i, jnp.sum(short, axis=1, keepdims=True), acc)
            for i in range(on_mxu):
                acc = jnp.where(lane == 32 * t + i, full[i * head:(i + 1) * head], acc)
            return acc

        mixed = lax.fori_loop(0, rows // 32, mix_step, jnp.zeros((head, rows), F32))
        mark("att_send")
        mixed = jnp.transpose(mixed) + prob_new * v_f
        for e in (0, 1):
            first = mixed[e * sub:e * sub + sub // 2]
            second = mixed[e * sub + sub // 2:(e + 1) * sub]
            att_src[l, h, e] = jnp.concatenate([first, second], axis=1).astype(BF16)
        for i, e, target in everyone():
            remote(att_src.at[l, h, e], att_in.at[l, h, me], send_sem.at[3], att_sem.at[l, h, me], line + target)
        att_in[l, h, me] = att_src[l, h, side]
        fresh[l, h] = (k_f, v_f)

    def keep_fresh(l, h):
        k_f, v_f = fresh[l, h]
        k_out[l, :, h * rows:(h + 1) * rows] = jnp.transpose(k_f).astype(BF16)
        v_out[l, :, h * rows:(h + 1) * rows] = jnp.transpose(v_f).astype(BF16)

    def col_send(buf, sem, l, h):
        mark("col_send")
        for k in (2, 1, 3):
            remote(buf.at[l, h, mine], buf.at[l, h, mine], send_sem.at[4], sem.at[l, h, mine], col_peer(k, side))

    def col_recv(buf, sem, l, h, bias, base):
        mark("col_wait")
        for k in range(1, n_col):
            j = lax.rem(mine + k, n_col)
            await_recv(buf.at[l, h, j], sem.at[l, h, j])
        mark("col_sum")
        summed = buf[l, h, 0].astype(F32)
        for j in range(1, n_col):
            summed = summed + buf[l, h, j].astype(F32)
        return (base.astype(F32) + (summed + full_row(bias, l))).astype(BF16)

    def project(l, h):
        mark("att_wait")
        for k in range(1, n_row):
            j = lax.rem(me + k, n_row)
            await_recv(att_in.at[l, h, j], att_sem.at[l, h, j])
        mark("wo_mm")
        low_h = low[0:sub // 2]
        pieces = []
        for j in range(n_row):
            piece = att_in[l, h, j]
            none = jnp.zeros_like(piece)
            pieces.append(jnp.concatenate([jnp.where(low_h, piece, none), jnp.where(low_h, none, piece)], axis=0))
        total = jnp.dot(jnp.concatenate(pieces, axis=1), wo[l].reshape(n_row * lanes, near), preferred_element_type=F32)
        proj_in[l, h, mine] = total.astype(BF16)
        col_send(proj_in, proj_sem, l, h)

    def up_go(l, h):
        n = 2 * l + 1
        z = normalize(n, h, ln2g, l)
        send_stats(n, h)
        mark("up_mm")
        for first, last in ((0, 1), (1, n_chip)):
            full = jnp.dot(z, w1[l, :, first * 2 * ff:last * 2 * ff], preferred_element_type=F32).astype(BF16)
            for i in range(first, last):
                for c in (0, 1):
                    at = (2 * (i - first) + c) * ff
                    up_src[l, h, i, c] = full[:, at:at + ff]
            send_blocks(up_src, up_in, up_sem, l, h, first, last)

    def up_recv(l, h):
        mark("up_wait")
        if h == 0:
            const = b1[l:l + 1, pl.ds(pl.multiple_of(me * ff, ff), ff)].astype(F32) + cu_src[l, far, 1:2]
            cu_in[l, far] = cu_src[l, far]
            for i in range(far):
                await_recv(cu_in.at[l, i], cu_sem.at[l, i])
                const = const + cu_in[l, i, 1:2]
            cu_in[l, far, 1:2] = const
        scales, shifts = stat_columns(2 * l + 1, h)
        totals = []
        for e in (0, 1):
            total = jnp.broadcast_to(cu_in[l, far, 1:2], (sub, ff))
            for i in range(n_chip):
                total = total + shifts[e][i] * cu_in[l, i, 0:1]
            totals.append(total)
        for i, e in senders():
            await_recv(up_in.at[l, h, i, e], up_sem.at[l, h, i, e])
        mark("up_sum")
        for e in (0, 1):
            for i in range(n_chip):
                totals[e] = totals[e] + up_in[l, h, i, e].astype(F32) * scales[e][i]
            act_src[l, h, e] = jnp.maximum(totals[e].astype(BF16), 0)
        for i, e, target in everyone():
            remote(act_src.at[l, h, e], act_in.at[l, h, me], send_sem.at[5], act_sem.at[l, h, me], line + target)
        act_in[l, h, me] = act_src[l, h, side]

    def down(l, h):
        mark("act_wait")
        part = None
        for place, dc in enumerate((0, 1, 3, 2)):
            c = lax.rem(chip + n_chip - dc, n_chip)
            if dc == 0:
                await_recv(act_in.at[l, h, partner], act_sem.at[l, h, partner])
            else:
                for e in (0, 1):
                    await_recv(act_in.at[l, h, 2 * c + e], act_sem.at[l, h, 2 * c + e])
            both = jnp.concatenate([act_in[l, h, 2 * c], act_in[l, h, 2 * c + 1]], axis=1)
            at = pl.ds(pl.multiple_of(c * 2 * ff, 2 * ff), 2 * ff)
            term = jnp.dot(both, w2[l, at, :], preferred_element_type=F32)
            part = term if part is None else part + term
        mark("down_mm")
        part = part.astype(BF16)
        if l + 1 < layers:
            down_in[l, h, mine] = part
            col_send(down_in, down_sem, l, h)
            return
        mark("col_send")
        for c in (0, 1):
            h_src[h, c] = part[:, c * cols:(c + 1) * cols]
        for k in (2, 1, 3):
            for c in (0, 1):
                remote(h_src.at[h, c], h_in.at[h, mine, side], send_sem.at[4], h_sem.at[h, mine, side],
                       column[k] + chip * 2 + c)
        remote(h_src.at[h, 1 - core], h_in.at[h, mine, side], send_sem.at[4], h_sem.at[h, mine, side], line + partner)
        h_in[h, mine, side] = h_src[h, core]

    def finish(h):
        mark("col_wait")
        await_recv(mid_in.at[h], pair_sem.at[2, h])
        for k in range(1, n_col):
            for e in (0, 1):
                j = lax.rem(mine + k, n_col)
                await_recv(h_in.at[h, j, e], h_sem.at[h, j, e])
        await_recv(h_in.at[h, mine, 1 - side], h_sem.at[h, mine, 1 - side])
        mark("last")
        bias = b2[core, layers - 1:layers].astype(F32)
        for e in (0, 1):
            summed = h_in[h, 0, e].astype(F32)
            for j in range(1, n_col):
                summed = summed + h_in[h, j, e].astype(F32)
            base = jnp.where(side == e, state[2 * layers - 1, h, :, own_at].astype(F32), mid_in[h].astype(F32))
            at = h * rows + e * sub
            h_out[at:at + sub] = (base + (summed + bias)).astype(BF16)

    mark("side0")
    for h in range(HALVES):
        await_recv(state.at[0, h, :, own_at], pair_sem.at[0, h])
    await_recv(ln1g.at[core], pair_sem.at[1, 0])
    def own_head(vec_ref, l):
        total = jnp.zeros((1, head), F32)
        for j in range(n_row):
            total = total + jnp.where(me == j, vec_ref[l:l + 1, j * head:(j + 1) * head].astype(F32), 0.0)
        return total

    def own_biases():
        zero = jnp.zeros((1, lanes), F32)
        for l in range(layers):
            vb = own_head(bv, l)
            bias_own[l] = jnp.concatenate([zero, jnp.concatenate([own_head(bq, l), own_head(bk, l)], axis=1), zero,
                                           jnp.concatenate([vb, vb], axis=1)] + [zero] * 4, axis=0)

    last = HALVES - 1
    for stage, l, h in stage_order(layers, HALVES):
        n = 2 * l
        if l > 0 and stage == "go":
            new_state = col_recv(down_in, down_sem, l - 1, h, b2, state[n - 1, h])
        if stage == "go":
            if l > 0:
                state[n, h] = new_state
            qkv_go(l, h)
            mark("side")
            if l == 0 and h == 0:
                for i in range(1, len(shared)):
                    await_recv(shared[i][1].at[core], pair_sem.at[1, i])
                qkv_side(0)
            if l == 0 and h == last:
                own_biases()
                share_rest(0, ONLY_WO)
                share_rest(0, ONLY_W1)
                share_rest(0, ONLY_W2)
                for later in range(1, layers):
                    load_cache(later)
                    loads["rest", later] = load_rest(later)
            if l > 0 and h == 0:
                await_rest(l, ONLY_W1)
                up_side(l)
        elif stage == "attend":
            qkv_recv(l, h)
            attend(l, h)
            if l + 1 < layers and h == last:
                mark("side")
                for copy in loads["qkv", l + 1]:
                    copy.wait()
                share_qkv(l + 1)
        elif stage == "project":
            if h == 0:
                await_rest(l, ONLY_WO)
            project(l, h)
            mark("side")
            if h == 0 and l == 0:
                await_rest(l, ONLY_W1)
                up_side(l)
            if h < last:
                keep_fresh(l, h)
        elif stage == "up":
            state[n + 1, h] = col_recv(proj_in, proj_sem, l, h, bo, state[n, h])
            up_go(l, h)
            if h == 0:
                mark("side")
                keep_fresh(l, last)
                if l + 1 < layers:
                    share_rest(l + 1, ONLY_WO)
                    share_rest(l + 1, ONLY_W1)
                    share_rest(l + 1, ONLY_W2)
            if l + 1 == layers:
                there = pl.ds(pl.multiple_of((1 - core) * cols, cols), cols)
                remote(state.at[n + 1, h, :, there], mid_in.at[h], send_sem.at[0], pair_sem.at[2, h], line + partner)
            if h == 0 and l + 1 < layers:
                mark("side")
                for i in range(n_chip):
                    await_qkv(l + 1, i)
                qkv_side(l + 1)
        elif stage == "act":
            up_recv(l, h)
        elif stage == "down":
            if h == 0:
                await_rest(l, ONLY_W2)
            down(l, h)
        else:
            finish(h)
    mark("tail")
    for copy in pending:
        copy.wait_send()
    mark(None)


def store(*refs):
    copies = [pltpu.make_async_copy(refs[i], refs[3 + i], refs[6].at[i]) for i in range(3)]
    for copy in copies:
        copy.start()
    for copy in copies:
        copy.wait()


def solution(mesh):
    n_row = mesh.shape["row"]
    n_col = mesh.shape["col"]
    act_spec = P("dp", "row")
    cache_spec = P(None, "dp", ("col", "row"), None, None)
    fresh_spec = P(None, "dp", ("col", "row"), None)
    in_weight = P(None, "row", "col")
    out_weight = P(None, "col", "row")
    col_vec = P(None, "col")
    row_vec = P(None, "row")
    in_specs = (act_spec, P("dp"), cache_spec, cache_spec, row_vec, row_vec,
                in_weight, col_vec, in_weight, col_vec, in_weight, col_vec,
                out_weight, row_vec, row_vec, row_vec, in_weight, col_vec, out_weight, row_vec)

    def local_step(hidden, cache_len, k_cache, v_cache, *params):
        rows, cols = hidden.shape
        layers, _, _, s_max, head = k_cache.shape
        keys = jnp.swapaxes(k_cache, 3, 4).reshape(layers, rows, head, s_max)
        values = jnp.swapaxes(v_cache, 3, 4).reshape(layers, rows, head, s_max)
        operands = [hidden, cache_len.reshape(1, rows), keys, values, *params]
        packs = 2
        operands[12] = params[8].reshape(layers, n_row, head, cols)
        dma = pltpu.SemaphoreType.DMA
        ff = params[12].shape[2]
        n_chip = n_row // 2
        ff_own = ff // n_row
        near = 2 * cols
        sub = rows // HALVES // 2
        shapes = [(2,) + a.shape if i in (4, 5, 13, 14, 15, 19) else a.shape for i, a in enumerate(operands)]
        shapes[6] = (layers, near, 3 * shapes[6][2])
        shapes[16] = (layers, near, ff)
        shapes[12] = (layers, n_row, 2, head, near)
        shapes[18] = (layers, ff, near)
        vmem = [pltpu.VMEM(s, a.dtype) for i, (s, a) in enumerate(zip(shapes, operands)) if i not in (8, 10)]
        block = sub + sub // 2
        scratch = vmem + [
            pltpu.VMEM((2 * layers, HALVES, sub, near), BF16),
            pltpu.VMEM((2 * layers, HALVES, 2, 128), F32),
            pltpu.VMEM((2 * layers, HALVES, n_chip, 2, 2, 128), F32),
            pltpu.VMEM((layers, n_chip, 8, 2 * head), F32),
            pltpu.VMEM((layers, n_chip, 8, 2 * head), F32),
            pltpu.VMEM((layers, n_chip, 8, ff_own), F32),
            pltpu.VMEM((layers, n_chip, 8, ff_own), F32),
            pltpu.VMEM((layers, 8, 2 * head), F32),
            pltpu.VMEM((layers, HALVES, n_chip, 2, block, 2 * head), BF16),
            pltpu.VMEM((layers, HALVES, n_chip, 2, block, 2 * head), BF16),
            pltpu.VMEM((layers, HALVES, 2, sub // 2, 2 * head), BF16),
            pltpu.VMEM((layers, HALVES, n_row, sub // 2, 2 * head), BF16),
            pltpu.VMEM((layers, HALVES, n_col, sub, near), BF16),
            pltpu.VMEM((layers, HALVES, n_chip, 2, sub, ff_own), BF16),
            pltpu.VMEM((layers, HALVES, n_chip, 2, sub, ff_own), BF16),
            pltpu.VMEM((layers, HALVES, 2, sub, ff_own), BF16),
            pltpu.VMEM((layers, HALVES, n_row, sub, ff_own), BF16),
            pltpu.VMEM((layers, HALVES, n_col, sub, near), BF16),
            pltpu.VMEM((HALVES, 2, sub, cols), BF16),
            pltpu.VMEM((HALVES, n_col, 2, sub, cols), BF16),
            pltpu.VMEM((HALVES, sub, cols), BF16),
            pltpu.VMEM((rows, 2 * head), BF16),
            pltpu.VMEM((16, 16 * head), BF16),
            pltpu.VMEM((rows, s_max), F32),
            pltpu.VMEM((HALVES, s_max, rows // HALVES), BF16),
            dma((1 + layers, 24)),
            dma((layers, 2, rows // 16)),
            dma((9,)),
            dma((layers, 5 + packs + n_chip)),
            dma((3, 8)),
            dma((2 * layers, HALVES, n_chip, 2)),
            dma((layers, n_chip)),
            dma((layers, n_chip)),
            dma((layers, HALVES, n_chip, 2)),
            dma((layers, HALVES, n_row)),
            dma((layers, HALVES, n_col)),
            dma((layers, HALVES, n_chip, 2)),
            dma((layers, HALVES, n_row)),
            dma((layers, HALVES, n_col)),
            dma((HALVES, n_col, 2)),
            dma((layers, n_chip)),
        ]
        h, kt, vt = pl.pallas_call(
            functools.partial(kernel, n_row, n_col, cols * n_row),
            out_shape=(pltpu.VMEM((rows, cols), BF16),
                       pltpu.VMEM((layers, head, rows), BF16),
                       pltpu.VMEM((layers, head, rows), BF16)),
            in_specs=[pl.BlockSpec(memory_space=pltpu.HBM)] * len(operands),
            out_specs=[pl.BlockSpec(memory_space=pltpu.VMEM)] * 3,
            scratch_shapes=scratch,
            compiler_params=pltpu.CompilerParams(collective_id=0, has_side_effects=True,
                                                 vmem_limit_bytes=63 * 2 ** 20),
        )(*operands)
        h, kt, vt = pl.pallas_call(
            store,
            out_shape=(jax.ShapeDtypeStruct((rows, cols), BF16),
                       jax.ShapeDtypeStruct((layers, head, rows), BF16),
                       jax.ShapeDtypeStruct((layers, head, rows), BF16)),
            in_specs=[pl.BlockSpec(memory_space=pltpu.VMEM)] * 3,
            out_specs=[pl.BlockSpec(memory_space=pltpu.HBM)] * 3,
            scratch_shapes=[dma((3,))],
        )(*[pltpu.with_memory_space_constraint(a, pltpu.VMEM) for a in (h, kt, vt)])
        k_new = jnp.swapaxes(kt, 1, 2).reshape(layers, rows, 1, head)
        v_new = jnp.swapaxes(vt, 1, 2).reshape(layers, rows, 1, head)
        return h, k_new, v_new

    return jax.shard_map(local_step, mesh=mesh, in_specs=in_specs,
                         out_specs=(act_spec, fresh_spec, fresh_spec), check_vma=False)
```

```python
import functools

import jax
import jax.numpy as jnp
from jax import lax
from jax.experimental import pallas as pl
from jax.experimental.pallas import tpu as pltpu
from jax.sharding import PartitionSpec as P

EPS_LN = 1e-5
F32 = jnp.float32
BF16 = jnp.bfloat16
LOGICAL = pl.DeviceIdType.LOGICAL


class Marks:
    def __init__(self):
        self.open = None

    def __call__(self, name):
        if self.open is not None:
            self.open.__exit__(None, None, None)
        self.open = None
        if name:
            self.open = jax.named_scope(name)
            self.open.__enter__()


HALVES = 2
SCORES_ON_VPU = 4
ON_VPU = 20
STAGES = {"go": (0.6, 3.6), "attend": (3.1, 3.4), "project": (0.3, 3.6), "up": (0.6, 3.8), "act": (0.3, 3.7), "down": (0.4, 3.6)}


def stage_order(layers, parts):
    names = list(STAGES)
    ready = {part: 0.0 for part in range(parts)}
    done = {part: 0 for part in range(parts)}
    now, order = 0.0, []
    while ready:
        part = min(ready, key=lambda p: (max(ready[p], now), -done[p], p))
        if done[part] == layers * len(names):
            order.append(("end", layers, part))
            del ready[part]
            continue
        layer, name = divmod(done[part], len(names))
        cost, delay = STAGES[names[name]]
        now = max(now, ready[part]) + cost
        order.append((names[name], layer, part))
        done[part] += 1
        ready[part] = now + delay
    return order


def kernel(n_row, n_col, width,
           x_hbm, len_hbm, k_hbm, v_hbm, ln1g_hbm, ln1b_hbm, wq_hbm, bq_hbm, wk_hbm, bk_hbm, wv_hbm, bv_hbm,
           wo_hbm, bo_hbm, ln2g_hbm, ln2b_hbm, w1_hbm, b1_hbm, w2_hbm, b2_hbm,
           h_out, k_out, v_out,
           x_buf, len_buf, k_buf, v_buf, ln1g, ln1b, wqkv, bq, bk, bv, wo, bo, ln2g, ln2b, w1, b1, w2, b2,
           state, stat_src, stat_in, cq_src, cq_in, cu_src, cu_in, bias_own,
           qkv_src, qkv_in, att_src, att_in, proj_in, up_src, up_in, act_src, act_in, down_in, h_src, h_in, mid_in,
           twin, onehot, scores, probs_t,
           in_sem, kv_sem, send_sem, pw_sem, pair_sem, stat_sem, cq_sem, cu_sem,
           qkv_sem, att_sem, proj_sem, up_sem, act_sem, down_sem, h_sem, qw_sem):
    mark = Marks()
    mark("entry")
    layers = wo.shape[0]
    batch, cols = x_buf.shape
    rows = batch // HALVES
    sub = rows // 2
    head = k_buf.shape[2]
    s_max = k_buf.shape[3]
    lanes = 2 * head
    n_chip = n_row // 2
    near = 2 * cols
    ff = w1.shape[2] // n_row
    packs = 2
    me = lax.axis_index("row")
    mine = lax.axis_index("col")
    chip = me // 2
    core = lax.rem(me, 2)
    partner = chip * 2 + (1 - core)
    flip = mine // 2
    side = lax.rem(core + flip, 2)
    hops = [2, 1, 3]
    far = len(hops)
    chips = [lax.rem(chip + dc, n_chip) for dc in hops] + [chip]
    mates = [c * 2 + core for c in chips[:far]]
    own_at = pl.ds(pl.multiple_of(core * cols, cols), cols)
    pending = []
    line = (lax.axis_index("dp") * n_col + mine) * n_row
    column = [(lax.axis_index("dp") * n_col + lax.rem(mine + k, n_col)) * n_row for k in range(n_col)]

    def local(src, dst, sem):
        copy = pltpu.make_async_copy(src, dst, sem)
        copy.start()
        return copy

    def remote(src, dst, ssem, rsem, target):
        copy = pltpu.make_async_remote_copy(src_ref=src, dst_ref=dst, send_sem=ssem, recv_sem=rsem,
                                            device_id=target, device_id_type=LOGICAL)
        copy.start()
        pending.append(copy)

    def await_recv(dst, sem):
        pltpu.make_async_remote_copy(src_ref=dst, dst_ref=dst, send_sem=sem, recv_sem=sem,
                                     device_id=line + me, device_id_type=LOGICAL).wait_recv()

    def everyone():
        for i in range(far):
            for e in (0, 1):
                yield i, e, chips[i] * 2 + lax.rem(e + flip, 2)
        yield far, 1 - side, partner

    def senders():
        for i in range(far):
            for e in (0, 1):
                yield i, e
        yield far, 1 - side

    def col_peer(k, half):
        y = lax.rem(mine + k, n_col)
        return column[k] + chip * 2 + lax.rem(half + y // 2, 2)

    def cache_copy(l, which, t):
        src, dst = ((k_hbm, k_buf), (v_hbm, v_buf))[which]
        return pltpu.make_async_copy(src.at[l, pl.ds(16 * t, 16)], dst.at[l, pl.ds(16 * t, 16)], kv_sem.at[l, which, t])

    shared = [(ln1g_hbm, ln1g), (ln1b_hbm, ln1b), (ln2g_hbm, ln2g), (ln2b_hbm, ln2b), (bo_hbm, bo), (b2_hbm, b2)]
    smalls = ([(x_hbm, x_buf), (len_hbm, len_buf), (bq_hbm, bq), (bk_hbm, bk), (bv_hbm, bv), (b1_hbm, b1)]
              + [(src, dst.at[core]) for src, dst in shared])
    small_copies = [local(src, dst, in_sem.at[0, i]) for i, (src, dst) in enumerate(smalls)]

    def load_qkv(l):
        return [local(src.at[l, :, pl.ds(pl.multiple_of(chips[i] * lanes, lanes), lanes)],
                      wqkv.at[l, own_at, (3 * i + t) * lanes:(3 * i + t + 1) * lanes],
                      in_sem.at[1 + l, 3 * i + t]) for i in range(n_chip) for t, src in enumerate((wq_hbm, wk_hbm, wv_hbm))]

    loads = {("qkv", 0): load_qkv(0)}
    barrier = pltpu.get_barrier_semaphore()
    for k in range(1, n_row):
        pl.semaphore_signal(barrier, inc=1, device_id=line + lax.rem(me + k, n_row), device_id_type=LOGICAL)
    for k in range(1, n_col):
        for e in (0, 1):
            pl.semaphore_signal(barrier, inc=1, device_id=col_peer(k, e), device_id_type=LOGICAL)

    def rest_of(l):
        return ([(wo_hbm.at[l], wo.at[l, :, i, :, own_at]) for i in range(packs)]
                + [(w2_hbm.at[l], w2.at[l, :, own_at])]
                + [(w1_hbm.at[l, :, pl.ds(pl.multiple_of(chips[i] * 2 * ff, 2 * ff), 2 * ff)],
                    w1.at[l, own_at, i * 2 * ff:(i + 1) * 2 * ff]) for i in range(n_chip)])

    def load_rest(l):
        return [local(src, dst, in_sem.at[1 + l, 3 * n_chip + i]) for i, (src, dst) in enumerate(rest_of(l))]

    def tile_at(i):
        return slice(i * 3 * lanes, (i + 1) * 3 * lanes)

    def share_qkv(l):
        for i in range(n_chip):
            share_tile(l, i)

    def share_tile(l, i):
        tile = wqkv.at[l, own_at, tile_at(i)]
        remote(tile, tile, send_sem.at[6], qw_sem.at[l, i], line + partner)

    def await_qkv(l, i):
        await_recv(wqkv.at[l, own_at, tile_at(i)], qw_sem.at[l, i])

    def share_rest(l, which):
        for i, (src, dst) in enumerate(rest_of(l)):
            if i in which:
                remote(src, dst, send_sem.at[7], pw_sem.at[l, 3 + i], line + partner)

    def await_rest(l, which):
        for i, (src, dst) in enumerate(rest_of(l)):
            if i in which:
                loads["rest", l][i].wait()
                await_recv(dst, pw_sem.at[l, 3 + i])

    ONLY_WO, ONLY_W2, ONLY_W1 = range(packs), (packs,), range(packs + 1, packs + 1 + n_chip)

    def load_cache(l):
        for which in range(2):
            for t in range(batch // 16):
                cache_copy(l, which, t).start()

    low = lax.broadcasted_iota(jnp.int32, (rows, lanes), 1) < head
    lane_id = lax.broadcasted_iota(jnp.int32, (16, 16 * head), 1)
    row_id = lax.broadcasted_iota(jnp.int32, (16, 16 * head), 0)
    onehot[...] = jnp.where(lane_id // head == row_id, 1.0, 0.0).astype(BF16)
    for copy in small_copies:
        copy.wait()

    mark("barrier")
    pl.semaphore_wait(barrier, n_row + 2 * n_col - 3)
    mark("entry2")
    for h in range(HALVES):
        there = pl.ds(pl.multiple_of(h * rows + (1 - side) * sub, sub), sub)
        remote(x_buf.at[there], state.at[0, h, :, own_at], send_sem.at[0], pair_sem.at[0, h], line + partner)

    def share_vectors(which):
        for i in which:
            mine_half = shared[i][1].at[core]
            remote(mine_half, mine_half, send_sem.at[6], pair_sem.at[1, i], line + partner)

    share_vectors((0,))
    for i in range(n_chip):
        for t in range(3):
            loads["qkv", 0][3 * i + t].wait()
        share_tile(0, i)
    share_vectors(range(1, len(shared)))
    for h in range(HALVES):
        state[0, h, :, own_at] = x_buf[pl.ds(pl.multiple_of(h * rows + side * sub, sub), sub)]
    load_cache(0)
    loads["rest", 0] = load_rest(0)
    for l in range(1, layers):
        loads["qkv", l] = load_qkv(l)
    len_all = jnp.transpose(jnp.broadcast_to(len_buf[...], (batch, batch)))

    def full_row(ref, l):
        return jnp.concatenate([ref[0, l:l + 1], ref[1, l:l + 1]], axis=1).astype(F32)

    def side_operand(gain, shift, l):
        at = lax.broadcasted_iota(jnp.int32, (16, near), 0)
        return jnp.where(at == 0, full_row(gain, l), jnp.where(at == 1, full_row(shift, l), 0.0)).astype(BF16)

    def qkv_tiles(lhs, l, first, last):
        full = jnp.dot(lhs, wqkv[l, :, first * 3 * lanes:last * 3 * lanes], preferred_element_type=F32)
        return [[full[:, (3 * i + t) * lanes:(3 * i + t + 1) * lanes] for t in range(3)] for i in range(last - first)]

    def qkv_side(l):
        lhs = side_operand(ln1g, ln1b, l)
        for i, tiles in enumerate(qkv_tiles(lhs, l, 0, n_chip)):
            q, k, v = [a[0:8] for a in tiles]
            q_r, k_r, v_r = [pltpu.roll(a, head, axis=1) for a in (q, k, v)]
            low8 = low[0:8]
            qk = jnp.where(core == 0, jnp.where(low8, q, k_r), jnp.where(low8, q_r, k))
            vs = jnp.where(core == 0, jnp.where(low8, v, v_r), jnp.where(low8, v_r, v))
            at = lax.broadcasted_iota(jnp.int32, (8, lanes), 0)
            cq_src[l, i] = jnp.where(at < 2, qk, pltpu.roll(vs, 2, axis=0))
        for i in range(far):
            remote(cq_src.at[l, i], cq_in.at[l, i], send_sem.at[1], cq_sem.at[l, i], line + mates[i])

    def up_side(l):
        lhs = side_operand(ln2g, ln2b, l)
        for i in range(n_chip):
            at = pl.ds(pl.multiple_of((2 * i + core) * ff, ff), ff)
            cu_src[l, i] = jnp.dot(lhs, w1[l, :, at], preferred_element_type=F32)[0:8]
        for i in range(far):
            remote(cu_src.at[l, i], cu_in.at[l, i], send_sem.at[1], cu_sem.at[l, i], line + mates[i])

    def normalize(n, h, gain, l):
        mark("norm")
        x = state[n, h].astype(F32)
        s1 = jnp.sum(x, axis=1, keepdims=True)
        s2 = jnp.sum(x * x, axis=1, keepdims=True)
        mean = s1 / near
        inv = lax.rsqrt(jnp.maximum(s2 / near - mean * mean, 0.0) + EPS_LN)
        z = ((x - mean) * inv * full_row(gain, l)).astype(BF16)
        lane = lax.broadcasted_iota(jnp.int32, (sub, 128), 1)
        both = jnp.where(lane == 0, s1, jnp.where(lane == 1, s2, 0.0))
        both = jnp.concatenate([both, jnp.zeros((128 - sub, 128), F32)], axis=0)
        mine_stat = jnp.transpose(both)[0:2]
        stat_src[n, h] = mine_stat
        stat_in[n, h, far, side] = mine_stat
        return z

    def send_stats(n, h):
        for i, e, target in everyone():
            remote(stat_src.at[n, h], stat_in.at[n, h, i, side], send_sem.at[1], stat_sem.at[n, h, i, side], line + target)

    def stat_columns(n, h):
        for i, e in senders():
            await_recv(stat_in.at[n, h, i, e], stat_sem.at[n, h, i, e])
        table = []
        for e in (0, 1):
            parts = [stat_in[n, h, i, e] for i in range(n_chip)]
            total = parts[0]
            for part in parts[1:]:
                total = total + part
            mean = total[0:1] / width
            inv = lax.rsqrt(total[1:2] / width - mean * mean + EPS_LN)
            shifts = []
            for part in parts:
                near_mean = part[0:1] / near
                near_var = jnp.maximum(part[1:2] / near - near_mean * near_mean, 0.0) + EPS_LN
                table.append(inv * (near_var * lax.rsqrt(near_var)))
                shifts.append(inv * (near_mean - mean))
            table.extend(shifts)
        columns = jnp.transpose(jnp.concatenate(table, axis=0))[0:sub]

        def pick(start):
            return [[columns[:, e * 2 * n_chip + start + i:e * 2 * n_chip + start + i + 1] for i in range(n_chip)] for e in (0, 1)]

        return pick(0), pick(n_chip)

    def fold(column):
        return jnp.where(low[0:sub // 2], column[0:sub // 2], column[sub // 2:])

    def send_blocks(src, dst, sem, l, h, first, last):
        for i in range(first, last):
            for c in (0, 1) if i < far else (1 - core,):
                remote(src.at[l, h, i, c], dst.at[l, h, i, side], send_sem.at[2], sem.at[l, h, i, side],
                       line + chips[i] * 2 + c)
        if last == n_chip:
            dst[l, h, far, side] = src[l, h, far, core]

    fresh = {}

    def qkv_go(l, h):
        n = 2 * l
        z = normalize(n, h, ln1g, l)
        send_stats(n, h)
        mark("qkv_mm")
        for i in range(n_chip):
            if l == 0 and h == 0:
                await_qkv(0, i)
                q, k, v = qkv_tiles(z, l, i, i + 1)[0]
            else:
                if i in (0, 2):
                    tiles = qkv_tiles(z, l, i, i + 2)
                q, k, v = tiles[i % 2]
            q_r, k_r, v_r = [pltpu.roll(a, head, axis=1) for a in (q, k, v)]
            low_s, low_h = low[0:sub], low[0:sub // 2]
            qkv_src[l, h, i, 0, 0:sub] = jnp.where(low_s, q, k_r).astype(BF16)
            qkv_src[l, h, i, 1, 0:sub] = jnp.where(low_s, q_r, k).astype(BF16)
            qkv_src[l, h, i, 0, sub:] = jnp.where(low_h, v[:sub // 2], v_r[sub // 2:]).astype(BF16)
            qkv_src[l, h, i, 1, sub:] = jnp.where(low_h, v_r[:sub // 2], v[sub // 2:]).astype(BF16)
            if i == 1:
                send_blocks(qkv_src, qkv_in, qkv_sem, l, h, 0, 2)
        send_blocks(qkv_src, qkv_in, qkv_sem, l, h, 2, n_chip)

    def qkv_recv(l, h):
        mark("qkv_wait")
        if h == 0:
            const = bias_own[l] + cq_src[l, far]
            cq_in[l, far] = cq_src[l, far]
            for i in range(far):
                await_recv(cq_in.at[l, i], cq_sem.at[l, i])
                const = const + cq_in[l, i]
            bias_own[l] = const
        scales, shifts = stat_columns(2 * l, h)
        qk, vv = [], []
        for e in (0, 1):
            a = jnp.broadcast_to(bias_own[l, 1:2], (sub, lanes))
            b = jnp.broadcast_to(bias_own[l, 3:4], (sub // 2, lanes))
            for i in range(n_chip):
                a = a + shifts[e][i] * cq_in[l, i, 0:1]
                b = b + fold(shifts[e][i]) * cq_in[l, i, 2:3]
            qk.append(a)
            vv.append(b)
        for i, e in senders():
            await_recv(qkv_in.at[l, h, i, e], qkv_sem.at[l, h, i, e])
        mark("qkv_sum")
        for e in (0, 1):
            for i in range(n_chip):
                qk[e] = qk[e] + qkv_in[l, h, i, e, 0:sub].astype(F32) * scales[e][i]
                vv[e] = vv[e] + qkv_in[l, h, i, e, sub:].astype(F32) * fold(scales[e][i])
        qk = jnp.concatenate(qk, axis=0)
        q_b = (qk[:, 0:head] * (head ** -0.5)).astype(BF16)
        k_new = pltpu.roll(qk, head, axis=1)[:, 0:head].astype(BF16)
        v_new = jnp.concatenate([piece for b in vv for piece in (b[:, 0:head], pltpu.roll(b, head, axis=1)[:, 0:head])],
                                axis=0).astype(BF16)
        q_f = q_b.astype(F32)
        k_f = k_new.astype(F32)
        twin[h * rows:(h + 1) * rows, :] = jnp.concatenate([q_f, q_f], axis=1).astype(BF16)
        fresh[l, h] = (jnp.sum(q_f * k_f, axis=1, keepdims=True), k_f, v_new.astype(F32))

    def attend(l, h):
        score_new, k_f, v_f = fresh[l, h]
        base = h * rows
        mine_rows = slice(base, base + rows)
        mark("scores")
        for t in range(rows // 16):
            cache_copy(l, 0, base // 16 + t).wait()
        on_mxu = 16 - SCORES_ON_VPU
        q_t = jnp.transpose(twin[mine_rows, :].astype(F32))[0:head]
        for t in range(rows // 16):
            at = slice(base + 16 * t, base + 16 * (t + 1))
            q_diag = jnp.concatenate([twin[at, :]] * (on_mxu * head // lanes), axis=1) * onehot[:, 0:on_mxu * head]
            keys = k_buf[l, base + 16 * t:base + 16 * t + on_mxu].reshape(on_mxu * head, s_max)
            scores[base + 16 * t:base + 16 * t + on_mxu, :] = jnp.dot(q_diag, keys, preferred_element_type=F32)[0:on_mxu]
            for i in range(on_mxu, 16):
                b = 16 * t + i
                terms = k_buf[l, base + b].astype(F32) * q_t[:, b:b + 1]
                scores[base + b:base + b + 1, :] = jnp.sum(terms, axis=0, keepdims=True)
        mark("softmax")
        sc = scores[mine_rows, :]
        position = lax.broadcasted_iota(jnp.int32, sc.shape, 1)
        sc = jnp.where(position < len_all[mine_rows, 0:1], sc, -jnp.inf)
        peak = jnp.maximum(jnp.max(sc, axis=1, keepdims=True), score_new)
        ex = jnp.exp(sc - peak)
        ex_new = jnp.exp(score_new - peak)
        mass = jnp.sum(ex, axis=1, keepdims=True) + ex_new
        inv = 1.0 / mass
        scores[mine_rows, :] = (ex * inv).astype(BF16).astype(F32)
        prob_new = (ex_new * inv).astype(BF16).astype(F32)
        for b in range(s_max // 128):
            probs_t[h, b * 128:(b + 1) * 128, :] = jnp.transpose(scores[mine_rows, b * 128:(b + 1) * 128]).astype(BF16)
        lane = lax.broadcasted_iota(jnp.int32, (head, rows), 1)
        mark("mix")

        def mix_step(t, acc):
            for u in range(2):
                cache_copy(l, 1, base // 16 + 2 * t + u).wait()
            on_mxu = 32 - ON_VPU
            values = v_buf[l, pl.ds(base + 32 * t, on_mxu)].reshape(on_mxu * head, s_max)
            full = jnp.dot(values, probs_t[h], preferred_element_type=F32)
            for i in range(on_mxu, 32):
                prob = scores[pl.ds(base + 32 * t + i, 1), :]
                terms = v_buf[l, base + 32 * t + i].astype(F32) * prob
                short = terms[:, 0:128]
                for b in range(1, s_max // 128):
                    short = short + terms[:, b * 128:(b + 1) * 128]
                acc = jnp.where(lane == 32 * t + i, jnp.sum(short, axis=1, keepdims=True), acc)
            for i in range(on_mxu):
                acc = jnp.where(lane == 32 * t + i, full[i * head:(i + 1) * head], acc)
            return acc

        mixed = lax.fori_loop(0, rows // 32, mix_step, jnp.zeros((head, rows), F32))
        mark("att_send")
        mixed = jnp.transpose(mixed) + prob_new * v_f
        for e in (0, 1):
            first = mixed[e * sub:e * sub + sub // 2]
            second = mixed[e * sub + sub // 2:(e + 1) * sub]
            att_src[l, h, e] = jnp.concatenate([first, second], axis=1).astype(BF16)
        for i, e, target in everyone():
            remote(att_src.at[l, h, e], att_in.at[l, h, me], send_sem.at[3], att_sem.at[l, h, me], line + target)
        att_in[l, h, me] = att_src[l, h, side]
        fresh[l, h] = (k_f, v_f)

    def keep_fresh(l, h):
        k_f, v_f = fresh[l, h]
        k_out[l, :, h * rows:(h + 1) * rows] = jnp.transpose(k_f).astype(BF16)
        v_out[l, :, h * rows:(h + 1) * rows] = jnp.transpose(v_f).astype(BF16)

    def col_send(buf, sem, l, h):
        mark("col_send")
        for k in (2, 1, 3):
            remote(buf.at[l, h, mine], buf.at[l, h, mine], send_sem.at[4], sem.at[l, h, mine], col_peer(k, side))

    def col_recv(buf, sem, l, h, bias, base):
        mark("col_wait")
        for k in range(1, n_col):
            j = lax.rem(mine + k, n_col)
            await_recv(buf.at[l, h, j], sem.at[l, h, j])
        mark("col_sum")
        summed = buf[l, h, 0].astype(F32)
        for j in range(1, n_col):
            summed = summed + buf[l, h, j].astype(F32)
        return (base.astype(F32) + (summed + full_row(bias, l))).astype(BF16)

    def project(l, h):
        mark("att_wait")
        for k in range(1, n_row):
            j = lax.rem(me + k, n_row)
            await_recv(att_in.at[l, h, j], att_sem.at[l, h, j])
        mark("wo_mm")
        low_h = low[0:sub // 2]
        pieces = []
        for j in range(n_row):
            piece = att_in[l, h, j]
            none = jnp.zeros_like(piece)
            pieces.append(jnp.concatenate([jnp.where(low_h, piece, none), jnp.where(low_h, none, piece)], axis=0))
        total = jnp.dot(jnp.concatenate(pieces, axis=1), wo[l].reshape(n_row * lanes, near), preferred_element_type=F32)
        proj_in[l, h, mine] = total.astype(BF16)
        col_send(proj_in, proj_sem, l, h)

    def up_go(l, h):
        n = 2 * l + 1
        z = normalize(n, h, ln2g, l)
        send_stats(n, h)
        mark("up_mm")
        for first, last in ((0, 2), (2, n_chip)):
            full = jnp.dot(z, w1[l, :, first * 2 * ff:last * 2 * ff], preferred_element_type=F32).astype(BF16)
            for i in range(first, last):
                for c in (0, 1):
                    at = (2 * (i - first) + c) * ff
                    up_src[l, h, i, c] = full[:, at:at + ff]
            send_blocks(up_src, up_in, up_sem, l, h, first, last)

    def up_recv(l, h):
        mark("up_wait")
        if h == 0:
            const = b1[l:l + 1, pl.ds(pl.multiple_of(me * ff, ff), ff)].astype(F32) + cu_src[l, far, 1:2]
            cu_in[l, far] = cu_src[l, far]
            for i in range(far):
                await_recv(cu_in.at[l, i], cu_sem.at[l, i])
                const = const + cu_in[l, i, 1:2]
            cu_in[l, far, 1:2] = const
        scales, shifts = stat_columns(2 * l + 1, h)
        totals = []
        for e in (0, 1):
            total = jnp.broadcast_to(cu_in[l, far, 1:2], (sub, ff))
            for i in range(n_chip):
                total = total + shifts[e][i] * cu_in[l, i, 0:1]
            totals.append(total)
        for i, e in senders():
            await_recv(up_in.at[l, h, i, e], up_sem.at[l, h, i, e])
        mark("up_sum")
        for e in (0, 1):
            for i in range(n_chip):
                totals[e] = totals[e] + up_in[l, h, i, e].astype(F32) * scales[e][i]
            act_src[l, h, e] = jnp.maximum(totals[e].astype(BF16), 0)
        for i, e, target in everyone():
            remote(act_src.at[l, h, e], act_in.at[l, h, me], send_sem.at[5], act_sem.at[l, h, me], line + target)
        act_in[l, h, me] = act_src[l, h, side]

    def down(l, h):
        mark("act_wait")
        part = None
        for place, dc in enumerate((0, 1, 3, 2)):
            c = lax.rem(chip + n_chip - dc, n_chip)
            if dc == 0:
                await_recv(act_in.at[l, h, partner], act_sem.at[l, h, partner])
            else:
                for e in (0, 1):
                    await_recv(act_in.at[l, h, 2 * c + e], act_sem.at[l, h, 2 * c + e])
            both = jnp.concatenate([act_in[l, h, 2 * c], act_in[l, h, 2 * c + 1]], axis=1)
            at = pl.ds(pl.multiple_of(c * 2 * ff, 2 * ff), 2 * ff)
            term = jnp.dot(both, w2[l, at, :], preferred_element_type=F32)
            part = term if part is None else part + term
        mark("down_mm")
        part = part.astype(BF16)
        if l + 1 < layers:
            down_in[l, h, mine] = part
            col_send(down_in, down_sem, l, h)
            return
        mark("col_send")
        for c in (0, 1):
            h_src[h, c] = part[:, c * cols:(c + 1) * cols]
        for k in (2, 1, 3):
            for c in (0, 1):
                remote(h_src.at[h, c], h_in.at[h, mine, side], send_sem.at[4], h_sem.at[h, mine, side],
                       column[k] + chip * 2 + c)
        remote(h_src.at[h, 1 - core], h_in.at[h, mine, side], send_sem.at[4], h_sem.at[h, mine, side], line + partner)
        h_in[h, mine, side] = h_src[h, core]

    def finish(h):
        mark("col_wait")
        await_recv(mid_in.at[h], pair_sem.at[2, h])
        for k in range(1, n_col):
            for e in (0, 1):
                j = lax.rem(mine + k, n_col)
                await_recv(h_in.at[h, j, e], h_sem.at[h, j, e])
        await_recv(h_in.at[h, mine, 1 - side], h_sem.at[h, mine, 1 - side])
        mark("last")
        bias = b2[core, layers - 1:layers].astype(F32)
        for e in (0, 1):
            summed = h_in[h, 0, e].astype(F32)
            for j in range(1, n_col):
                summed = summed + h_in[h, j, e].astype(F32)
            base = jnp.where(side == e, state[2 * layers - 1, h, :, own_at].astype(F32), mid_in[h].astype(F32))
            at = h * rows + e * sub
            h_out[at:at + sub] = (base + (summed + bias)).astype(BF16)

    mark("side0")
    for h in range(HALVES):
        await_recv(state.at[0, h, :, own_at], pair_sem.at[0, h])
    await_recv(ln1g.at[core], pair_sem.at[1, 0])
    def own_head(vec_ref, l):
        total = jnp.zeros((1, head), F32)
        for j in range(n_row):
            total = total + jnp.where(me == j, vec_ref[l:l + 1, j * head:(j + 1) * head].astype(F32), 0.0)
        return total

    def own_biases():
        zero = jnp.zeros((1, lanes), F32)
        for l in range(layers):
            vb = own_head(bv, l)
            bias_own[l] = jnp.concatenate([zero, jnp.concatenate([own_head(bq, l), own_head(bk, l)], axis=1), zero,
                                           jnp.concatenate([vb, vb], axis=1)] + [zero] * 4, axis=0)

    last = HALVES - 1
    for stage, l, h in stage_order(layers, HALVES):
        n = 2 * l
        if l > 0 and stage == "go":
            new_state = col_recv(down_in, down_sem, l - 1, h, b2, state[n - 1, h])
        if stage == "go":
            if l > 0:
                state[n, h] = new_state
            qkv_go(l, h)
            mark("side")
            if l == 0 and h == 0:
                for i in range(1, len(shared)):
                    await_recv(shared[i][1].at[core], pair_sem.at[1, i])
                qkv_side(0)
            if l == 0 and h == last:
                own_biases()
                share_rest(0, ONLY_WO)
                share_rest(0, ONLY_W1)
                share_rest(0, ONLY_W2)
                for later in range(1, layers):
                    load_cache(later)
                    loads["rest", later] = load_rest(later)
            if l > 0 and h == 0:
                await_rest(l, ONLY_W1)
                up_side(l)
        elif stage == "attend":
            qkv_recv(l, h)
            attend(l, h)
            if l + 1 < layers and h == last:
                mark("side")
                for copy in loads["qkv", l + 1]:
                    copy.wait()
                share_qkv(l + 1)
        elif stage == "project":
            if h == 0:
                await_rest(l, ONLY_WO)
            project(l, h)
            mark("side")
            if h == 0 and l == 0:
                await_rest(l, ONLY_W1)
                up_side(l)
            if h < last:
                keep_fresh(l, h)
        elif stage == "up":
            state[n + 1, h] = col_recv(proj_in, proj_sem, l, h, bo, state[n, h])
            up_go(l, h)
            if h == 0:
                mark("side")
                keep_fresh(l, last)
                if l + 1 < layers:
                    share_rest(l + 1, ONLY_WO)
                    share_rest(l + 1, ONLY_W1)
                    share_rest(l + 1, ONLY_W2)
            if l + 1 == layers:
                there = pl.ds(pl.multiple_of((1 - core) * cols, cols), cols)
                remote(state.at[n + 1, h, :, there], mid_in.at[h], send_sem.at[0], pair_sem.at[2, h], line + partner)
            if h == 0 and l + 1 < layers:
                mark("side")
                for i in range(n_chip):
                    await_qkv(l + 1, i)
                qkv_side(l + 1)
        elif stage == "act":
            up_recv(l, h)
        elif stage == "down":
            if h == 0:
                await_rest(l, ONLY_W2)
            down(l, h)
        else:
            finish(h)
    mark("tail")
    for copy in pending:
        copy.wait_send()
    mark(None)


def store(*refs):
    copies = [pltpu.make_async_copy(refs[i], refs[3 + i], refs[6].at[i]) for i in range(3)]
    for copy in copies:
        copy.start()
    for copy in copies:
        copy.wait()


def solution(mesh):
    n_row = mesh.shape["row"]
    n_col = mesh.shape["col"]
    act_spec = P("dp", "row")
    cache_spec = P(None, "dp", ("col", "row"), None, None)
    fresh_spec = P(None, "dp", ("col", "row"), None)
    in_weight = P(None, "row", "col")
    out_weight = P(None, "col", "row")
    col_vec = P(None, "col")
    row_vec = P(None, "row")
    in_specs = (act_spec, P("dp"), cache_spec, cache_spec, row_vec, row_vec,
                in_weight, col_vec, in_weight, col_vec, in_weight, col_vec,
                out_weight, row_vec, row_vec, row_vec, in_weight, col_vec, out_weight, row_vec)

    def local_step(hidden, cache_len, k_cache, v_cache, *params):
        rows, cols = hidden.shape
        layers, _, _, s_max, head = k_cache.shape
        keys = jnp.swapaxes(k_cache, 3, 4).reshape(layers, rows, head, s_max)
        values = jnp.swapaxes(v_cache, 3, 4).reshape(layers, rows, head, s_max)
        operands = [hidden, cache_len.reshape(1, rows), keys, values, *params]
        packs = 2
        operands[12] = params[8].reshape(layers, n_row, head, cols)
        dma = pltpu.SemaphoreType.DMA
        ff = params[12].shape[2]
        n_chip = n_row // 2
        ff_own = ff // n_row
        near = 2 * cols
        sub = rows // HALVES // 2
        shapes = [(2,) + a.shape if i in (4, 5, 13, 14, 15, 19) else a.shape for i, a in enumerate(operands)]
        shapes[6] = (layers, near, 3 * shapes[6][2])
        shapes[16] = (layers, near, ff)
        shapes[12] = (layers, n_row, 2, head, near)
        shapes[18] = (layers, ff, near)
        vmem = [pltpu.VMEM(s, a.dtype) for i, (s, a) in enumerate(zip(shapes, operands)) if i not in (8, 10)]
        block = sub + sub // 2
        scratch = vmem + [
            pltpu.VMEM((2 * layers, HALVES, sub, near), BF16),
            pltpu.VMEM((2 * layers, HALVES, 2, 128), F32),
            pltpu.VMEM((2 * layers, HALVES, n_chip, 2, 2, 128), F32),
            pltpu.VMEM((layers, n_chip, 8, 2 * head), F32),
            pltpu.VMEM((layers, n_chip, 8, 2 * head), F32),
            pltpu.VMEM((layers, n_chip, 8, ff_own), F32),
            pltpu.VMEM((layers, n_chip, 8, ff_own), F32),
            pltpu.VMEM((layers, 8, 2 * head), F32),
            pltpu.VMEM((layers, HALVES, n_chip, 2, block, 2 * head), BF16),
            pltpu.VMEM((layers, HALVES, n_chip, 2, block, 2 * head), BF16),
            pltpu.VMEM((layers, HALVES, 2, sub // 2, 2 * head), BF16),
            pltpu.VMEM((layers, HALVES, n_row, sub // 2, 2 * head), BF16),
            pltpu.VMEM((layers, HALVES, n_col, sub, near), BF16),
            pltpu.VMEM((layers, HALVES, n_chip, 2, sub, ff_own), BF16),
            pltpu.VMEM((layers, HALVES, n_chip, 2, sub, ff_own), BF16),
            pltpu.VMEM((layers, HALVES, 2, sub, ff_own), BF16),
            pltpu.VMEM((layers, HALVES, n_row, sub, ff_own), BF16),
            pltpu.VMEM((layers, HALVES, n_col, sub, near), BF16),
            pltpu.VMEM((HALVES, 2, sub, cols), BF16),
            pltpu.VMEM((HALVES, n_col, 2, sub, cols), BF16),
            pltpu.VMEM((HALVES, sub, cols), BF16),
            pltpu.VMEM((rows, 2 * head), BF16),
            pltpu.VMEM((16, 16 * head), BF16),
            pltpu.VMEM((rows, s_max), F32),
            pltpu.VMEM((HALVES, s_max, rows // HALVES), BF16),
            dma((1 + layers, 24)),
            dma((layers, 2, rows // 16)),
            dma((9,)),
            dma((layers, 5 + packs + n_chip)),
            dma((3, 8)),
            dma((2 * layers, HALVES, n_chip, 2)),
            dma((layers, n_chip)),
            dma((layers, n_chip)),
            dma((layers, HALVES, n_chip, 2)),
            dma((layers, HALVES, n_row)),
            dma((layers, HALVES, n_col)),
            dma((layers, HALVES, n_chip, 2)),
            dma((layers, HALVES, n_row)),
            dma((layers, HALVES, n_col)),
            dma((HALVES, n_col, 2)),
            dma((layers, n_chip)),
        ]
        h, kt, vt = pl.pallas_call(
            functools.partial(kernel, n_row, n_col, cols * n_row),
            out_shape=(pltpu.VMEM((rows, cols), BF16),
                       pltpu.VMEM((layers, head, rows), BF16),
                       pltpu.VMEM((layers, head, rows), BF16)),
            in_specs=[pl.BlockSpec(memory_space=pltpu.HBM)] * len(operands),
            out_specs=[pl.BlockSpec(memory_space=pltpu.VMEM)] * 3,
            scratch_shapes=scratch,
            compiler_params=pltpu.CompilerParams(collective_id=0, has_side_effects=True,
                                                 vmem_limit_bytes=63 * 2 ** 20),
        )(*operands)
        h, kt, vt = pl.pallas_call(
            store,
            out_shape=(jax.ShapeDtypeStruct((rows, cols), BF16),
                       jax.ShapeDtypeStruct((layers, head, rows), BF16),
                       jax.ShapeDtypeStruct((layers, head, rows), BF16)),
            in_specs=[pl.BlockSpec(memory_space=pltpu.VMEM)] * 3,
            out_specs=[pl.BlockSpec(memory_space=pltpu.HBM)] * 3,
            scratch_shapes=[dma((3,))],
        )(*[pltpu.with_memory_space_constraint(a, pltpu.VMEM) for a in (h, kt, vt)])
        k_new = jnp.swapaxes(kt, 1, 2).reshape(layers, rows, 1, head)
        v_new = jnp.swapaxes(vt, 1, 2).reshape(layers, rows, 1, head)
        return h, k_new, v_new

    return jax.shard_map(local_step, mesh=mesh, in_specs=in_specs,
                         out_specs=(act_spec, fresh_spec, fresh_spec), check_vma=False)
```
